32 devices in a mesh: gx: 4 (over x, core), gy: 2 (over y), gz: 4 (over z).
Axes of the slice: x: 2, y: 2, z: 4, core: 2. Of those that a mesh axis runs over, the one named last changes fastest.
Arguments:
- start_field: float32 [256, 128, 1024], P('gx', 'gy', 'gz'), may hold values from -6 to 6
- right_side: float32 [256, 128, 1024], P('gx', 'gy', 'gz'), may hold values from -6 to 6
Outputs:
- corrected: float32 [256, 128, 1024], P('gx', 'gy', 'gz')
The draws below stay inside these ranges and needn't reach their ends.
All inputs are finite; a program needn't handle non-finite values.
Results may differ from the reference program's by a relative error of at most 0.00002.
Values sent between devices are 32-bit elements; how exact they have to be, the bound alone decides.
No kernel may reach another device: no remote copies, remote signals or barrier semaphores. Data moves between devices by JAX's collectives and lax.ppermute only.
A program may use at most 128 MiB of HBM per device.

```python
import jax
import jax.numpy as jnp
from jax import lax

FINE_SWEEPS = 2
COARSE_SWEEPS = 4
NX = 256
NY = 128
NZ = 1024


def draw_right_side(key, part):
    noise_field = jnp.clip(jax.random.normal(key, (NX, NY, NZ), jnp.float32), -6.0, 6.0)
    return noise_field


def levels(stream_key, dims, shards, smallest, top_value):
    def one(position, shards_of):
        draws = jax.random.uniform(jax.random.fold_in(jax.random.fold_in(stream_key, 6), position), (shards_of,), jnp.float32, smallest / len(shards), top_value / len(shards))
        return jnp.repeat(jnp.exp(draws), dims[position] // shards_of).reshape((-1,) + (1,) * (len(dims) - position - 1))

    factor_of = one(*shards[0])
    for cut in shards[1:]:
        factor_of = factor_of * one(*cut)
    return factor_of


def bell_draw(key, shape, spread, reach, pieces=(), kind=jnp.bfloat16):
    drawn = jax.random.normal(key, shape, jnp.float32) * spread
    if len(pieces) > 0:
        drawn = levels(key, shape, pieces, -0.22, 0.18) * drawn
    return jnp.clip(drawn, min=-reach, max=reach).astype(kind)


def setup_inputs(seed: int = 0) -> dict:
    seeds = jax.random.split(jax.random.key(seed), 3)
    start_field = bell_draw(seeds[0], (NX, NY, NZ), 1.0, 6.0, ((0, 4), (1, 2), (2, 4)), jnp.float32)
    right_side = draw_right_side(jax.random.fold_in(seeds[2], 71), 0)
    return {"start_field": start_field, "right_side": right_side}


relaxation = 6.0 / 7.0


def apply_stencil(values):
    padded = jnp.pad(values, 1)
    beside = padded[2:, 1:-1, 1:-1] + padded[:-2, 1:-1, 1:-1]
    beside = beside + padded[1:-1, 2:, 1:-1] + padded[1:-1, :-2, 1:-1]
    beside = beside + padded[1:-1, 1:-1, 2:] + padded[1:-1, 1:-1, :-2]
    return 6.0 * values - beside


def restrict_axis(values, which_axis):
    length = values.shape[which_axis]
    half_len = length // 2
    even_rows = lax.slice_in_dim(values, 0, length, 2, which_axis)
    odd_rows = lax.slice_in_dim(values, 1, length, 2, which_axis)
    zero_row = jnp.zeros_like(lax.slice_in_dim(even_rows, 0, 1, 1, which_axis))
    following = jnp.concatenate([lax.slice_in_dim(even_rows, 1, half_len, 1, which_axis), zero_row], which_axis)
    return 0.25 * even_rows + 0.5 * odd_rows + 0.25 * following


def prolong_axis(values, which_axis):
    length = values.shape[which_axis]
    zero_row = jnp.zeros_like(lax.slice_in_dim(values, 0, 1, 1, which_axis))
    previous = jnp.concatenate([zero_row, lax.slice_in_dim(values, 0, length - 1, 1, which_axis)], which_axis)
    even_rows = 0.5 * (previous + values)
    paired = jnp.stack([even_rows, values], which_axis + 1)
    new_shape = list(values.shape)
    new_shape[which_axis] = 2 * length
    return jnp.reshape(paired, new_shape)


def reference(start_field, right_side):
    smoothed = start_field
    for sweep_num in range(FINE_SWEEPS):
        smoothed = smoothed + (relaxation / 6.0) * (right_side - apply_stencil(smoothed))
    residual = right_side - apply_stencil(smoothed)
    coarse_rhs = restrict_axis(restrict_axis(restrict_axis(residual, 0), 1), 2)
    correction = jnp.zeros_like(coarse_rhs)
    for sweep_num in range(COARSE_SWEEPS):
        correction = correction + (relaxation / 1.5) * (coarse_rhs - 0.25 * apply_stencil(correction))
    fine_corr = prolong_axis(prolong_axis(prolong_axis(correction, 0), 1), 2)
    return smoothed + fine_corr
```

```python
import functools

import jax
import jax.numpy as jnp
from jax import lax
from jax.experimental import pallas as pl
from jax.experimental.pallas import tpu as pltpu
from jax.sharding import PartitionSpec as P

LANES = 128
F = 3
G = 2
SLOT = F + G
PER = LANES // SLOT
CL = 4
CH = 3
CPER = LANES // CL

VMEM = pl.BlockSpec(memory_space=pltpu.VMEM)
ANY = pl.BlockSpec(memory_space=pl.ANY)


def f32(*shape):
    return jax.ShapeDtypeStruct(shape, jnp.float32)


def call(body, name, ins, outs, scratch=(), alias=None, limit=None, out_specs=None):
    return pl.pallas_call(
        body,
        name=name,
        in_specs=[VMEM] * len(ins),
        out_specs=[VMEM] * len(outs) if out_specs is None else out_specs,
        out_shape=outs,
        scratch_shapes=list(scratch),
        input_output_aliases=alias or {},
        compiler_params=pltpu.CompilerParams(vmem_limit_bytes=limit),
    )(*ins)


def iota(shape, dim):
    return lax.broadcasted_iota(jnp.int32, shape, dim)


def ends(axis):
    i = lax.axis_index(axis)
    return i == 0, i == lax.axis_size(axis) - 1


def exchange(msgs, axis):
    n = lax.axis_size(axis)
    if n == 2:
        return [lax.ppermute(msgs[0], axis, [(0, 1), (1, 0)])]
    down = lax.ppermute(msgs[0], axis, [(i + 1, i) for i in range(n - 1)])
    up = lax.ppermute(msgs[1], axis, [(i, i + 1) for i in range(n - 1)])
    return [down, up]


def emit(outs, index, axis, low, high):
    if len(outs) == 1:
        outs[0][index] = jnp.where(ends(axis)[0], high(), low())
    else:
        outs[0][index] = low()
        outs[1][index] = high()


def arrived(refs, index, axis):
    if len(refs) == 1:
        value = refs[0][index]
        first = ends(axis)[0]
        zero = jnp.zeros_like(value)
        return jnp.where(first, value, zero), jnp.where(first, zero, value)
    return refs[0][index], refs[1][index]


def count(axis):
    return 1 if lax.axis_size(axis) == 2 else 2


def build_body(start, right, se, re):
    nx, ny, nz = start.shape

    def plane(p, _):
        for t in range(nz // LANES):
            se[t, p, 0:ny, :] = start[p, :, t * LANES:(t + 1) * LANES]
            re[t, p, 0:ny, :] = right[p, :, t * LANES:(t + 1) * LANES]
        return 0

    lax.fori_loop(0, nx, plane, 0, unroll=2)


def xhalo_body(nx, ny, nz, nin, *refs):
    halo = refs[:nin]
    se, re, outs = refs[nin + 2], refs[nin + 3], refs[nin + 4:]
    xe, ye = nx + 8, ny + 8
    nt = nz // LANES
    for t in range(nt):
        cut = slice(t * LANES, (t + 1) * LANES)
        for k in range(SLOT):
            high, low = arrived(halo, (k, slice(None), cut), "gx")
            dst, size, j = (se, F, k) if k < F else (re, G, k - F)
            dst[t, nx + j, 0:ny, :] = high
            dst[t, xe - size + j, 0:ny, :] = low
    se2 = se.reshape(nt + 1, xe * ye, LANES)
    re2 = re.reshape(nt + 1, xe * ye, LANES)
    for t in range(nt):
        for k in range(SLOT):
            src, size, j = (se2, F, k) if k < F else (re2, G, k - F)
            emit(
                outs, (k * nt + t,), "gy",
                lambda: src[t, pl.ds(j, xe, stride=ye), :],
                lambda: src[t, pl.ds(ny - size + j, xe, stride=ye), :],
            )


def yhalo_body(nx, ny, nz, nin, *refs):
    halo = refs[:nin]
    se, re, outs = refs[nin + 2], refs[nin + 3], refs[nin + 4:]
    xe, ye = nx + 8, ny + 8
    nt = nz // LANES
    se2 = se.reshape(nt + 1, xe * ye, LANES)
    re2 = re.reshape(nt + 1, xe * ye, LANES)
    for t in range(nt):
        for k in range(SLOT):
            high, low = arrived(halo, (k * nt + t,), "gy")
            dst, size, j = (se2, F, k) if k < F else (re2, G, k - F)
            dst[t, pl.ds(ny + j, xe, stride=ye), :] = high
            dst[t, pl.ds(ye - size + j, xe, stride=ye), :] = low
    lane = iota((ye, LANES), 1)

    def tile(group, _):
        low = jnp.zeros((ye, LANES), jnp.float32)
        high = jnp.zeros((ye, LANES), jnp.float32)
        for j in range(PER):
            p = jnp.minimum(group * PER + j, xe - 1)
            at = j * SLOT
            in_s = (lane >= at) & (lane < at + F)
            in_r = (lane >= at + F) & (lane < at + SLOT)
            low = jnp.where(in_s, pltpu.roll(se[0, p], at, 1), low)
            low = jnp.where(in_r, pltpu.roll(re[0, p], at + F, 1), low)
            high = jnp.where(in_s, pltpu.roll(se[nt - 1, p], (at + F) % LANES, 1), high)
            high = jnp.where(in_r, pltpu.roll(re[nt - 1, p], (at + SLOT) % LANES, 1), high)
        emit(outs, (group,), "gz", lambda: low, lambda: high)
        return 0

    lax.fori_loop(0, -(-xe // PER), tile, 0)


def neighbours(ref, q, before, after, tiles):
    total = ref.shape[0]
    rows = ref.shape[2]
    lane = iota((rows, LANES), 1)
    centre = [ref[t, q] for t in range(total)]
    left = [pltpu.roll(c, 1, 1) for c in centre]
    right = [pltpu.roll(c, LANES - 1, 1) for c in centre]
    found = []
    for t in range(tiles):
        c = centre[t]
        near = jnp.where(lane == 0, left[t - 1], left[t])
        near = near + jnp.where(lane == LANES - 1, right[(t + 1) % total], right[t])
        near = near + (pltpu.roll(c, 1, 0) + pltpu.roll(c, rows - 1, 0))
        near = near + (ref[t, before] + ref[t, after])
        found.append((c, near))
    return found


def wrap(q, size):
    return jnp.where(q < 0, q + size, jnp.where(q >= size, q - size, q))


def inside(shape, dim, cells, low, high, axis):
    first, last = ends(axis)
    at = iota(shape, dim)
    size = shape[dim]
    up = jnp.where(last, 0.0, 1.0)
    down = jnp.where(first, 0.0, 1.0)
    return jnp.where(at < cells, 1.0, jnp.where(at < cells + high, up, jnp.where(at >= size - low, down, 0.0)))


def split_dot(value, weight):
    high = value.astype(jnp.bfloat16)
    rest = value - high.astype(jnp.float32)
    mid = rest.astype(jnp.bfloat16)
    small = (rest - mid.astype(jnp.float32)).astype(jnp.bfloat16)
    dot = functools.partial(jnp.dot, preferred_element_type=jnp.float32)
    return dot(high, weight) + dot(mid, weight) + dot(small, weight)


def smooth_body(nx, ny, nz, nin, *refs):
    halo = refs[:nin]
    se, re, s2, coarse = refs[nin + 2:nin + 6]
    outs = refs[nin + 6:-4]
    s1, rx, rz, mask = refs[-4:]
    xe, ye = nx + 8, ny + 8
    nt = nz // LANES
    lane = iota((ye, LANES), 1)

    def unpack(group, _):
        high, low = arrived(halo, (group,), "gz")
        for j in range(PER):
            p = jnp.minimum(group * PER + j, xe - 1)
            at = j * SLOT

            @pl.when(group * PER + j < xe)
            def _():
                se[nt, p] = jnp.where(
                    lane < 64, pltpu.roll(high, (-at) % LANES, 1), pltpu.roll(low, (-F - at) % LANES, 1)
                )
                re[nt, p] = jnp.where(
                    lane < 64, pltpu.roll(high, (-at - F) % LANES, 1), pltpu.roll(low, (-G - at - F) % LANES, 1)
                )
        return 0

    lax.fori_loop(0, -(-xe // PER), unpack, 0)

    valid = inside((ye, LANES), 0, ny, F, F, "gy")
    for t in range(nt):
        mask[t] = valid * (1.0 / 7.0)
    mask[nt] = valid * inside((ye, LANES), 1, 0, F, F, "gz") * (1.0 / 7.0)

    first, last = ends("gx")
    up = jnp.where(last, 0.0, 1.0)
    down = jnp.where(first, 0.0, 1.0)

    def sweep(src, dst, reach):
        def plane(q, factor):
            found = neighbours(src, q, wrap(q - 1, xe), wrap(q + 1, xe), nt + 1)
            for t, (c, near) in enumerate(found):
                m = mask[t] if factor is None else mask[t] * factor
                dst[t, q] = m * (near + (c + re[t, q]))

        def inner(q, _):
            plane(q, None)
            return 0

        lax.fori_loop(0, nx, inner, 0)

        def outer(k, _):
            plane(jnp.where(k < reach, nx + k, xe - 2 * reach + k), jnp.where(k < reach, up, down))
            return 0

        lax.fori_loop(0, 2 * reach, outer, 0)

    sweep(se, s1, 2)
    sweep(s1, s2, 1)

    def residual(q):
        found = neighbours(s2, q, wrap(q - 1, xe), wrap(q + 1, xe), nt)
        return [(re[t, q] + (near - 6.0 * c))[0:ny] for t, (c, near) in enumerate(found)]

    for t in range(nt):
        rx[0:ny, t * LANES:(t + 1) * LANES] = jnp.zeros((ny, LANES), jnp.float32)

    def pair(i, _):
        even = residual(2 * i)
        at = pl.multiple_of(i * ny, 8)
        for t in range(nt):
            cut = slice(t * LANES, (t + 1) * LANES)
            rx[pl.ds(at, ny), cut] = rx[pl.ds(at, ny), cut] + 0.25 * even[t]
        odd = residual(2 * i + 1)
        for t in range(nt):
            cut = slice(t * LANES, (t + 1) * LANES)
            rx[pl.ds(at + ny, ny), cut] = 0.25 * even[t] + 0.5 * odd[t]
        return 0

    lax.fori_loop(0, nx // 2, pair, 0)

    cz = nz // 2
    ct = cz // LANES
    wide = (ct + 1) * LANES
    z = iota((nz, wide), 0)
    k = iota((nz, wide), 1)
    k = jnp.where(k >= cz, k - wide, k)
    off = z - 2 * k
    weight = jnp.where((off == 0) | (off == 2), 0.25, jnp.where(off == 1, 0.5, 0.0))
    weight = jnp.where(k < -1, 0.0, weight).astype(jnp.bfloat16)

    def zpart(i, _):
        at = pl.multiple_of(i * ny, 8)
        got = split_dot(rx[pl.ds(at, ny), :], weight)
        for t in range(ct + 1):
            rz[t, pl.ds(at, ny), :] = got[:, t * LANES:(t + 1) * LANES]
        return 0

    cx, cy = nx // 2, ny // 2
    lax.fori_loop(0, cx + 1, zpart, 0, unroll=3)

    row = iota((cy, LANES), 0)
    row8 = iota((8, LANES), 0)

    def ypart(i, _):
        q = jnp.where(i == 0, cx + 7, i - 1)
        for t in range(ct + 1):
            even = rz[t, pl.ds(i * ny, cy, stride=2), :]
            odd = rz[t, pl.ds(i * ny + 1, cy, stride=2), :]
            after = rz[t, pl.ds(i * ny + 2, cy, stride=2), :]
            after = jnp.where(row == cy - 1, 0.0, after)
            coarse[t, q, 0:cy, :] = 0.25 * even + 0.5 * odd + 0.25 * after
            coarse[t, q, cy:cy + 8, :] = jnp.where(row8 == 7, 0.25 * even[0:1], 0.0)
        return 0

    rz[:, (cx + 1) * ny:(cx + 1) * ny + 8, :] = jnp.zeros((ct + 1, 8, LANES), jnp.float32)
    lax.fori_loop(0, cx + 1, ypart, 0)
    for q in range(cx, cx + 7):
        for t in range(ct + 1):
            coarse[t, q] = jnp.zeros((cy + 8, LANES), jnp.float32)

    def layer(t, q):
        return coarse[t, q]

    faces(outs, "gx", lambda t, j: coarse[t, (cx + 7 + j) % (cx + 8)], lambda t, j: coarse[t, cx - CL + j], ct)


def faces(outs, axis, low, high, ct):
    extra_low = extra_high = None
    for j in range(CL):
        for t in range(ct):
            emit(outs, (j * ct + t,), axis, lambda: low(t, j), lambda: high(t, j))
        a = pltpu.roll(low(ct, j), (j + 1) % LANES, 1)
        b = pltpu.roll(high(ct, j), (j + 1) % LANES, 1)
        lane = iota(a.shape, 1)
        extra_low = a if j == 0 else jnp.where(lane == j, a, extra_low)
        extra_high = b if j == 0 else jnp.where(lane == j, b, extra_high)
    emit(outs, (CL * ct,), axis, lambda: extra_low, lambda: extra_high)


def place_faces(refs, axis, ct, size, read, write):
    for t in range(ct + 1):
        for j in range(CL):
            if t < ct:
                high, low = arrived(refs, (j * ct + t,), axis)
            else:
                high, low = arrived(refs, (CL * ct,), axis)
                lane = iota(high.shape, 1)
                turn = (LANES - 1 - j) % LANES
                high = jnp.where(lane == LANES - 1, pltpu.roll(high, turn, 1), 0.0)
                low = jnp.where(lane == LANES - 1, pltpu.roll(low, turn, 1), 0.0)
            if j == 0:
                write(t, size - 1, read(t, size - 1) + high)
            else:
                write(t, size + j - 1, high)
            if j == CL - 1:
                write(t, size + 7, read(t, size + 7) + low)
            else:
                write(t, size + 4 + j, low)


def coarse_x_body(cx, cy, cz, nin, *refs):
    halo = refs[:nin]
    coarse, outs = refs[nin + 1], refs[nin + 2:]
    ct = cz // LANES
    xe, ye = cx + 8, cy + 8

    def write(t, q, value):
        coarse[t, q] = value

    place_faces(halo, "gx", ct, cx, lambda t, q: coarse[t, q], write)
    flat = coarse.reshape(ct + 1, xe * ye, LANES)
    faces(
        outs, "gy",
        lambda t, j: flat[t, pl.ds((cy + 7 + j) % ye, xe, stride=ye), :],
        lambda t, j: flat[t, pl.ds(cy - CL + j, xe, stride=ye), :],
        ct,
    )


def coarse_y_body(cx, cy, cz, nin, *refs):
    halo = refs[:nin]
    coarse, outs = refs[nin + 1], refs[nin + 2:]
    ct = cz // LANES
    xe, ye = cx + 8, cy + 8
    flat = coarse.reshape(ct + 1, xe * ye, LANES)

    def write(t, q, value):
        flat[t, pl.ds(q, xe, stride=ye), :] = value

    place_faces(halo, "gy", ct, cy, lambda t, q: flat[t, pl.ds(q, xe, stride=ye), :], write)
    lane = iota((ye, LANES), 1)

    def tile(group, _):
        low = jnp.zeros((ye, LANES), jnp.float32)
        high = jnp.zeros((ye, LANES), jnp.float32)
        for j in range(CPER):
            p = jnp.minimum(group * CPER + j, xe - 1)
            at = j * CL
            head = jnp.where(lane < CL - 1, coarse[0, p], coarse[ct, p])
            head = pltpu.roll(head, (at + 1) % LANES, 1)
            here = (lane >= at) & (lane < at + CL)
            low = jnp.where(here, head, low)
            high = jnp.where(here, pltpu.roll(coarse[ct - 1, p], (at + CL) % LANES, 1), high)
        emit(outs, (group,), "gz", lambda: low, lambda: high)
        return 0

    lax.fori_loop(0, -(-xe // CPER), tile, 0)


def finish_body(cx, cy, cz, nin, *refs):
    halo = refs[:nin]
    smooth, _, coarse, out = refs[nin:nin + 4]
    ca, cb, mask, fine, stage, sems = refs[nin + 4:]
    ct = cz // LANES
    xe, ye = cx + 8, cy + 8
    nx, ny, nz = 2 * cx, 2 * cy, 2 * cz
    nt = nz // LANES
    lane = iota((ye, LANES), 1)
    first, last = ends("gx")
    up = jnp.where(last, 0.0, 1.0)
    down = jnp.where(first, 0.0, 1.0)

    valid = inside((ye, LANES), 0, cy, CL, CH, "gy")
    for t in range(ct):
        mask[t] = valid * (1.0 / 7.0)
    mask[ct] = valid * inside((ye, LANES), 1, 0, CL, CH, "gz") * (1.0 / 7.0)

    def unpack(group, _):
        high, low = arrived(halo, (group,), "gz")
        for j in range(CPER):
            p = group * CPER + j
            at = j * CL

            @pl.when(p < xe)
            def _():
                q = jnp.minimum(p, xe - 1)
                fromhigh = pltpu.roll(high, (-at - 1) % LANES, 1)
                fromlow = pltpu.roll(low, (-CL - at) % LANES, 1)
                tail = coarse[ct - 1, q]
                tail = tail + jnp.where(lane == LANES - 1, fromhigh, 0.0)
                wing = jnp.where(lane < CH, fromhigh, jnp.where(lane >= LANES - CL, fromlow, 0.0))
                wing = wing + jnp.where(lane == LANES - 1, coarse[ct, q], 0.0)
                xm = jnp.where(p < cx, 1.0, jnp.where(p < cx + CL, up, down))
                coarse[ct - 1, q] = 4.0 * tail
                coarse[ct, q] = 4.0 * wing
                for t in range(ct - 1):
                    coarse[t, q] = 4.0 * coarse[t, q]
                for t in range(ct + 1):
                    ca[t, q] = (mask[t] * xm) * coarse[t, q]
        return 0

    lax.fori_loop(0, -(-xe // CPER), unpack, 0)

    def sweep(src, dst, low, high):
        def step(k, _):
            p = k - low
            q = wrap(p, xe)
            xm = jnp.where(p < 0, down, jnp.where(p >= cx, up, 1.0))
            found = neighbours(src, q, wrap(p - 1, xe), wrap(p + 1, xe), ct + 1)
            for t, (c, near) in enumerate(found):
                dst[t, q] = (mask[t] * xm) * (near + (c + coarse[t, q]))
            return 0

        lax.fori_loop(0, cx + low + high, step, 0)

    sweep(ca, cb, 3, 2)
    sweep(cb, ca, 2, 1)
    sweep(ca, cb, 1, 0)

    wide = (ct + 1) * LANES
    k = iota((wide, nz), 0)
    z = iota((wide, nz), 1)
    k = jnp.where(k >= cz, k - wide, k)
    off = z - 2 * k
    weight = jnp.where(off == 1, 1.0, jnp.where((off == 0) | (off == 2), 0.5, 0.0))
    weight = jnp.where(k < -1, 0.0, weight).astype(jnp.bfloat16)

    def prolong(i, _):
        q = jnp.where(i == 0, xe - 1, i - 1)
        value = jnp.concatenate([cb[t, q] for t in range(ct + 1)], axis=1)
        got = split_dot(value, weight)
        even = 0.5 * (got + pltpu.roll(got, 1, 0))
        for t in range(nt):
            cut = slice(t * LANES, (t + 1) * LANES)
            fine[t, pl.ds(i * ny, cy, stride=2), :] = even[0:cy, cut]
            fine[t, pl.ds(i * ny + 1, cy, stride=2), :] = got[0:cy, cut]
        return 0

    lax.fori_loop(0, cx + 1, prolong, 0, unroll=3)

    chunks = sems.shape[0]
    per = cx // chunks

    def send(c):
        at = c * 2 * per
        return pltpu.make_async_copy(stage.at[pl.ds(at, 2 * per)], out.at[pl.ds(at, 2 * per)], sems.at[c])

    for c in range(chunks):
        def add(i, _):
            at = pl.multiple_of(i * ny, 8)
            for t in range(nt):
                cut = slice(t * LANES, (t + 1) * LANES)
                here = fine[t, pl.ds(at + ny, ny), :]
                before = fine[t, pl.ds(at, ny), :]
                stage[2 * i, :, cut] = smooth[t, 2 * i, 0:ny, :] + 0.5 * (before + here)
                stage[2 * i + 1, :, cut] = smooth[t, 2 * i + 1, 0:ny, :] + here
            return 0

        lax.fori_loop(c * per, (c + 1) * per, add, 0)
        send(c).start()
    for c in range(chunks):
        send(c).wait()


def on_device(start, right):
    nx, ny, nz = start.shape
    nt = nz // LANES
    xe, ye = nx + 8, ny + 8
    cx, cy, cz = nx // 2, ny // 2, nz // 2
    ct = cz // LANES
    cxe, cye = cx + 8, cy + 8
    big = f32(nt + 1, xe, ye, LANES)
    mb = 1 << 20

    to_prev = jnp.concatenate([start[:F], right[:G]], axis=0)
    to_next = jnp.concatenate([start[nx - F:], right[nx - G:]], axis=0)
    if count("gx") == 1:
        to_prev = jnp.where(ends("gx")[0], to_next, to_prev)
    halo = exchange([to_prev, to_next], "gx")
    se, re = call(build_body, "build", [start, right], [big, big], limit=8 * mb)

    n = len(halo)
    se, re, *msgs = call(
        functools.partial(xhalo_body, nx, ny, nz, n), "xhalo", [*halo, se, re],
        [big, big] + [f32(SLOT * nt, xe, LANES)] * count("gy"), alias={n: 0, n + 1: 1}, limit=8 * mb,
    )
    halo = exchange(msgs, "gy")
    n = len(halo)
    se, re, *msgs = call(
        functools.partial(yhalo_body, nx, ny, nz, n), "yhalo", [*halo, se, re],
        [big, big] + [f32(-(-xe // PER), ye, LANES)] * count("gz"), alias={n: 0, n + 1: 1}, limit=8 * mb,
    )
    halo = exchange(msgs, "gz")
    n = len(halo)
    small = f32(ct + 1, cxe, cye, LANES)
    se, re, s2, coarse, *msgs = call(
        functools.partial(smooth_body, nx, ny, nz, n), "smooth", [*halo, se, re],
        [big, big, big, small] + [f32(CL * ct + 1, cye, LANES)] * count("gx"),
        scratch=[
            pltpu.VMEM((nt + 1, xe, ye, LANES), jnp.float32),
            pltpu.VMEM(((cx + 1) * ny, nz), jnp.float32),
            pltpu.VMEM((ct + 1, (cx + 1) * ny + 8, LANES), jnp.float32),
            pltpu.VMEM((nt + 1, ye, LANES), jnp.float32),
        ],
        alias={n: 0, n + 1: 1}, limit=24 * mb,
    )
    halo = exchange(msgs, "gx")
    n = len(halo)
    coarse, *msgs = call(
        functools.partial(coarse_x_body, cx, cy, cz, n), "coarse_x", [*halo, coarse],
        [small] + [f32(CL * ct + 1, cxe, LANES)] * count("gy"), alias={n: 0}, limit=8 * mb,
    )
    halo = exchange(msgs, "gy")
    n = len(halo)
    coarse, *msgs = call(
        functools.partial(coarse_y_body, cx, cy, cz, n), "coarse_y", [*halo, coarse],
        [small] + [f32(-(-cxe // CPER), cye, LANES)] * count("gz"), alias={n: 0}, limit=8 * mb,
    )
    halo = exchange(msgs, "gz")
    n = len(halo)
    _, out = call(
        functools.partial(finish_body, cx, cy, cz, n), "finish", [*halo, s2, coarse],
        [small, f32(nx, ny, nz)],
        scratch=[
            pltpu.VMEM((ct + 1, cxe, cye, LANES), jnp.float32),
            pltpu.VMEM((ct + 1, cxe, cye, LANES), jnp.float32),
            pltpu.VMEM((ct + 1, cye, LANES), jnp.float32),
            pltpu.VMEM((nt, (cx + 1) * ny, LANES), jnp.float32),
            pltpu.VMEM((nx, ny, nz), jnp.float32),
            pltpu.SemaphoreType.DMA((8,)),
        ],
        alias={n + 1: 0}, limit=24 * mb, out_specs=[VMEM, ANY],
    )
    return out


def solution(mesh):
    spec = P("gx", "gy", "gz")
    return jax.shard_map(on_device, mesh=mesh, in_specs=(spec, spec), out_specs=spec, check_vma=False)
```

```python
import functools

import jax
import jax.numpy as jnp
from jax import lax
from jax.experimental import pallas as pl
from jax.experimental.pallas import tpu as pltpu
from jax.sharding import PartitionSpec as P

LANES = 128
O = 4
F = 3
G = 2
SLOT = F + G
PER = LANES // SLOT
CL = 4
CH = 3
CPER = LANES // CL

VMEM = pl.BlockSpec(memory_space=pltpu.VMEM)
ANY = pl.BlockSpec(memory_space=pl.ANY)


def f32(*shape):
    return jax.ShapeDtypeStruct(shape, jnp.float32)


def call(body, name, ins, outs, scratch=(), alias=None, limit=None, out_specs=None):
    return pl.pallas_call(
        body,
        name=name,
        in_specs=[VMEM] * len(ins),
        out_specs=[VMEM] * len(outs) if out_specs is None else out_specs,
        out_shape=outs,
        scratch_shapes=list(scratch),
        input_output_aliases=alias or {},
        compiler_params=pltpu.CompilerParams(vmem_limit_bytes=limit),
    )(*ins)


def iota(shape, dim):
    return lax.broadcasted_iota(jnp.int32, shape, dim)


def ends(axis):
    i = lax.axis_index(axis)
    return i == 0, i == lax.axis_size(axis) - 1


def exchange(msgs, axis):
    n = lax.axis_size(axis)
    if n == 2:
        return [lax.ppermute(msgs[0], axis, [(0, 1), (1, 0)])]
    down = lax.ppermute(msgs[0], axis, [(i + 1, i) for i in range(n - 1)])
    up = lax.ppermute(msgs[1], axis, [(i, i + 1) for i in range(n - 1)])
    return [down, up]


def emit(outs, index, axis, low, high):
    if len(outs) == 1:
        outs[0][index] = jnp.where(ends(axis)[0], high(), low())
    else:
        outs[0][index] = low()
        outs[1][index] = high()


def arrived(refs, index, axis):
    if len(refs) == 1:
        value = refs[0][index]
        first = ends(axis)[0]
        zero = jnp.zeros_like(value)
        return jnp.where(first, value, zero), jnp.where(first, zero, value)
    return refs[0][index], refs[1][index]


def count(axis):
    return 1 if lax.axis_size(axis) == 2 else 2


def turn(value, lanes):
    return pltpu.roll(value, lanes % LANES, 1)


def build_body(start, right, se, re):
    nx, ny, nz = start.shape
    ye = ny + 2 * O

    def plane(p, _):
        for t in range(nz // LANES):
            at = (p + O) * ye + O
            se[t, pl.ds(at, ny), :] = start[p, :, t * LANES:(t + 1) * LANES]
            re[t, pl.ds(at, ny), :] = right[p, :, t * LANES:(t + 1) * LANES]
        return 0

    lax.fori_loop(0, nx, plane, 0, unroll=4)


def xhalo_body(nx, ny, nz, nin, *refs):
    halo = refs[:nin]
    se, re, outs = refs[nin + 2], refs[nin + 3], refs[nin + 4:]
    xe, ye = nx + 2 * O, ny + 2 * O
    nt = nz // LANES
    for t in range(nt):
        cut = slice(t * LANES, (t + 1) * LANES)
        for k in range(SLOT):
            high, low = arrived(halo, (k, slice(None), cut), "gx")
            dst, size, j = (se, F, k) if k < F else (re, G, k - F)
            dst[t, pl.ds((O + nx + j) * ye + O, ny), :] = high
            dst[t, pl.ds((O - size + j) * ye + O, ny), :] = low
    for t in range(nt):
        for k in range(SLOT):
            src, size, j = (se, F, k) if k < F else (re, G, k - F)
            emit(
                outs, (k * nt + t,), "gy",
                lambda: src[t, pl.ds(O + j, xe, stride=ye), :],
                lambda: src[t, pl.ds(O + ny - size + j, xe, stride=ye), :],
            )


def yhalo_body(nx, ny, nz, nin, *refs):
    halo = refs[:nin]
    se, re, outs = refs[nin + 2], refs[nin + 3], refs[nin + 4:]
    xe, ye = nx + 2 * O, ny + 2 * O
    nt = nz // LANES
    for t in range(nt):
        for k in range(SLOT):
            high, low = arrived(halo, (k * nt + t,), "gy")
            dst, size, j = (se, F, k) if k < F else (re, G, k - F)
            dst[t, pl.ds(O + ny + j, xe, stride=ye), :] = high
            dst[t, pl.ds(O - size + j, xe, stride=ye), :] = low
    lane = iota((8, LANES), 1)

    def rows(r, _):
        base = pl.multiple_of(r * 8, 8)
        for group in range(-(-xe // PER)):
            low = jnp.zeros((8, LANES), jnp.float32)
            high = low
            for j in range(min(PER, xe - group * PER)):
                at = j * SLOT
                here = pl.ds((group * PER + j) * ye + base, 8)
                in_s = (lane >= at) & (lane < at + F)
                in_r = (lane >= at + F) & (lane < at + SLOT)
                low = jnp.where(in_s, turn(se[0, here, :], at), low)
                low = jnp.where(in_r, turn(re[0, here, :], at + F), low)
                high = jnp.where(in_s, turn(se[nt - 1, here, :], at + F), high)
                high = jnp.where(in_r, turn(re[nt - 1, here, :], at + SLOT), high)
            emit(outs, (group, pl.ds(base, 8)), "gz", lambda: low, lambda: high)
        return 0

    lax.fori_loop(0, ye // 8, rows, 0)


def inside(shape, dim, offset, cells, axis):
    first, last = ends(axis)
    at = iota(shape, dim) - offset
    up = jnp.where(last, 0.0, 1.0)
    down = jnp.where(first, 0.0, 1.0)
    return jnp.where(at < 0, down, jnp.where(at < cells, 1.0, up))


def fill_mask(mask, ny):
    total, ye, _ = mask.shape
    valid = inside((ye, LANES), 0, O, ny, "gy") * (1.0 / 7.0)
    for t in range(total - 1):
        mask[t] = valid
    first, last = ends("gz")
    lane = iota((ye, LANES), 1)
    mask[total - 1] = valid * jnp.where(
        lane < CH, jnp.where(last, 0.0, 1.0), jnp.where(lane >= LANES - CL, jnp.where(first, 0.0, 1.0), 0.0)
    )


def stencil(ref, ye, base, planes, tiles, use):
    total = ref.shape[0]
    lane = iota((8, LANES), 1)

    def at(p, t, shift=0):
        return ref[t, pl.ds((p + O) * ye + base + shift, 8), :]

    before = [at(planes[0] - 1, t) for t in range(tiles)]
    centre = [at(planes[0], t) for t in range(total)]
    for p in planes:
        after = [at(p + 1, t) for t in range(total)]
        left = [turn(c, 1) for c in centre]
        right = [turn(c, -1) for c in centre]
        for t in range(tiles):
            near = jnp.where(lane == 0, left[t - 1], left[t])
            near = near + jnp.where(lane == LANES - 1, right[(t + 1) % total], right[t])
            near = near + (at(p, t, -1) + at(p, t, 1))
            near = near + (before[t] + after[t])
            use(p, t, centre[t], near)
        before, centre = centre, after


def sweep(src, dst, right, mask, nx, low, high):
    total, ye, _ = mask.shape
    first, last = ends("gx")
    up = jnp.where(last, 0.0, 1.0)
    down = jnp.where(first, 0.0, 1.0)

    def rows(r, _):
        base = pl.multiple_of(r * 8, 8)
        m = [mask[t, pl.ds(base, 8), :] for t in range(total)]

        def use(p, t, centre, near):
            here = pl.ds((p + O) * ye + base, 8)
            factor = m[t] * down if p < 0 else m[t] * up if p >= nx else m[t]
            dst[t, here, :] = factor * (near + (centre + right[t, here, :]))

        stencil(src, ye, base, range(-low, nx + high), total, use)
        return 0

    lax.fori_loop(0, ye // 8, rows, 0)


def split_dot(value, weight):
    high = value.astype(jnp.bfloat16)
    rest = value - high.astype(jnp.float32)
    mid = rest.astype(jnp.bfloat16)
    small = (rest - mid.astype(jnp.float32)).astype(jnp.bfloat16)
    dot = functools.partial(jnp.dot, preferred_element_type=jnp.float32)
    return dot(high, weight) + dot(mid, weight) + dot(small, weight)


def lane_dot(src, src_at, dst, dst_at, rows, weight):
    step = max(s for s in range(8, 273, 8) if rows % s == 0)
    for at in range(0, rows, step):
        value = jnp.concatenate([src[t, pl.ds(src_at + at, step), :] for t in range(weight.shape[0] // LANES)], axis=1)
        got = split_dot(value, weight)
        for t in range(weight.shape[1] // LANES):
            dst[t, pl.ds(dst_at + at, step), :] = got[:, t * LANES:(t + 1) * LANES]


def transfer_weights(fine, coarse, halo, fine_dim, inner, outer):
    shape = (fine, coarse + halo) if fine_dim == 0 else (coarse + halo, fine)
    z = iota(shape, fine_dim)
    k = iota(shape, 1 - fine_dim)
    k = jnp.where(k >= coarse, k - (coarse + halo), k)
    off = z - 2 * k
    weight = jnp.where(off == 1, inner, jnp.where((off == 0) | (off == 2), outer, 0.0))
    return jnp.where(k < -1, 0.0, weight).astype(jnp.bfloat16)


def smooth_body(nx, ny, nz, nin, *refs):
    halo = refs[:nin]
    se, re, s2, coarse = refs[nin + 2:nin + 6]
    outs = refs[nin + 6:-4]
    s1, rx, ry, mask = refs[-4:]
    xe, ye = nx + 2 * O, ny + 2 * O
    nt = nz // LANES
    lane = iota((8, LANES), 1)

    def unpack(r, _):
        base = pl.multiple_of(r * 8, 8)
        for group in range(-(-xe // PER)):
            high, low = arrived(halo, (group, pl.ds(base, 8)), "gz")
            for j in range(min(PER, xe - group * PER)):
                at = j * SLOT
                here = pl.ds((group * PER + j) * ye + base, 8)
                se[nt, here, :] = jnp.where(lane < 64, turn(high, -at), turn(low, -F - at))
                re[nt, here, :] = jnp.where(lane < 64, turn(high, -at - F), turn(low, -G - at - F))
        return 0

    lax.fori_loop(0, ye // 8, unpack, 0)
    fill_mask(mask, ny)
    sweep(se, s1, re, mask, nx, 2, 2)
    sweep(s1, s2, re, mask, nx, 1, 1)

    def restrict_x(r, _):
        base = r * 8 + O
        at = pl.multiple_of(r * 8, 8)
        quarter, half = {}, {}

        def use(p, t, centre, near):
            value = (near + re[t, pl.ds((p + O) * ye + base, 8), :]) - 6.0 * centre
            if p % 2:
                half[t] = 0.5 * value
                if p == nx - 1:
                    rx[t, pl.ds((nx // 2) * ny + at, 8), :] = quarter[t] + half[t]
                return
            value = 0.25 * value
            part = value if p == 0 else (quarter[t] + half[t]) + value
            rx[t, pl.ds((p // 2) * ny + at, 8), :] = part
            quarter[t] = value

        stencil(s2, ye, base, range(nx), nt, use)
        return 0

    lax.fori_loop(0, ny // 8, restrict_x, 0)

    cx, cy, cz = nx // 2, ny // 2, nz // 2
    ct = cz // LANES
    cye = cy + 2 * O
    row = iota((8, LANES), 0)
    zero = jnp.zeros((8, LANES), jnp.float32)
    for t in range(nt):
        rx[t, pl.ds((cx + 1) * ny, 8), :] = zero

    def restrict_y(i, _):
        for t in range(nt):
            for k in range(cy // 8):
                at = i * ny + 16 * k
                even = 0.25 * rx[t, pl.ds(at, 8, stride=2), :]
                odd = 0.5 * rx[t, pl.ds(at + 1, 8, stride=2), :]
                after = 0.25 * rx[t, pl.ds(at + 2, 8, stride=2), :]
                if k == cy // 8 - 1:
                    after = jnp.where(row == 7, 0.0, after)
                if k == 0:
                    ry[t, pl.ds(i * cye, 8), :] = jnp.where(row == O - 1, even[0:1], 0.0)
                    ry[t, pl.ds(i * cye + cy, 8), :] = zero
                ry[t, pl.ds(i * cye + O + 8 * k, 8), :] = (even + odd) + after
        return 0

    lax.fori_loop(0, cx + 1, restrict_y, 0, unroll=3 if cx % 3 == 2 else 1)
    weight = transfer_weights(nz, cz, LANES, 0, 0.5, 0.25)
    lane_dot(ry, 0, coarse, (O - 1) * cye, (cx + 1) * cye, weight)
    for t in range(ct + 1):
        coarse[t, pl.ds((cx + 2 * O - 1) * cye, cye), :] = jnp.zeros((cye, LANES), jnp.float32)
    faces(
        outs, "gx",
        lambda t, j: coarse[t, pl.ds((O - 1 + j) * cye, cye), :],
        lambda t, j: coarse[t, pl.ds((cx + j) * cye, cye), :],
        ct,
    )


def faces(outs, axis, low, high, ct):
    extra_low = extra_high = None
    for j in range(CL):
        for t in range(ct):
            emit(outs, (j * ct + t,), axis, lambda: low(t, j), lambda: high(t, j))
        a = turn(low(ct, j), j + 1)
        b = turn(high(ct, j), j + 1)
        lane = iota(a.shape, 1)
        extra_low = a if j == 0 else jnp.where(lane == j, a, extra_low)
        extra_high = b if j == 0 else jnp.where(lane == j, b, extra_high)
    emit(outs, (CL * ct,), axis, lambda: extra_low, lambda: extra_high)


def place_faces(refs, axis, ct, size, read, write):
    for t in range(ct + 1):
        for j in range(CL):
            if t < ct:
                high, low = arrived(refs, (j * ct + t,), axis)
            else:
                high, low = arrived(refs, (CL * ct,), axis)
                lane = iota(high.shape, 1)
                high = jnp.where(lane == LANES - 1, turn(high, -1 - j), 0.0)
                low = jnp.where(lane == LANES - 1, turn(low, -1 - j), 0.0)
            q = size - 1 + j
            write(t, q, read(t, q) + high if j == 0 else high)
            q = j - CL
            write(t, q, read(t, q) + low if j == CL - 1 else low)


def coarse_x_body(cx, cy, cz, nin, *refs):
    halo = refs[:nin]
    coarse, outs = refs[nin + 1], refs[nin + 2:]
    ct = cz // LANES
    xe, ye = cx + 2 * O, cy + 2 * O

    def read(t, q):
        return coarse[t, pl.ds((q + O) * ye, ye), :]

    def write(t, q, value):
        coarse[t, pl.ds((q + O) * ye, ye), :] = value

    place_faces(halo, "gx", ct, cx, read, write)
    faces(
        outs, "gy",
        lambda t, j: coarse[t, pl.ds(O - 1 + j, xe, stride=ye), :],
        lambda t, j: coarse[t, pl.ds(cy + j, xe, stride=ye), :],
        ct,
    )


def coarse_y_body(cx, cy, cz, nin, *refs):
    halo = refs[:nin]
    coarse, outs = refs[nin + 1], refs[nin + 2:]
    ct = cz // LANES
    xe, ye = cx + 2 * O, cy + 2 * O

    def read(t, q):
        return coarse[t, pl.ds(q + O, xe, stride=ye), :]

    def write(t, q, value):
        coarse[t, pl.ds(q + O, xe, stride=ye), :] = value

    place_faces(halo, "gy", ct, cy, read, write)
    lane = iota((8, LANES), 1)

    def rows(r, _):
        base = pl.multiple_of(r * 8, 8)
        for group in range(-(-xe // CPER)):
            low = jnp.zeros((8, LANES), jnp.float32)
            high = low
            for j in range(min(CPER, xe - group * CPER)):
                at = j * CL
                rows8 = pl.ds((group * CPER + j) * ye + base, 8)
                head = jnp.where(lane < CL - 1, coarse[0, rows8, :], coarse[ct, rows8, :])
                here = (lane >= at) & (lane < at + CL)
                low = jnp.where(here, turn(head, at + 1), low)
                high = jnp.where(here, turn(coarse[ct - 1, rows8, :], at + CL), high)
            emit(outs, (group, pl.ds(base, 8)), "gz", lambda: low, lambda: high)
        return 0

    lax.fori_loop(0, ye // 8, rows, 0)


def finish_body(cx, cy, cz, nin, *refs):
    halo = refs[:nin]
    smooth, _, coarse, out = refs[nin:nin + 4]
    ca, cb, mask, fine, stage, sems = refs[nin + 4:]
    ct = cz // LANES
    xe, ye = cx + 2 * O, cy + 2 * O
    nx, ny, nz = 2 * cx, 2 * cy, 2 * cz
    nt = nz // LANES
    lane = iota((8, LANES), 1)
    first, last = ends("gx")
    up = jnp.where(last, 0.0, 1.0)
    down = jnp.where(first, 0.0, 1.0)
    fill_mask(mask, cy)

    def unpack(r, _):
        base = pl.multiple_of(r * 8, 8)
        m = [mask[t, pl.ds(base, 8), :] for t in range(ct + 1)]
        for group in range(-(-xe // CPER)):
            high, low = arrived(halo, (group, pl.ds(base, 8)), "gz")
            for j in range(min(CPER, xe - group * CPER)):
                q = group * CPER + j
                here = pl.ds(q * ye + base, 8)
                fromhigh = turn(high, -j * CL - 1)
                fromlow = turn(low, -j * CL - CL)
                edge = lane == LANES - 1
                value = [coarse[t, here, :] for t in range(ct + 1)]
                value[ct - 1] = value[ct - 1] + jnp.where(edge, fromhigh, 0.0)
                wing = jnp.where(lane < CH, fromhigh, jnp.where(lane >= LANES - CL, fromlow, 0.0))
                value[ct] = wing + jnp.where(edge, value[ct], 0.0)
                for t in range(ct + 1):
                    factor = m[t] * down if q < O else m[t] * up if q >= O + cx else m[t]
                    scaled = 4.0 * value[t]
                    coarse[t, here, :] = scaled
                    ca[t, here, :] = factor * scaled
        return 0

    lax.fori_loop(0, ye // 8, unpack, 0)
    sweep(ca, cb, coarse, mask, cx, 3, 2)
    sweep(cb, ca, coarse, mask, cx, 2, 1)
    sweep(ca, cb, coarse, mask, cx, 1, 0)
    lane_dot(cb, (O - 1) * ye, fine, 0, (cx + 1) * ye, transfer_weights(nz, cz, LANES, 1, 1.0, 0.5))

    chunks = sems.shape[0]
    per = cx // chunks
    fye = ny + 2 * O
    flat = stage.reshape(nt, nx * ny, LANES)

    def send(c, t):
        at = c * 2 * per
        cut = pl.ds(t * LANES, LANES)
        return pltpu.make_async_copy(
            stage.at[t, pl.ds(at, 2 * per)], out.at[pl.ds(at, 2 * per), :, cut], sems.at[c, t]
        )

    def add(i, _):
        for t in range(nt):
            for k in range(cy // 8):
                at = (i + 1) * ye + O + 8 * k
                here = fine[t, pl.ds(at, 8), :]
                mid = 0.5 * (here + fine[t, pl.ds(at - 1, 8), :])
                before = fine[t, pl.ds(at - ye, 8), :]
                before_mid = 0.5 * (before + fine[t, pl.ds(at - ye - 1, 8), :])
                parts = (0.5 * (before_mid + mid), 0.5 * (before + here), mid, here)
                for n, part in enumerate(parts):
                    src = (2 * i + n // 2 + O) * fye + O + 16 * k + n % 2
                    dst = (2 * i + n // 2) * ny + 16 * k + n % 2
                    flat[t, pl.ds(dst, 8, stride=2), :] = smooth[t, pl.ds(src, 8, stride=2), :] + part
        return 0

    for c in range(chunks):
        lax.fori_loop(c * per, (c + 1) * per, add, 0)
        for t in range(nt):
            send(c, t).start()
    for c in range(chunks):
        for t in range(nt):
            send(c, t).wait()


def on_device(start, right):
    nx, ny, nz = start.shape
    nt = nz // LANES
    xe, ye = nx + 2 * O, ny + 2 * O
    cx, cy, cz = nx // 2, ny // 2, nz // 2
    ct = cz // LANES
    cxe, cye = cx + 2 * O, cy + 2 * O
    big = f32(nt + 1, xe * ye, LANES)
    mb = 1 << 20

    to_prev = jnp.concatenate([start[:F], right[:G]], axis=0)
    to_next = jnp.concatenate([start[nx - F:], right[nx - G:]], axis=0)
    if count("gx") == 1:
        to_prev = jnp.where(ends("gx")[0], to_next, to_prev)
    halo = exchange([to_prev, to_next], "gx")
    se, re = call(build_body, "build", [start, right], [big, big], limit=8 * mb)

    n = len(halo)
    se, re, *msgs = call(
        functools.partial(xhalo_body, nx, ny, nz, n), "xhalo", [*halo, se, re],
        [big, big] + [f32(SLOT * nt, xe, LANES)] * count("gy"), alias={n: 0, n + 1: 1}, limit=8 * mb,
    )
    halo = exchange(msgs, "gy")
    n = len(halo)
    se, re, *msgs = call(
        functools.partial(yhalo_body, nx, ny, nz, n), "yhalo", [*halo, se, re],
        [big, big] + [f32(-(-xe // PER), ye, LANES)] * count("gz"), alias={n: 0, n + 1: 1}, limit=8 * mb,
    )
    halo = exchange(msgs, "gz")
    n = len(halo)
    small = f32(ct + 1, cxe * cye, LANES)
    se, re, s2, coarse, *msgs = call(
        functools.partial(smooth_body, nx, ny, nz, n), "smooth", [*halo, se, re],
        [big, big, big, small] + [f32(CL * ct + 1, cye, LANES)] * count("gx"),
        scratch=[
            pltpu.VMEM((nt + 1, xe * ye, LANES), jnp.float32),
            pltpu.VMEM((nt, (cx + 1) * ny + 8, LANES), jnp.float32),
            pltpu.VMEM((nt, (cx + 1) * cye, LANES), jnp.float32),
            pltpu.VMEM((nt + 1, ye, LANES), jnp.float32),
        ],
        alias={n: 0, n + 1: 1}, limit=24 * mb,
    )
    halo = exchange(msgs, "gx")
    n = len(halo)
    coarse, *msgs = call(
        functools.partial(coarse_x_body, cx, cy, cz, n), "coarse_x", [*halo, coarse],
        [small] + [f32(CL * ct + 1, cxe, LANES)] * count("gy"), alias={n: 0}, limit=8 * mb,
    )
    halo = exchange(msgs, "gy")
    n = len(halo)
    coarse, *msgs = call(
        functools.partial(coarse_y_body, cx, cy, cz, n), "coarse_y", [*halo, coarse],
        [small] + [f32(-(-cxe // CPER), cye, LANES)] * count("gz"), alias={n: 0}, limit=8 * mb,
    )
    halo = exchange(msgs, "gz")
    n = len(halo)
    _, out = call(
        functools.partial(finish_body, cx, cy, cz, n), "finish", [*halo, s2, coarse],
        [small, f32(nx, ny, nz)],
        scratch=[
            pltpu.VMEM((ct + 1, cxe * cye, LANES), jnp.float32),
            pltpu.VMEM((ct + 1, cxe * cye, LANES), jnp.float32),
            pltpu.VMEM((ct + 1, cye, LANES), jnp.float32),
            pltpu.VMEM((nt, (cx + 1) * cye, LANES), jnp.float32),
            pltpu.VMEM((nt, nx, ny, LANES), jnp.float32),
            pltpu.SemaphoreType.DMA((8, nt)),
        ],
        alias={n + 1: 0}, limit=24 * mb, out_specs=[VMEM, ANY],
    )
    return out


def solution(mesh):
    spec = P("gx", "gy", "gz")
    return jax.shard_map(on_device, mesh=mesh, in_specs=(spec, spec), out_specs=spec, check_vma=False)
```

```python
import functools

import jax
import jax.numpy as jnp
from jax import lax
from jax.experimental import pallas as pl
from jax.experimental.pallas import tpu as pltpu
from jax.sharding import PartitionSpec as P

LANES = 128
O = 4
F = 3
G = 2
SLOT = F + G
PER = LANES // SLOT
CL = 4
CH = 3
CPER = LANES // CL

VMEM = pl.BlockSpec(memory_space=pltpu.VMEM)
ANY = pl.BlockSpec(memory_space=pl.ANY)


def f32(*shape):
    return jax.ShapeDtypeStruct(shape, jnp.float32)


def call(body, name, ins, outs, scratch=(), alias=None, limit=None, out_specs=None, cost=1e8):
    return pl.pallas_call(
        body,
        name=name,
        in_specs=[VMEM] * len(ins),
        out_specs=[VMEM] * len(outs) if out_specs is None else out_specs,
        out_shape=outs,
        scratch_shapes=list(scratch),
        input_output_aliases=alias or {},
        cost_estimate=pl.CostEstimate(flops=int(cost), bytes_accessed=0, transcendentals=0),
        compiler_params=pltpu.CompilerParams(vmem_limit_bytes=limit),
    )(*ins)


def iota(shape, dim):
    return lax.broadcasted_iota(jnp.int32, shape, dim)


def ends(axis):
    i = lax.axis_index(axis)
    return i == 0, i == lax.axis_size(axis) - 1


def paired(axis):
    return axis != "gx"


def exchange(msgs, axis):
    n = lax.axis_size(axis)
    if not paired(axis):
        down = lax.ppermute(msgs[0], axis, [(i, (i - 1) % n) for i in range(n)])
        up = lax.ppermute(msgs[1], axis, [(i, (i + 1) % n) for i in range(n)])
        return [down, up]
    found = [None] * len(msgs)
    for phase in reversed(range(len(msgs))):
        routes = []
        for i in range(phase, n - 1, 2):
            routes += [(i, i + 1), (i + 1, i)]
        found[phase] = lax.ppermute(msgs[phase], axis, routes)
    return found


def emit(outs, index, axis, low, high):
    if paired(axis):
        even = lax.axis_index(axis) % 2 == 0
        low, high = low(), high()
        outs[0][index] = jnp.where(even, high, low)
        if len(outs) > 1:
            outs[1][index] = jnp.where(even, low, high)
    else:
        outs[0][index] = low()
        outs[1][index] = high()


def arrived(refs, index, axis):
    a = refs[0][index]
    b = refs[1][index] if len(refs) > 1 else jnp.zeros_like(a)
    if paired(axis):
        even = lax.axis_index(axis) % 2 == 0
        return jnp.where(even, a, b), jnp.where(even, b, a)
    first, last = ends(axis)
    return jnp.where(last, 0.0, a), jnp.where(first, 0.0, b)


def written(outs, index, axis):
    a = outs[0][index]
    b = outs[1][index] if len(outs) > 1 else jnp.zeros_like(a)
    if paired(axis):
        even = lax.axis_index(axis) % 2 == 0
        return jnp.where(even, a, b), jnp.where(even, b, a)
    return b, a


def count(axis):
    return 1 if paired(axis) and lax.axis_size(axis) == 2 else 2


def turn(value, lanes):
    return pltpu.roll(value, lanes % LANES, 1)


def pack(outs, se, re, row, at_row, group, planes, ye, partial):
    lane = iota((8, LANES), 1)
    nt = se.shape[0] - 1
    low, high = partial
    for q in planes:
        at = (q - group * PER) * SLOT
        here = pl.ds(q * ye + row, 8)
        one = turn(jnp.where(lane < 64, se[0, here, :], re[nt - 1, here, :]), at + G)
        two = turn(jnp.where(lane < 64, re[0, here, :], se[nt - 1, here, :]), at)
        low = jnp.where((lane >= at + G) & (lane < at + SLOT), one, low)
        low = jnp.where((lane >= at) & (lane < at + G), two, low)
        back = (lane - (at - F)) % LANES
        high = jnp.where(back < F, two, high)
        high = jnp.where((back >= F) & (back < SLOT), one, high)
    emit(outs, (group, pl.ds(at_row, 8)), "gz", lambda: low, lambda: high)


def build_body(start, right, se, re, *outs):
    nx, ny, nz = start.shape
    xe, ye = nx + 2 * O, ny + 2 * O

    def plane(p, _):
        for t in range(nz // LANES):
            at = (p + O) * ye + O
            se[t, pl.ds(at, ny), :] = start[p, :, t * LANES:(t + 1) * LANES]
            re[t, pl.ds(at, ny), :] = right[p, :, t * LANES:(t + 1) * LANES]
        return 0

    lax.fori_loop(0, nx, plane, 0, unroll=4)

    def rows(r, _):
        at = pl.multiple_of(r * 8, 8)
        zero = jnp.zeros((8, LANES), jnp.float32)
        for group in range(-(-xe // PER)):
            planes = range(max(O, group * PER), min(O + nx, (group + 1) * PER))
            pack(outs, se, re, at + O, at, group, planes, ye, (zero, zero))
        return 0

    lax.fori_loop(0, ny // 8, rows, 0)


def xhalo_body(nx, ny, nz, nin, *refs):
    halo = refs[:nin]
    outs = refs[nin + 2 + count("gz"):]
    se, re, outs = outs[0], outs[1], outs[2:]
    xe, ye = nx + 2 * O, ny + 2 * O
    nt = nz // LANES
    for t in range(nt):
        cut = slice(t * LANES, (t + 1) * LANES)
        for k in range(SLOT):
            high, low = arrived(halo, (k, slice(None), cut), "gx")
            dst, size, j = (se, F, k) if k < F else (re, G, k - F)
            dst[t, pl.ds((O + nx + j) * ye + O, ny), :] = high
            dst[t, pl.ds((O - size + j) * ye + O, ny), :] = low

    def rows(r, _):
        at = pl.multiple_of(r * 8, 8)
        for group in range(-(-xe // PER)):
            span = range(group * PER, min(xe, (group + 1) * PER))
            planes = [q for q in span if O - F <= q < O or O + nx <= q < O + nx + F]
            if planes:
                high, low = written(outs, (group, pl.ds(at, 8)), "gz")
                pack(outs, se, re, at + O, at, group, planes, ye, (low, high))
        return 0

    lax.fori_loop(0, ny // 8, rows, 0)


def zhalo_body(nx, ny, nz, nin, *refs):
    halo = refs[:nin]
    se, re, outs = refs[nin + 2], refs[nin + 3], refs[nin + 4:]
    xe, ye = nx + 2 * O, ny + 2 * O
    nt = nz // LANES
    lane = iota((8, LANES), 1)

    def unpack(r, _):
        at_row = pl.multiple_of(r * 8, 8)
        for group in range(-(-xe // PER)):
            high, low = arrived(halo, (group, pl.ds(at_row, 8)), "gz")
            pick = lane % SLOT < G
            one = jnp.where(pick, high, low)
            two = jnp.where(pick, low, high)
            one = jnp.where(lane >= LANES - F, low, one)
            for j in range(min(PER, xe - group * PER)):
                a = turn(one, -j * SLOT)
                b = turn(two, -j * SLOT - G)
                here = pl.ds((group * PER + j) * ye + at_row + O, 8)
                se[nt, here, :] = jnp.where(lane < 64, b, a)
                re[nt, here, :] = jnp.where(lane < 64, a, b)
        return 0

    lax.fori_loop(0, ny // 8, unpack, 0)
    lane = iota((xe, LANES), 1)
    extra_low = extra_high = jnp.zeros((xe, LANES), jnp.float32)
    for k in range(SLOT):
        src, size, j = (se, F, k) if k < F else (re, G, k - F)
        for t in range(nt + 1):
            low = src[t, pl.ds(O + j, xe, stride=ye), :]
            high = src[t, pl.ds(O + ny - size + j, xe, stride=ye), :]
            if t < nt:
                emit(outs, (k * nt + t,), "gy", lambda: low, lambda: high)
            else:
                here = (lane >= 8 * k) & (lane < 8 * k + 2 * F)
                extra_low = jnp.where(here, turn(low, 8 * k + F), extra_low)
                extra_high = jnp.where(here, turn(high, 8 * k + F), extra_high)
    emit(outs, (SLOT * nt,), "gy", lambda: extra_low, lambda: extra_high)


def place_y(halo, se, re, nx, ny):
    xe, ye = nx + 2 * O, ny + 2 * O
    nt = se.shape[0] - 1
    for k in range(SLOT):
        dst, size, j = (se, F, k) if k < F else (re, G, k - F)
        for t in range(nt + 1):
            if t < nt:
                high, low = arrived(halo, (k * nt + t,), "gy")
            else:
                high, low = (turn(v, -8 * k - F) for v in arrived(halo, (SLOT * nt,), "gy"))
            dst[t, pl.ds(O + ny + j, xe, stride=ye), :] = high
            dst[t, pl.ds(O - size + j, xe, stride=ye), :] = low


def inside(shape, dim, offset, cells, axis):
    first, last = ends(axis)
    at = iota(shape, dim) - offset
    up = jnp.where(last, 0.0, 1.0)
    down = jnp.where(first, 0.0, 1.0)
    return jnp.where(at < 0, down, jnp.where(at < cells, 1.0, up))


def fill_mask(mask, ny):
    total, ye, _ = mask.shape
    valid = inside((ye, LANES), 0, O, ny, "gy") * (1.0 / 7.0)
    for t in range(total - 1):
        mask[t] = valid
    first, last = ends("gz")
    lane = iota((ye, LANES), 1)
    mask[total - 1] = valid * jnp.where(
        lane < CH, jnp.where(last, 0.0, 1.0), jnp.where(lane >= LANES - CL, jnp.where(first, 0.0, 1.0), 0.0)
    )


def stencil(ref, ye, base, planes, tiles, use):
    total = ref.shape[0]
    lane = iota((8, LANES), 1)

    def at(p, t, shift=0):
        return ref[t, pl.ds((p + O) * ye + base + shift, 8), :]

    before = [at(planes[0] - 1, t) for t in range(tiles)]
    centre = [at(planes[0], t) for t in range(total)]
    for p in planes:
        after = [at(p + 1, t) for t in range(total)]
        for t in range(tiles):
            wrapped = jnp.where(lane == LANES - 1, centre[t - 1], centre[t])
            near = turn(wrapped, 1)
            wrapped = jnp.where(lane == 0, centre[(t + 1) % total], centre[t])
            near = near + turn(wrapped, -1)
            near = near + (at(p, t, -1) + at(p, t, 1))
            near = near + (before[t] + after[t])
            use(p, t, centre[t], near)
        before, centre = centre, after


def sweep(src, dst, right, mask, nx, low, high, tiles):
    total, ye, _ = mask.shape
    first, last = ends("gx")
    up = jnp.where(last, 0.0, 1.0)
    down = jnp.where(first, 0.0, 1.0)

    def rows(r, _):
        base = tiles[1](r)
        m = [mask[t, pl.ds(base, 8), :] for t in range(total)]

        def use(p, t, centre, near):
            here = pl.ds((p + O) * ye + base, 8)
            factor = m[t] * down if p < 0 else m[t] * up if p >= nx else m[t]
            dst[t, here, :] = factor * (near + (centre + right[t, here, :]))

        stencil(src, ye, base, range(-low, nx + high), total, use)
        return 0

    lax.fori_loop(0, tiles[0], rows, 0)


def residual_x(s2, re, rx, nx, ny, tiles):
    ye = ny + 2 * O

    def rows(r, _):
        base = tiles[1](r)
        at = base - O
        quarter, half = {}, {}

        def use(p, t, centre, near):
            value = (near + re[t, pl.ds((p + O) * ye + base, 8), :]) - 6.0 * centre
            if p % 2:
                half[t] = 0.5 * value
                if p == nx - 1:
                    rx[t, pl.ds((nx // 2) * ny + at, 8), :] = quarter[t] + half[t]
                return
            value = 0.25 * value
            part = value if p == 0 else (quarter[t] + half[t]) + value
            rx[t, pl.ds((p // 2) * ny + at, 8), :] = part
            quarter[t] = value

        stencil(s2, ye, base, range(nx), rx.shape[0], use)
        return 0

    lax.fori_loop(0, tiles[0], rows, 0)


def every(ye):
    return ye // 8, lambda r: pl.multiple_of(r * 8, 8)


def split_dot(value, weight):
    high = value.astype(jnp.bfloat16)
    rest = value - high.astype(jnp.float32)
    mid = rest.astype(jnp.bfloat16)
    small = (rest - mid.astype(jnp.float32)).astype(jnp.bfloat16)
    dot = functools.partial(jnp.dot, preferred_element_type=jnp.float32)
    return dot(high, weight) + dot(mid, weight) + dot(small, weight)


def lane_dot(src, src_at, dst, dst_at, rows, weight):
    step = max(s for s in range(8, 273, 8) if rows % s == 0)
    for at in range(0, rows, step):
        value = jnp.concatenate([src[t, pl.ds(src_at + at, step), :] for t in range(weight.shape[0] // LANES)], axis=1)
        got = split_dot(value, weight)
        for t in range(weight.shape[1] // LANES):
            dst[t, pl.ds(dst_at + at, step), :] = got[:, t * LANES:(t + 1) * LANES]


def transfer_weights(fine, coarse, halo, fine_dim, inner, outer):
    shape = (fine, coarse + halo) if fine_dim == 0 else (coarse + halo, fine)
    z = iota(shape, fine_dim)
    k = iota(shape, 1 - fine_dim)
    k = jnp.where(k >= coarse, k - (coarse + halo), k)
    off = z - 2 * k
    weight = jnp.where(off == 1, inner, jnp.where((off == 0) | (off == 2), outer, 0.0))
    return jnp.where(k < -1, 0.0, weight).astype(jnp.bfloat16)


def inner_body(nx, ny, nz, se, re, s1, s2, rx, mask):
    fill_mask(mask, ny)
    many = ny // 8 - 1
    sweep(se, s1, re, mask, nx, 2, 2, (many, lambda r: pl.multiple_of(r * 8 + 8, 8)))
    sweep(s1, s2, re, mask, nx, 1, 1, (many, lambda r: jnp.minimum(r * 8 + 9, ny - 9)))
    residual_x(s2, re, rx, nx, ny, (many, lambda r: O + jnp.minimum(r * 8 + 6, ny - 14)))


def outer_body(nx, ny, nz, nin, *refs):
    halo = refs[:nin]
    se, re, s1, s2, rx, coarse = refs[nin + 5:nin + 11]
    outs = refs[nin + 11:-2]
    ry, mask = refs[-2:]
    nt = nz // LANES
    place_y(halo, se, re, nx, ny)
    fill_mask(mask, ny)
    sweep(se, s1, re, mask, nx, 2, 2, (2, lambda r: pl.multiple_of(r * ny, 8)))
    sweep(s1, s2, re, mask, nx, 1, 1, (2, lambda r: r * (ny - 2) + 1))
    residual_x(s2, re, rx, nx, ny, (2, lambda r: O + r * (ny - 8)))

    cx, cy, cz = nx // 2, ny // 2, nz // 2
    ct = cz // LANES
    cye = cy + 2 * O
    row = iota((8, LANES), 0)
    zero = jnp.zeros((8, LANES), jnp.float32)
    for t in range(nt):
        rx[t, pl.ds((cx + 1) * ny, 8), :] = zero

    def restrict_y(i, _):
        for t in range(nt):
            for k in range(cy // 8):
                at = i * ny + 16 * k
                even = 0.25 * rx[t, pl.ds(at, 8, stride=2), :]
                odd = 0.5 * rx[t, pl.ds(at + 1, 8, stride=2), :]
                after = 0.25 * rx[t, pl.ds(at + 2, 8, stride=2), :]
                if k == cy // 8 - 1:
                    after = jnp.where(row == 7, 0.0, after)
                if k == 0:
                    ry[t, pl.ds(i * cye, 8), :] = jnp.where(row == O - 1, even[0:1], 0.0)
                    ry[t, pl.ds(i * cye + cy, 8), :] = zero
                ry[t, pl.ds(i * cye + O + 8 * k, 8), :] = (even + odd) + after
        return 0

    lax.fori_loop(0, cx + 1, restrict_y, 0, unroll=3 if cx % 3 == 2 else 1)
    weight = transfer_weights(nz, cz, LANES, 0, 0.5, 0.25)
    lane_dot(ry, 0, coarse, (O - 1) * cye, (cx + 1) * cye, weight)
    for t in range(ct + 1):
        coarse[t, pl.ds((cx + 2 * O - 1) * cye, cye), :] = jnp.zeros((cye, LANES), jnp.float32)
    faces(
        outs, "gx",
        lambda t, j: coarse[t, pl.ds((O - 1 + j) * cye, cye), :],
        lambda t, j: coarse[t, pl.ds((cx + j) * cye, cye), :],
        ct,
    )


def faces(outs, axis, low, high, ct):
    extra_low = extra_high = None
    for j in range(CL):
        for t in range(ct):
            emit(outs, (j * ct + t,), axis, lambda: low(t, j), lambda: high(t, j))
        a = turn(low(ct, j), j + 1)
        b = turn(high(ct, j), j + 1)
        lane = iota(a.shape, 1)
        extra_low = a if j == 0 else jnp.where(lane == j, a, extra_low)
        extra_high = b if j == 0 else jnp.where(lane == j, b, extra_high)
    emit(outs, (CL * ct,), axis, lambda: extra_low, lambda: extra_high)


def place_faces(refs, axis, ct, size, read, write):
    for t in range(ct + 1):
        for j in range(CL):
            if t < ct:
                high, low = arrived(refs, (j * ct + t,), axis)
            else:
                high, low = arrived(refs, (CL * ct,), axis)
                lane = iota(high.shape, 1)
                high = jnp.where(lane == LANES - 1, turn(high, -1 - j), 0.0)
                low = jnp.where(lane == LANES - 1, turn(low, -1 - j), 0.0)
            q = size - 1 + j
            write(t, q, read(t, q) + high if j == 0 else high)
            q = j - CL
            write(t, q, read(t, q) + low if j == CL - 1 else low)


def coarse_x_body(cx, cy, cz, nin, *refs):
    halo = refs[:nin]
    coarse, outs = refs[nin + 1], refs[nin + 2:]
    ct = cz // LANES
    xe, ye = cx + 2 * O, cy + 2 * O

    def read(t, q):
        return coarse[t, pl.ds((q + O) * ye, ye), :]

    def write(t, q, value):
        coarse[t, pl.ds((q + O) * ye, ye), :] = value

    place_faces(halo, "gx", ct, cx, read, write)
    faces(
        outs, "gy",
        lambda t, j: coarse[t, pl.ds(O - 1 + j, xe, stride=ye), :],
        lambda t, j: coarse[t, pl.ds(cy + j, xe, stride=ye), :],
        ct,
    )


def coarse_y_body(cx, cy, cz, nin, *refs):
    halo = refs[:nin]
    coarse, outs = refs[nin + 1], refs[nin + 2:]
    ct = cz // LANES
    xe, ye = cx + 2 * O, cy + 2 * O

    def read(t, q):
        return coarse[t, pl.ds(q + O, xe, stride=ye), :]

    def write(t, q, value):
        coarse[t, pl.ds(q + O, xe, stride=ye), :] = value

    place_faces(halo, "gy", ct, cy, read, write)
    lane = iota((8, LANES), 1)

    def rows(r, _):
        base = pl.multiple_of(r * 8, 8)
        for group in range(-(-xe // CPER)):
            low = jnp.zeros((8, LANES), jnp.float32)
            high = low
            for j in range(min(CPER, xe - group * CPER)):
                at = j * CL
                rows8 = pl.ds((group * CPER + j) * ye + base, 8)
                head = jnp.where(lane < CL - 1, coarse[0, rows8, :], coarse[ct, rows8, :])
                here = (lane >= at) & (lane < at + CL)
                low = jnp.where(here, turn(head, at + 1), low)
                high = jnp.where(here, turn(coarse[ct - 1, rows8, :], at + CL), high)
            emit(outs, (group, pl.ds(base, 8)), "gz", lambda: low, lambda: high)
        return 0

    lax.fori_loop(0, ye // 8, rows, 0)


def finish_body(cx, cy, cz, nin, *refs):
    halo = refs[:nin]
    smooth, _, coarse, out = refs[nin:nin + 4]
    ca, cb, mask, fine, stage, sems = refs[nin + 4:]
    ct = cz // LANES
    xe, ye = cx + 2 * O, cy + 2 * O
    nx, ny, nz = 2 * cx, 2 * cy, 2 * cz
    nt = nz // LANES
    lane = iota((8, LANES), 1)
    first, last = ends("gx")
    up = jnp.where(last, 0.0, 1.0)
    down = jnp.where(first, 0.0, 1.0)
    fill_mask(mask, cy)

    def unpack(r, _):
        base = pl.multiple_of(r * 8, 8)
        m = [mask[t, pl.ds(base, 8), :] for t in range(ct + 1)]
        for group in range(-(-xe // CPER)):
            high, low = arrived(halo, (group, pl.ds(base, 8)), "gz")
            for j in range(min(CPER, xe - group * CPER)):
                q = group * CPER + j
                here = pl.ds(q * ye + base, 8)
                fromhigh = turn(high, -j * CL - 1)
                fromlow = turn(low, -j * CL - CL)
                edge = lane == LANES - 1
                value = [coarse[t, here, :] for t in range(ct + 1)]
                value[ct - 1] = value[ct - 1] + jnp.where(edge, fromhigh, 0.0)
                wing = jnp.where(lane < CH, fromhigh, jnp.where(lane >= LANES - CL, fromlow, 0.0))
                value[ct] = wing + jnp.where(edge, value[ct], 0.0)
                for t in range(ct + 1):
                    factor = m[t] * down if q < O else m[t] * up if q >= O + cx else m[t]
                    scaled = 4.0 * value[t]
                    coarse[t, here, :] = scaled
                    ca[t, here, :] = factor * scaled
        return 0

    lax.fori_loop(0, ye // 8, unpack, 0)
    sweep(ca, cb, coarse, mask, cx, 3, 2, every(ye))
    sweep(cb, ca, coarse, mask, cx, 2, 1, every(ye))
    sweep(ca, cb, coarse, mask, cx, 1, 0, every(ye))
    lane_dot(cb, (O - 1) * ye, fine, 0, (cx + 1) * ye, transfer_weights(nz, cz, LANES, 1, 1.0, 0.5))

    chunks = sems.shape[0]
    per = cx // chunks
    fye = ny + 2 * O
    flat = stage.reshape(nt, nx * ny, LANES)

    def send(c, t):
        at = c * 2 * per
        cut = pl.ds(t * LANES, LANES)
        return pltpu.make_async_copy(
            stage.at[t, pl.ds(at, 2 * per)], out.at[pl.ds(at, 2 * per), :, cut], sems.at[c, t]
        )

    def add(i, _):
        for t in range(nt):
            for k in range(cy // 8):
                at = (i + 1) * ye + O + 8 * k
                here = fine[t, pl.ds(at, 8), :]
                mid = 0.5 * (here + fine[t, pl.ds(at - 1, 8), :])
                before = fine[t, pl.ds(at - ye, 8), :]
                before_mid = 0.5 * (before + fine[t, pl.ds(at - ye - 1, 8), :])
                parts = (0.5 * (before_mid + mid), 0.5 * (before + here), mid, here)
                for n, part in enumerate(parts):
                    src = (2 * i + n // 2 + O) * fye + O + 16 * k + n % 2
                    dst = (2 * i + n // 2) * ny + 16 * k + n % 2
                    flat[t, pl.ds(dst, 8, stride=2), :] = smooth[t, pl.ds(src, 8, stride=2), :] + part
        return 0

    for c in range(chunks):
        lax.fori_loop(c * per, (c + 1) * per, add, 0)
        for t in range(nt):
            send(c, t).start()
    for c in range(chunks):
        for t in range(nt):
            send(c, t).wait()


def on_device(start, right):
    nx, ny, nz = start.shape
    nt = nz // LANES
    xe, ye = nx + 2 * O, ny + 2 * O
    cx, cy, cz = nx // 2, ny // 2, nz // 2
    ct = cz // LANES
    cxe, cye = cx + 2 * O, cy + 2 * O
    big = f32(nt + 1, xe * ye, LANES)
    mb = 1 << 20

    to_prev = jnp.concatenate([start[:F], right[:G]], axis=0)
    to_next = jnp.concatenate([start[nx - F:], right[nx - G:]], axis=0)
    halo = exchange([to_prev, to_next], "gx")
    face = [f32(-(-xe // PER), ny, LANES)] * count("gz")
    se, re, *msgs = call(build_body, "build", [start, right], [big, big] + face, limit=8 * mb)

    n = len(halo)
    alias = {n + i: i for i in range(2 + len(msgs))}
    se, re, *msgs = call(
        functools.partial(xhalo_body, nx, ny, nz, n), "xhalo", [*halo, se, re, *msgs],
        [big, big] + face, alias=alias, limit=8 * mb,
    )
    halo = exchange(msgs, "gz")
    n = len(halo)
    se, re, *msgs = call(
        functools.partial(zhalo_body, nx, ny, nz, n), "zhalo", [*halo, se, re],
        [big, big] + [f32(SLOT * nt + 1, xe, LANES)] * count("gy"), alias={n: 0, n + 1: 1}, limit=8 * mb,
    )
    halo = exchange(msgs, "gy")
    part = f32(nt, (cx + 1) * ny + 8, LANES)
    masks = pltpu.VMEM((nt + 1, ye, LANES), jnp.float32)
    s1, s2, rx = call(
        functools.partial(inner_body, nx, ny, nz), "inner", [se, re], [big, big, part], scratch=[masks],
        limit=8 * mb, cost=9e9,
    )
    n = len(halo)
    small = f32(ct + 1, cxe * cye, LANES)
    se, re, s1, s2, rx, coarse, *msgs = call(
        functools.partial(outer_body, nx, ny, nz, n), "outer", [*halo, se, re, s1, s2, rx],
        [big, big, big, big, part, small] + [f32(CL * ct + 1, cye, LANES)] * count("gx"),
        scratch=[pltpu.VMEM((nt, (cx + 1) * cye, LANES), jnp.float32), masks],
        alias={n + i: i for i in range(5)}, limit=8 * mb,
    )
    halo = exchange(msgs, "gx")
    n = len(halo)
    coarse, *msgs = call(
        functools.partial(coarse_x_body, cx, cy, cz, n), "coarse_x", [*halo, coarse],
        [small] + [f32(CL * ct + 1, cxe, LANES)] * count("gy"), alias={n: 0}, limit=8 * mb,
    )
    halo = exchange(msgs, "gy")
    n = len(halo)
    coarse, *msgs = call(
        functools.partial(coarse_y_body, cx, cy, cz, n), "coarse_y", [*halo, coarse],
        [small] + [f32(-(-cxe // CPER), cye, LANES)] * count("gz"), alias={n: 0}, limit=8 * mb,
    )
    halo = exchange(msgs, "gz")
    n = len(halo)
    _, out = call(
        functools.partial(finish_body, cx, cy, cz, n), "finish", [*halo, s2, coarse],
        [small, f32(nx, ny, nz)],
        scratch=[
            pltpu.VMEM((ct + 1, cxe * cye, LANES), jnp.float32),
            pltpu.VMEM((ct + 1, cxe * cye, LANES), jnp.float32),
            pltpu.VMEM((ct + 1, cye, LANES), jnp.float32),
            pltpu.VMEM((nt, (cx + 1) * cye, LANES), jnp.float32),
            pltpu.VMEM((nt, nx, ny, LANES), jnp.float32),
            pltpu.SemaphoreType.DMA((8, nt)),
        ],
        alias={n + 1: 0}, limit=12 * mb, out_specs=[VMEM, ANY],
    )
    return out


def solution(mesh):
    spec = P("gx", "gy", "gz")
    return jax.shard_map(on_device, mesh=mesh, in_specs=(spec, spec), out_specs=spec, check_vma=False)
```

```python
import functools

import jax
import jax.numpy as jnp
from jax import lax
from jax.experimental import pallas as pl
from jax.experimental.pallas import tpu as pltpu
from jax.sharding import PartitionSpec as P

LANES = 128
O = 4
F = 3
G = 2
SLOT = F + G
PER = LANES // SLOT
CL = 4
CH = 3
CPER = LANES // CL

VMEM = pl.BlockSpec(memory_space=pltpu.VMEM)
ANY = pl.BlockSpec(memory_space=pl.ANY)


def f32(*shape):
    return jax.ShapeDtypeStruct(shape, jnp.float32)


def call(body, name, ins, outs, scratch=(), alias=None, limit=None, out_specs=None, cost=1e8,
         in_specs=None):
    return pl.pallas_call(
        body,
        name=name,
        in_specs=[VMEM] * len(ins) if in_specs is None else in_specs,
        out_specs=[VMEM] * len(outs) if out_specs is None else out_specs,
        out_shape=outs,
        scratch_shapes=list(scratch),
        input_output_aliases=alias or {},
        cost_estimate=pl.CostEstimate(flops=int(cost), bytes_accessed=0, transcendentals=0),
        compiler_params=pltpu.CompilerParams(vmem_limit_bytes=limit),
    )(*ins)


def iota(shape, dim):
    return lax.broadcasted_iota(jnp.int32, shape, dim)


RING = "gx/ring"


def size_of(axis):
    return lax.axis_size(axis.split("/")[0])


def ends(axis):
    i = lax.axis_index(axis.split("/")[0])
    return i == 0, i == size_of(axis) - 1


def paired(axis):
    return axis != RING


def exchange(msgs, axis):
    n = size_of(axis)
    if not paired(axis):
        axis = axis.split("/")[0]
        down = lax.ppermute(msgs[0], axis, [(i, (i - 1) % n) for i in range(n)])
        up = lax.ppermute(msgs[1], axis, [(i, (i + 1) % n) for i in range(n)])
        return [down, up]
    found = [None] * len(msgs)
    for phase in reversed(range(len(msgs))):
        routes = []
        for i in range(phase, n - 1, 2):
            routes += [(i, i + 1), (i + 1, i)]
        found[phase] = lax.ppermute(msgs[phase], axis, routes)
    return found


def emit(outs, index, axis, low, high):
    if isinstance(outs, Kept):
        outs.lows.append(low())
        outs.highs.append(high())
    elif paired(axis):
        even = lax.axis_index(axis) % 2 == 0
        low, high = low(), high()
        outs[0][index] = jnp.where(even, high, low)
        if len(outs) > 1:
            outs[1][index] = jnp.where(even, low, high)
    else:
        outs[0][index] = low()
        outs[1][index] = high()


def arrived(refs, index, axis):
    a = refs[0][index]
    b = refs[1][index] if len(refs) > 1 else jnp.zeros_like(a)
    if paired(axis):
        even = lax.axis_index(axis) % 2 == 0
        return jnp.where(even, a, b), jnp.where(even, b, a)
    first, last = ends(axis)
    return jnp.where(last, 0.0, a), jnp.where(first, 0.0, b)


def written(outs, index, axis):
    a = outs[0][index]
    b = outs[1][index] if len(outs) > 1 else jnp.zeros_like(a)
    if paired(axis):
        even = lax.axis_index(axis) % 2 == 0
        return jnp.where(even, a, b), jnp.where(even, b, a)
    return b, a


def count(axis):
    return 1 if paired(axis) and size_of(axis) == 2 else 2


def turn(value, lanes):
    return pltpu.roll(value, lanes % LANES, 1)


def xpack_body(*refs):
    first_s, first_r, last_s, last_r, *outs = refs
    for k in range(SLOT):
        low, high, j = (first_s, last_s, k) if k < F else (first_r, last_r, k - F)
        emit(outs, (k,), "gx", lambda: low[j], lambda: high[j])


def pack(outs, at_row, group, planes, load, partial):
    lane = iota((8, LANES), 1)
    low, high = partial
    done = None
    wrapped = None
    for q in planes:
        at = (q - group * PER) * SLOT
        s_low, s_high, r_low, r_high = load(q)
        one = turn(jnp.where(lane < 64, s_low, r_high), at + G)
        two = turn(jnp.where(lane < 64, r_low, s_high), at)
        start_at = lane >= at
        start_g = lane >= at + G
        if done is not None and done != q - 1:
            raise ValueError("planes")
        low = jnp.where(start_g, one, jnp.where(start_at, two, low))
        if at == 0:
            wrapped = two
            high = jnp.where(start_at, one, high)
        else:
            high = jnp.where(start_at, one, jnp.where(lane >= at - F, two, high))
        done = q
    if wrapped is not None:
        high = jnp.where(lane >= LANES - F, wrapped, high)
    if planes:
        emit(outs, (group, pl.ds(at_row, 8)), "gz", lambda: low, lambda: high)


def build_body(start, right, se, re, *outs):
    nx, ny, nz = start.shape
    xe, ye = nx + 2 * O, ny + 2 * O
    nt = nz // LANES

    def rows(r, _):
        at = pl.multiple_of(r * 8, 8)
        zero = jnp.zeros((8, LANES), jnp.float32)

        def load(q):
            found = {}
            for t in range(nt):
                for key, src, dst in (("s", start, se), ("r", right, re)):
                    value = src[q - O, pl.ds(at, 8), t * LANES:(t + 1) * LANES]
                    dst[t, pl.ds(q * ye + at + O, 8), :] = value
                    found[key, t] = value
            return found["s", 0], found["s", nt - 1], found["r", 0], found["r", nt - 1]

        for group in range(-(-xe // PER)):
            planes = range(max(O, group * PER), min(O + nx, (group + 1) * PER))
            pack(outs, at, group, planes, load, (zero, zero))
        return 0

    lax.fori_loop(0, ny // 8, rows, 0)


def xhalo_body(nx, ny, nz, nin, *refs):
    halo = refs[:nin]
    outs = refs[nin + 2 + count("gz"):]
    se, re, outs = outs[0], outs[1], outs[2:]
    xe, ye = nx + 2 * O, ny + 2 * O
    nt = nz // LANES
    for t in range(nt):
        cut = slice(t * LANES, (t + 1) * LANES)
        for k in range(SLOT):
            high, low = arrived(halo, (k, slice(None), cut), "gx")
            dst, size, j = (se, F, k) if k < F else (re, G, k - F)
            dst[t, pl.ds((O + nx + j) * ye + O, ny), :] = high
            dst[t, pl.ds((O - size + j) * ye + O, ny), :] = low

    lane = iota((8, LANES), 1)

    def rows(r, _):
        at = pl.multiple_of(r * 8, 8)

        def load(q):
            here = pl.ds(q * ye + at + O, 8)
            return se[0, here, :], se[nt - 1, here, :], re[0, here, :], re[nt - 1, here, :]

        for group in range(-(-xe // PER)):
            span = range(group * PER, min(xe, (group + 1) * PER))
            before = [q for q in span if O - F <= q < O]
            after = [q for q in span if O + nx <= q < O + nx + F]
            if not before and not after:
                continue
            core_high, core_low = written(outs, (group, pl.ds(at, 8)), "gz")
            lows, highs = [], []
            pack(Kept(lows, highs), at, group, before, load, (core_low, core_high))
            if before:
                top = (O - group * PER) * SLOT
                low = jnp.where(lane < top, lows[0], core_low)
                high = jnp.where((lane < top - F) | (lane >= LANES - F), highs[0], core_high)
                core_low, core_high = low, high
            if after:
                lows, highs = [], []
                pack(Kept(lows, highs), at, group, after, load, (core_low, core_high))
                core_low, core_high = lows[0], jnp.where(lane >= LANES - F, core_high, highs[0])
            emit(outs, (group, pl.ds(at, 8)), "gz", lambda: core_low, lambda: core_high)
        return 0

    lax.fori_loop(0, ny // 8, rows, 0)


class Kept:
    def __init__(self, lows, highs):
        self.lows, self.highs = lows, highs


def zhalo_body(nx, ny, nz, nin, *refs):
    halo = refs[:nin]
    se, re, outs = refs[nin + 2], refs[nin + 3], refs[nin + 4:]
    xe, ye = nx + 2 * O, ny + 2 * O
    nt = nz // LANES
    lane = iota((8, LANES), 1)

    def unpack(r, _):
        at_row = pl.multiple_of(r * 8, 8)
        for group in range(-(-xe // PER)):
            high, low = arrived(halo, (group, pl.ds(at_row, 8)), "gz")
            pick = lane % SLOT < G
            one = jnp.where(pick, high, low)
            two = jnp.where(pick, low, high)
            one = jnp.where(lane >= LANES - F, low, one)
            for j in range(min(PER, xe - group * PER)):
                a = turn(one, -j * SLOT)
                b = turn(two, -j * SLOT - G)
                here = pl.ds((group * PER + j) * ye + at_row + O, 8)
                se[nt, here, :] = jnp.where(lane < 64, b, a)
                re[nt, here, :] = jnp.where(lane < 64, a, b)
        return 0

    lax.fori_loop(0, ny // 8, unpack, 0)
    lane = iota((xe, LANES), 1)
    extra_low = extra_high = jnp.zeros((xe, LANES), jnp.float32)
    for k in range(SLOT):
        src, size, j = (se, F, k) if k < F else (re, G, k - F)
        for t in range(nt + 1):
            low = src[t, pl.ds(O + j, xe, stride=ye), :]
            high = src[t, pl.ds(O + ny - size + j, xe, stride=ye), :]
            if t < nt:
                emit(outs, (k * nt + t,), "gy", lambda: low, lambda: high)
            else:
                here = (lane >= 8 * k) & (lane < 8 * k + 2 * F)
                extra_low = jnp.where(here, turn(low, 8 * k + F), extra_low)
                extra_high = jnp.where(here, turn(high, 8 * k + F), extra_high)
    emit(outs, (SLOT * nt,), "gy", lambda: extra_low, lambda: extra_high)


def place_y(halo, se, re, nx, ny):
    xe, ye = nx + 2 * O, ny + 2 * O
    nt = se.shape[0] - 1
    for k in range(SLOT):
        dst, size, j = (se, F, k) if k < F else (re, G, k - F)
        for t in range(nt + 1):
            if t < nt:
                high, low = arrived(halo, (k * nt + t,), "gy")
            else:
                high, low = (turn(v, -8 * k - F) for v in arrived(halo, (SLOT * nt,), "gy"))
            dst[t, pl.ds(O + ny + j, xe, stride=ye), :] = high
            dst[t, pl.ds(O - size + j, xe, stride=ye), :] = low


def inside(shape, dim, offset, cells, axis):
    first, last = ends(axis)
    at = iota(shape, dim) - offset
    up = jnp.where(last, 0.0, 1.0)
    down = jnp.where(first, 0.0, 1.0)
    return jnp.where(at < 0, down, jnp.where(at < cells, 1.0, up))


def fill_mask(mask, ny):
    total, ye, _ = mask.shape
    valid = inside((ye, LANES), 0, O, ny, "gy") * (1.0 / 7.0)
    for t in range(total - 1):
        mask[t] = valid
    first, last = ends("gz")
    lane = iota((ye, LANES), 1)
    mask[total - 1] = valid * jnp.where(
        lane < CH, jnp.where(last, 0.0, 1.0), jnp.where(lane >= LANES - CL, jnp.where(first, 0.0, 1.0), 0.0)
    )


def stencil(ref, ye, base, planes, tiles, use):
    total = ref.shape[0]
    lane = iota((8, LANES), 1)

    def at(p, t, shift=0):
        return ref[t, pl.ds((p + O) * ye + base + shift, 8), :]

    before = [at(planes[0] - 1, t) for t in range(tiles)]
    centre = [at(planes[0], t) for t in range(total)]
    for p in planes:
        after = [at(p + 1, t) for t in range(total)]
        for t in range(tiles):
            wrapped = jnp.where(lane == LANES - 1, centre[t - 1], centre[t])
            near = turn(wrapped, 1)
            wrapped = jnp.where(lane == 0, centre[(t + 1) % total], centre[t])
            near = near + turn(wrapped, -1)
            near = near + (at(p, t, -1) + at(p, t, 1))
            near = near + (before[t] + after[t])
            use(p, t, centre[t], near)
        before, centre = centre, after


def sweep(src, dst, right, mask, nx, low, high, tiles):
    total, ye, _ = mask.shape
    first, last = ends("gx")
    up = jnp.where(last, 0.0, 1.0)
    down = jnp.where(first, 0.0, 1.0)

    def rows(r, _):
        base = tiles[1](r)
        m = [mask[t, pl.ds(base, 8), :] for t in range(total)]

        def use(p, t, centre, near):
            here = pl.ds((p + O) * ye + base, 8)
            factor = m[t] * down if p < 0 else m[t] * up if p >= nx else m[t]
            dst[t, here, :] = factor * (near + (centre + right[t, here, :]))

        stencil(src, ye, base, range(-low, nx + high), total, use)
        return 0

    lax.fori_loop(0, tiles[0], rows, 0)


def residual_x(s2, re, rx, nx, ny, tiles):
    ye = ny + 2 * O

    def rows(r, _):
        base = tiles[1](r)
        at = base - O
        quarter, half = {}, {}

        def use(p, t, centre, near):
            value = (near + re[t, pl.ds((p + O) * ye + base, 8), :]) - 6.0 * centre
            if p % 2:
                half[t] = 0.5 * value
                if p == nx - 1:
                    rx[t, pl.ds((nx // 2) * ny + at, 8), :] = quarter[t] + half[t]
                return
            value = 0.25 * value
            part = value if p == 0 else (quarter[t] + half[t]) + value
            rx[t, pl.ds((p // 2) * ny + at, 8), :] = part
            quarter[t] = value

        stencil(s2, ye, base, range(nx), rx.shape[0], use)
        return 0

    lax.fori_loop(0, tiles[0], rows, 0)


def every(ye):
    return ye // 8, lambda r: pl.multiple_of(r * 8, 8)


def split_dot(value, weight):
    high = value.astype(jnp.bfloat16)
    rest = value - high.astype(jnp.float32)
    mid = rest.astype(jnp.bfloat16)
    small = (rest - mid.astype(jnp.float32)).astype(jnp.bfloat16)
    dot = functools.partial(jnp.dot, preferred_element_type=jnp.float32)
    return dot(high, weight) + dot(mid, weight) + dot(small, weight)


def lane_dot(src, src_at, dst, dst_at, rows, weight):
    step = max(s for s in range(8, 273, 8) if rows % s == 0)
    for at in range(0, rows, step):
        value = jnp.concatenate([src[t, pl.ds(src_at + at, step), :] for t in range(weight.shape[0] // LANES)], axis=1)
        got = split_dot(value, weight)
        for t in range(weight.shape[1] // LANES):
            dst[t, pl.ds(dst_at + at, step), :] = got[:, t * LANES:(t + 1) * LANES]


def transfer_weights(fine, coarse, halo, fine_dim, inner, outer):
    shape = (fine, coarse + halo) if fine_dim == 0 else (coarse + halo, fine)
    z = iota(shape, fine_dim)
    k = iota(shape, 1 - fine_dim)
    k = jnp.where(k >= coarse, k - (coarse + halo), k)
    off = z - 2 * k
    weight = jnp.where(off == 1, inner, jnp.where((off == 0) | (off == 2), outer, 0.0))
    return jnp.where(k < -1, 0.0, weight).astype(jnp.bfloat16)


def inner_body(nx, ny, nz, se, re, s1, s2, rx, mask):
    fill_mask(mask, ny)
    many = ny // 8 - 1
    sweep(se, s1, re, mask, nx, 2, 2, (many, lambda r: pl.multiple_of(r * 8 + 8, 8)))
    sweep(s1, s2, re, mask, nx, 1, 1, (many, lambda r: jnp.minimum(r * 8 + 9, ny - 9)))
    residual_x(s2, re, rx, nx, ny, (many, lambda r: O + jnp.minimum(r * 8 + 6, ny - 14)))


def outer_body(nx, ny, nz, nin, *refs):
    halo = refs[:nin]
    se, re, s1, s2, rx, coarse = refs[nin + 5:nin + 11]
    outs = refs[nin + 11:-2]
    ry, mask = refs[-2:]
    nt = nz // LANES
    place_y(halo, se, re, nx, ny)
    fill_mask(mask, ny)
    sweep(se, s1, re, mask, nx, 2, 2, (2, lambda r: pl.multiple_of(r * ny, 8)))
    sweep(s1, s2, re, mask, nx, 1, 1, (2, lambda r: r * (ny - 2) + 1))
    residual_x(s2, re, rx, nx, ny, (2, lambda r: O + r * (ny - 8)))

    cx, cy, cz = nx // 2, ny // 2, nz // 2
    ct = cz // LANES
    cye = cy + 2 * O
    row = iota((8, LANES), 0)
    zero = jnp.zeros((8, LANES), jnp.float32)
    for t in range(nt):
        rx[t, pl.ds((cx + 1) * ny, 8), :] = zero

    def restrict_y(i, _):
        for t in range(nt):
            for k in range(cy // 8):
                at = i * ny + 16 * k
                even = 0.25 * rx[t, pl.ds(at, 8, stride=2), :]
                odd = 0.5 * rx[t, pl.ds(at + 1, 8, stride=2), :]
                after = 0.25 * rx[t, pl.ds(at + 2, 8, stride=2), :]
                if k == cy // 8 - 1:
                    after = jnp.where(row == 7, 0.0, after)
                if k == 0:
                    ry[t, pl.ds(i * cye, 8), :] = jnp.where(row == O - 1, even[0:1], 0.0)
                    ry[t, pl.ds(i * cye + cy, 8), :] = zero
                ry[t, pl.ds(i * cye + O + 8 * k, 8), :] = (even + odd) + after
        return 0

    lax.fori_loop(0, cx + 1, restrict_y, 0, unroll=3 if cx % 3 == 2 else 1)
    weight = transfer_weights(nz, cz, LANES, 0, 2.0, 1.0)
    lane_dot(ry, 0, coarse, (O - 1) * cye, (cx + 1) * cye, weight)
    for t in range(ct + 1):
        coarse[t, pl.ds((cx + 2 * O - 1) * cye, cye), :] = jnp.zeros((cye, LANES), jnp.float32)
    pack_coarse(outs, coarse, cx, cy)


def pack_coarse(outs, coarse, cx, cy):
    ct = coarse.shape[0] - 1
    ye = cy + 2 * O
    lane = iota((8, LANES), 1)

    def rows(r, _):
        base = pl.multiple_of(r * 8, 8)
        for group in range(-(-(cx + 1) // CPER)):
            low = high = None
            for j in range(min(CPER, cx + 1 - group * CPER)):
                at = j * CL
                rows8 = pl.ds((O - 1 + group * CPER + j) * ye + base, 8)
                head = jnp.where(lane < CL - 1, coarse[0, rows8, :], coarse[ct, rows8, :])
                head = turn(head, at + 1)
                tail = turn(coarse[ct - 1, rows8, :], at + CL)
                low = head if low is None else jnp.where(lane >= at, head, low)
                high = tail if high is None else jnp.where(lane >= at, tail, high)
            emit(outs, (group, pl.ds(base, 8)), "gz", lambda: low, lambda: high)
        return 0

    lax.fori_loop(0, ye // 8, rows, 0)


def faces(outs, axis, low, high, ct):
    extra_low = extra_high = None
    for j in range(CL):
        for t in range(ct):
            emit(outs, (j * ct + t,), axis, lambda: low(t, j), lambda: high(t, j))
        a = turn(low(ct, j), 8 * j + CL)
        b = turn(high(ct, j), 8 * j + CL)
        lane = iota(a.shape, 1)
        extra_low = a if j == 0 else jnp.where(lane >= 8 * j, a, extra_low)
        extra_high = b if j == 0 else jnp.where(lane >= 8 * j, b, extra_high)
    emit(outs, (CL * ct,), axis, lambda: extra_low, lambda: extra_high)


def place_faces(refs, axis, ct, size, read, write):
    for t in range(ct + 1):
        for j in range(CL):
            if t < ct:
                high, low = arrived(refs, (j * ct + t,), axis)
            else:
                high, low = arrived(refs, (CL * ct,), axis)
                lane = iota(high.shape, 1)
                used = (lane < CH) | (lane >= LANES - CL)
                high = jnp.where(used, turn(high, -8 * j - CL), 0.0)
                low = jnp.where(used, turn(low, -8 * j - CL), 0.0)
            q = size - 1 + j
            write(t, q, read(t, q) + high if j == 0 else high)
            q = j - CL
            write(t, q, read(t, q) + low if j == CL - 1 else low)


def coarse_z_body(cx, cy, cz, nin, *refs):
    halo = refs[:nin]
    coarse, outs = refs[nin + 1], refs[nin + 2:]
    ct = cz // LANES
    xe, ye = cx + 2 * O, cy + 2 * O
    lane = iota((8, LANES), 1)

    def unpack(r, _):
        base = pl.multiple_of(r * 8, 8)
        for group in range(-(-(cx + 1) // CPER)):
            high, low = arrived(halo, (group, pl.ds(base, 8)), "gz")
            for j in range(min(CPER, cx + 1 - group * CPER)):
                here = pl.ds((O - 1 + group * CPER + j) * ye + base, 8)
                fromhigh = turn(high, -j * CL - 1)
                fromlow = turn(low, -j * CL - CL)
                edge = lane == LANES - 1
                tail = coarse[ct - 1, here, :]
                own = coarse[ct, here, :]
                coarse[ct - 1, here, :] = tail + jnp.where(edge, fromhigh, 0.0)
                wing = jnp.where(lane < CH, fromhigh, jnp.where(lane >= LANES - CL, fromlow, 0.0))
                coarse[ct, here, :] = wing + jnp.where(edge, own, 0.0)
        return 0

    lax.fori_loop(0, ye // 8, unpack, 0)
    faces(
        outs, RING,
        lambda t, j: coarse[t, pl.ds((O - 1 + j) * ye, ye), :],
        lambda t, j: coarse[t, pl.ds((cx + j) * ye, ye), :],
        ct,
    )


def coarse_x_body(cx, cy, cz, nin, *refs):
    halo = refs[:nin]
    coarse, outs = refs[nin + 1], refs[nin + 2:]
    ct = cz // LANES
    xe, ye = cx + 2 * O, cy + 2 * O

    def read(t, q):
        return coarse[t, pl.ds((q + O) * ye, ye), :]

    def write(t, q, value):
        coarse[t, pl.ds((q + O) * ye, ye), :] = value

    place_faces(halo, RING, ct, cx, read, write)
    faces(
        outs, "gy",
        lambda t, j: coarse[t, pl.ds(O - 1 + j, xe, stride=ye), :],
        lambda t, j: coarse[t, pl.ds(cy + j, xe, stride=ye), :],
        ct,
    )


def coarse_sweeps(coarse, c, mask, cx, cy, first, tiles):
    total, ye, _ = mask.shape
    begin, last = ends("gx")
    up = jnp.where(last, 0.0, 1.0)
    down = jnp.where(begin, 0.0, 1.0)

    def rows(r, _):
        base = first[1](r)
        m = [mask[t, pl.ds(base, 8), :] for t in range(total)]
        for q in range(cx + 2 * O - 1):
            here = pl.ds(q * ye + base, 8)
            for t in range(total):
                factor = m[t] * down if q < O else m[t] * up if q >= O + cx else m[t]
                c[0][t, here, :] = factor * coarse[t, here, :]
        return 0

    lax.fori_loop(0, first[0], rows, 0)
    for n, (low, high) in enumerate(((3, 2), (2, 1), (1, 0))):
        sweep(c[n], c[n + 1], coarse, mask, cx, low, high, tiles[n])


def prolong_add(c, fine, smooth, stage, cx, cy, cz, pieces, tiles):
    ye = cy + 2 * O
    nx, ny, nz = 2 * cx, 2 * cy, 2 * cz
    nt = nz // LANES
    fye = ny + 2 * O
    weight = transfer_weights(nz, cz, LANES, 1, 1.0, 0.5)
    starts = [q * ye + piece for q in range(cx + 1) for piece in pieces]
    for at in range(0, len(starts), 33):
        some = starts[at:at + 33]
        wide = range(weight.shape[0] // LANES)
        value = jnp.concatenate(
            [
                jnp.concatenate([c[t, pl.ds((O - 1) * ye + s, 8), :] for s in some], axis=0)
                for t in wide
            ],
            axis=1,
        )
        got = split_dot(value, weight)
        for n, s in enumerate(some):
            for t in range(nt):
                fine[t, pl.ds(s, 8), :] = got[8 * n:8 * n + 8, t * LANES:(t + 1) * LANES]
    flat = stage.reshape(nt, nx * ny, LANES)

    def add(i, _):
        for t in range(nt):
            for row in tiles:
                at = (i + 1) * ye + O + row
                here = fine[t, pl.ds(at, 8), :]
                mid = 0.5 * (here + fine[t, pl.ds(at - 1, 8), :])
                before = fine[t, pl.ds(at - ye, 8), :]
                before_mid = 0.5 * (before + fine[t, pl.ds(at - ye - 1, 8), :])
                parts = (0.5 * (before_mid + mid), 0.5 * (before + here), mid, here)
                for n, part in enumerate(parts):
                    src = (2 * i + n // 2 + O) * fye + O + 2 * row + n % 2
                    dst = (2 * i + n // 2) * ny + 2 * row + n % 2
                    flat[t, pl.ds(dst, 8, stride=2), :] = smooth[t, pl.ds(src, 8, stride=2), :] + part
        return 0

    return add


def write_out(add, stage, out, sems, cx, spans):
    chunks = sems.shape[0]
    per = cx // chunks
    nt = stage.shape[0]

    def copies(c):
        at = c * 2 * per
        return [
            pltpu.make_async_copy(
                stage.at[t, pl.ds(at, 2 * per), pl.ds(row, many)],
                out.at[pl.ds(at, 2 * per), pl.ds(row, many), pl.ds(t * LANES, LANES)],
                sems.at[c, t * len(spans) + n],
            )
            for t in range(nt)
            for n, (row, many) in enumerate(spans)
        ]

    for c in range(chunks):
        lax.fori_loop(c * per, (c + 1) * per, add, 0)
        for copy in copies(c):
            copy.start()
    for c in range(chunks):
        for copy in copies(c):
            copy.wait()


def finish_inner_body(cx, cy, cz, smooth, coarse, c0, c1, c2, c3, out, mask, fine, stage, sems):
    c = [c0, c1, c2, c3]
    fill_mask(mask, cy)
    tiles = []
    for n in (1, 2, 3):
        many = -(-(cy - 1 - 2 * n) // 8)
        tiles.append((many, lambda r, n=n: jnp.minimum(O + n + 8 * r, O + cy - 1 - n - 8)))
    coarse_sweeps(coarse, c, mask, cx, cy, every(cy + 2 * O), tiles)
    add = prolong_add(c3, fine, smooth, stage, cx, cy, cz, range(0, cy, 8), range(4, cy - 4, 8))
    write_out(add, stage, out, sems, cx, [(8, 2 * cy - 16)])


def finish_outer_body(cx, cy, cz, nin, *refs):
    halo = refs[:nin]
    smooth, coarse = refs[nin], refs[nin + 7]
    c = refs[nin + 8:nin + 12]
    out = refs[nin + 12]
    mask, fine, stage, sems = refs[nin + 13:]
    ct = cz // LANES
    xe, ye = cx + 2 * O, cy + 2 * O

    def read(t, q):
        return coarse[t, pl.ds(q + O, xe, stride=ye), :]

    def write(t, q, value):
        coarse[t, pl.ds(q + O, xe, stride=ye), :] = value

    place_faces(halo, "gy", ct, cy, read, write)
    fill_mask(mask, cy)
    both = (2, lambda r: pl.multiple_of(r * cy, 8))
    coarse_sweeps(coarse, c, mask, cx, cy, both, [both] * 3)
    add = prolong_add(c[3], fine, smooth, stage, cx, cy, cz, (0, cy - 8, cy), (0, cy - 8))
    write_out(add, stage, out, sems, cx, [(0, 8), (2 * cy - 8, 8)])


def on_device(start, right):
    nx, ny, nz = start.shape
    nt = nz // LANES
    xe, ye = nx + 2 * O, ny + 2 * O
    cx, cy, cz = nx // 2, ny // 2, nz // 2
    ct = cz // LANES
    cxe, cye = cx + 2 * O, cy + 2 * O
    big = f32(nt + 1, xe * ye, LANES)
    mb = 1 << 20

    msgs = call(
        xpack_body, "xpack", [start[:F], right[:G], start[nx - F:], right[nx - G:]],
        [f32(SLOT, ny, nz)] * count("gx"), limit=4 * mb, cost=9e9,
    )
    halo = exchange(msgs, "gx")
    face = [f32(-(-xe // PER), ny, LANES)] * count("gz")
    se, re, *msgs = call(build_body, "build", [start, right], [big, big] + face, limit=8 * mb)

    n = len(halo)
    alias = {n + i: i for i in range(2 + len(msgs))}
    se, re, *msgs = call(
        functools.partial(xhalo_body, nx, ny, nz, n), "xhalo", [*halo, se, re, *msgs],
        [big, big] + face, alias=alias, limit=8 * mb,
    )
    halo = exchange(msgs, "gz")
    n = len(halo)
    se, re, *msgs = call(
        functools.partial(zhalo_body, nx, ny, nz, n), "zhalo", [*halo, se, re],
        [big, big] + [f32(SLOT * nt + 1, xe, LANES)] * count("gy"), alias={n: 0, n + 1: 1}, limit=8 * mb,
    )
    halo = exchange(msgs, "gy")
    part = f32(nt, (cx + 1) * ny + 8, LANES)
    masks = pltpu.VMEM((nt + 1, ye, LANES), jnp.float32)
    s1, s2, rx = call(
        functools.partial(inner_body, nx, ny, nz), "inner", [se, re], [big, big, part], scratch=[masks],
        limit=8 * mb, cost=9e9,
    )
    n = len(halo)
    small = f32(ct + 1, cxe * cye, LANES)
    se, re, s1, s2, rx, coarse, *msgs = call(
        functools.partial(outer_body, nx, ny, nz, n), "outer", [*halo, se, re, s1, s2, rx],
        [big, big, big, big, part, small] + [f32(-(-(cx + 1) // CPER), cye, LANES)] * count("gz"),
        scratch=[pltpu.VMEM((nt, (cx + 1) * cye, LANES), jnp.float32), masks],
        alias={n + i: i for i in range(5)}, limit=8 * mb,
    )
    halo = exchange(msgs, "gz")
    n = len(halo)
    coarse, *msgs = call(
        functools.partial(coarse_z_body, cx, cy, cz, n), "coarse_z", [*halo, coarse],
        [small] + [f32(CL * ct + 1, cye, LANES)] * count(RING), alias={n: 0}, limit=8 * mb,
    )
    halo = exchange(msgs, RING)
    n = len(halo)
    coarse, *msgs = call(
        functools.partial(coarse_x_body, cx, cy, cz, n), "coarse_x", [*halo, coarse],
        [small] + [f32(CL * ct + 1, cxe, LANES)] * count("gy"), alias={n: 0}, limit=8 * mb,
    )
    halo = exchange(msgs, "gy")
    n = len(halo)
    stage = [
        pltpu.VMEM((ct + 1, cye, LANES), jnp.float32),
        pltpu.VMEM((nt, (cx + 1) * cye, LANES), jnp.float32),
        pltpu.VMEM((nt, nx, ny, LANES), jnp.float32),
    ]
    *c, out = call(
        functools.partial(finish_inner_body, cx, cy, cz), "finish_inner", [s2, coarse],
        [small] * 4 + [f32(nx, ny, nz)], scratch=stage + [pltpu.SemaphoreType.DMA((8, nt))],
        limit=10 * mb, out_specs=[VMEM] * 4 + [ANY], cost=5e9,
    )
    *_, out = call(
        functools.partial(finish_outer_body, cx, cy, cz, n), "finish_outer", [*halo, s2, coarse, *c, out],
        [small] * 5 + [f32(nx, ny, nz)], scratch=stage + [pltpu.SemaphoreType.DMA((2, 2 * nt))],
        alias={n + 1 + i: i for i in range(6)}, limit=10 * mb,
        in_specs=[VMEM] * (n + 6) + [ANY], out_specs=[VMEM] * 5 + [ANY],
    )
    return out


def solution(mesh):
    spec = P("gx", "gy", "gz")
    return jax.shard_map(on_device, mesh=mesh, in_specs=(spec, spec), out_specs=spec, check_vma=False)
```

```python
import functools

import jax
import jax.numpy as jnp
from jax import lax
from jax.experimental import pallas as pl
from jax.experimental.pallas import tpu as pltpu
from jax.sharding import PartitionSpec as P

LANES = 128
O = 4
F = 3
G = 2
SLOT = F + G
PER = LANES // SLOT
CL = 4
CH = 3
CPER = LANES // CL

VMEM = pl.BlockSpec(memory_space=pltpu.VMEM)
ANY = pl.BlockSpec(memory_space=pl.ANY)


def f32(*shape):
    return jax.ShapeDtypeStruct(shape, jnp.float32)


def call(body, name, ins, outs, scratch=(), alias=None, limit=None, out_specs=None, cost=1e8,
         in_specs=None):
    return pl.pallas_call(
        body,
        name=name,
        in_specs=[VMEM] * len(ins) if in_specs is None else in_specs,
        out_specs=[VMEM] * len(outs) if out_specs is None else out_specs,
        out_shape=outs,
        scratch_shapes=list(scratch),
        input_output_aliases=alias or {},
        cost_estimate=pl.CostEstimate(flops=int(cost), bytes_accessed=0, transcendentals=0),
        compiler_params=pltpu.CompilerParams(vmem_limit_bytes=limit),
    )(*ins)


def iota(shape, dim):
    return lax.broadcasted_iota(jnp.int32, shape, dim)


RING = "gx/ring"


def size_of(axis):
    return lax.axis_size(axis.split("/")[0])


def ends(axis):
    i = lax.axis_index(axis.split("/")[0])
    return i == 0, i == size_of(axis) - 1


def paired(axis):
    return axis != RING


def exchange(msgs, axis):
    n = size_of(axis)
    if not paired(axis):
        axis = axis.split("/")[0]
        down = lax.ppermute(msgs[0], axis, [(i, (i - 1) % n) for i in range(n)])
        up = lax.ppermute(msgs[1], axis, [(i, (i + 1) % n) for i in range(n)])
        return [down, up]
    found = [None] * len(msgs)
    for phase in reversed(range(len(msgs))):
        routes = []
        for i in range(phase, n - 1, 2):
            routes += [(i, i + 1), (i + 1, i)]
        found[phase] = lax.ppermute(msgs[phase], axis, routes)
    return found


def emit(outs, index, axis, low, high):
    if isinstance(outs, Kept):
        outs.lows.append(low())
        outs.highs.append(high())
    elif paired(axis):
        even = lax.axis_index(axis) % 2 == 0
        low, high = low(), high()
        outs[0][index] = jnp.where(even, high, low)
        if len(outs) > 1:
            outs[1][index] = jnp.where(even, low, high)
    else:
        outs[0][index] = low()
        outs[1][index] = high()


def arrived(refs, index, axis):
    a = refs[0][index]
    b = refs[1][index] if len(refs) > 1 else jnp.zeros_like(a)
    if paired(axis):
        even = lax.axis_index(axis) % 2 == 0
        return jnp.where(even, a, b), jnp.where(even, b, a)
    first, last = ends(axis)
    return jnp.where(last, 0.0, a), jnp.where(first, 0.0, b)


def written(outs, index, axis):
    a = outs[0][index]
    b = outs[1][index] if len(outs) > 1 else jnp.zeros_like(a)
    if paired(axis):
        even = lax.axis_index(axis) % 2 == 0
        return jnp.where(even, a, b), jnp.where(even, b, a)
    return b, a


def count(axis):
    return 1 if paired(axis) and size_of(axis) == 2 else 2


def turn(value, lanes):
    return pltpu.roll(value, lanes % LANES, 1)


def xpack_body(*refs):
    first_s, first_r, last_s, last_r, *outs = refs
    for k in range(SLOT):
        low, high, j = (first_s, last_s, k) if k < F else (first_r, last_r, k - F)
        emit(outs, (k,), "gx", lambda: low[j], lambda: high[j])


def pack(outs, at_row, group, planes, load, partial):
    lane = iota((8, LANES), 1)
    low, high = partial
    done = None
    wrapped = None
    for q in planes:
        at = (q - group * PER) * SLOT
        s_low, s_high, r_low, r_high = load(q)
        one = turn(jnp.where(lane < 64, s_low, r_high), at + G)
        two = turn(jnp.where(lane < 64, r_low, s_high), at)
        start_at = lane >= at
        start_g = lane >= at + G
        if done is not None and done != q - 1:
            raise ValueError("planes")
        low = jnp.where(start_g, one, jnp.where(start_at, two, low))
        if at == 0:
            wrapped = two
            high = jnp.where(start_at, one, high)
        else:
            high = jnp.where(start_at, one, jnp.where(lane >= at - F, two, high))
        done = q
    if wrapped is not None:
        high = jnp.where(lane >= LANES - F, wrapped, high)
    if planes:
        emit(outs, (group, pl.ds(at_row, 8)), "gz", lambda: low, lambda: high)


def build_body(start, right, se, re, *outs):
    nx, ny, nz = start.shape
    xe, ye = nx + 2 * O, ny + 2 * O
    nt = nz // LANES

    def rows(r, _):
        at = pl.multiple_of(r * 8, 8)
        zero = jnp.zeros((8, LANES), jnp.float32)

        def load(q):
            found = {}
            for t in range(nt):
                for key, src, dst in (("s", start, se), ("r", right, re)):
                    value = src[q - O, pl.ds(at, 8), t * LANES:(t + 1) * LANES]
                    dst[t, pl.ds(q * ye + at + O, 8), :] = value
                    found[key, t] = value
            return found["s", 0], found["s", nt - 1], found["r", 0], found["r", nt - 1]

        for group in range(-(-xe // PER)):
            planes = range(max(O, group * PER), min(O + nx, (group + 1) * PER))
            pack(outs, at, group, planes, load, (zero, zero))
        return 0

    lax.fori_loop(0, ny // 8, rows, 0, unroll=2)


def xhalo_body(nx, ny, nz, nin, *refs):
    halo = refs[:nin]
    outs = refs[nin + count("gz"):]
    xe = nx + 2 * O
    first, final = slice(0, LANES), slice(nz - LANES, nz)
    lane = iota((8, LANES), 1)

    def rows(r, _):
        at = pl.multiple_of(r * 8, 8)

        def load(q):
            after = q >= O
            s_layer = q - O - nx if after else q - O + F
            r_layer = F + (min(q - O - nx, G - 1) if after else max(q - O + G, 0))

            def get(layer, cut):
                high, low = arrived(halo, (layer, pl.ds(at, 8), cut), "gx")
                return high if after else low

            return get(s_layer, first), get(s_layer, final), get(r_layer, first), get(r_layer, final)

        for group in range(-(-xe // PER)):
            span = range(group * PER, min(xe, (group + 1) * PER))
            before = [q for q in span if O - F <= q < O]
            after = [q for q in span if O + nx <= q < O + nx + F]
            if not before and not after:
                continue
            core_high, core_low = written(outs, (group, pl.ds(at, 8)), "gz")
            lows, highs = [], []
            pack(Kept(lows, highs), at, group, before, load, (core_low, core_high))
            if before:
                top = (O - group * PER) * SLOT
                low = jnp.where(lane < top, lows[0], core_low)
                high = jnp.where((lane < top - F) | (lane >= LANES - F), highs[0], core_high)
                core_low, core_high = low, high
            if after:
                lows, highs = [], []
                pack(Kept(lows, highs), at, group, after, load, (core_low, core_high))
                core_low, core_high = lows[0], jnp.where(lane >= LANES - F, core_high, highs[0])
            emit(outs, (group, pl.ds(at, 8)), "gz", lambda: core_low, lambda: core_high)
        return 0

    lax.fori_loop(0, ny // 8, rows, 0, unroll=2)


class Kept:
    def __init__(self, lows, highs):
        self.lows, self.highs = lows, highs


def middle_body(nx, ny, nz, nin, *refs):
    halo = refs[:nin]
    se, re, outs = refs[nin + 2], refs[nin + 3], refs[nin + 4:]
    xe, ye = nx + 2 * O, ny + 2 * O
    nt = nz // LANES
    for t in range(nt):
        cut = slice(t * LANES, (t + 1) * LANES)
        for k in range(SLOT):
            high, low = arrived(halo, (k, slice(None), cut), "gx")
            dst, size, j = (se, F, k) if k < F else (re, G, k - F)
            dst[t, pl.ds((O + nx + j) * ye + O, ny), :] = high
            dst[t, pl.ds((O - size + j) * ye + O, ny), :] = low
    for k in range(SLOT):
        src, size, j = (se, F, k) if k < F else (re, G, k - F)
        for t in range(nt):
            emit(
                outs, (k * nt + t,), "gy",
                lambda: src[t, pl.ds(O + j, xe, stride=ye), :],
                lambda: src[t, pl.ds(O + ny - size + j, xe, stride=ye), :],
            )


def zhalo_body(nx, ny, nz, nin, *refs):
    halo = refs[:nin]
    outs = refs[nin + 2 + count("gy"):]
    se, re, outs = outs[0], outs[1], outs[2:]
    xe, ye = nx + 2 * O, ny + 2 * O
    nt = nz // LANES
    lane = iota((8, LANES), 1)

    def unpack(r, _):
        at_row = pl.multiple_of(r * 8, 8)
        for group in range(-(-xe // PER)):
            high, low = arrived(halo, (group, pl.ds(at_row, 8)), "gz")
            pick = lane % SLOT < G
            one = jnp.where(pick, high, low)
            two = jnp.where(pick, low, high)
            one = jnp.where(lane >= LANES - F, low, one)
            for j in range(min(PER, xe - group * PER)):
                a = turn(one, -j * SLOT)
                b = turn(two, -j * SLOT - G)
                here = pl.ds((group * PER + j) * ye + at_row + O, 8)
                se[nt, here, :] = jnp.where(lane < 64, b, a)
                re[nt, here, :] = jnp.where(lane < 64, a, b)
        return 0

    lax.fori_loop(0, ny // 8, unpack, 0, unroll=2)
    lane = iota((xe, LANES), 1)
    extra_low = extra_high = jnp.zeros((xe, LANES), jnp.float32)
    for k in range(SLOT):
        src, size, j = (se, F, k) if k < F else (re, G, k - F)
        low = src[nt, pl.ds(O + j, xe, stride=ye), :]
        high = src[nt, pl.ds(O + ny - size + j, xe, stride=ye), :]
        here = (lane >= 8 * k) & (lane < 8 * k + 2 * F)
        extra_low = jnp.where(here, turn(low, 8 * k + F), extra_low)
        extra_high = jnp.where(here, turn(high, 8 * k + F), extra_high)
    emit(outs, (SLOT * nt,), "gy", lambda: extra_low, lambda: extra_high)


def place_y(halo, se, re, nx, ny):
    xe, ye = nx + 2 * O, ny + 2 * O
    nt = se.shape[0] - 1
    for k in range(SLOT):
        dst, size, j = (se, F, k) if k < F else (re, G, k - F)
        for t in range(nt + 1):
            if t < nt:
                high, low = arrived(halo, (k * nt + t,), "gy")
            else:
                high, low = (turn(v, -8 * k - F) for v in arrived(halo, (SLOT * nt,), "gy"))
            dst[t, pl.ds(O + ny + j, xe, stride=ye), :] = high
            dst[t, pl.ds(O - size + j, xe, stride=ye), :] = low


def inside(shape, dim, offset, cells, axis):
    first, last = ends(axis)
    at = iota(shape, dim) - offset
    up = jnp.where(last, 0.0, 1.0)
    down = jnp.where(first, 0.0, 1.0)
    return jnp.where(at < 0, down, jnp.where(at < cells, 1.0, up))


def fill_mask(mask, ny):
    total, ye, _ = mask.shape
    valid = inside((ye, LANES), 0, O, ny, "gy") * (1.0 / 7.0)
    for t in range(total - 1):
        mask[t] = valid
    first, last = ends("gz")
    lane = iota((ye, LANES), 1)
    mask[total - 1] = valid * jnp.where(
        lane < CH, jnp.where(last, 0.0, 1.0), jnp.where(lane >= LANES - CL, jnp.where(first, 0.0, 1.0), 0.0)
    )


def stencil(ref, ye, base, planes, tiles, use):
    total = ref.shape[0]
    lane = iota((8, LANES), 1)

    def at(p, t, shift=0):
        return ref[t, pl.ds((p + O) * ye + base + shift, 8), :]

    before = [at(planes[0] - 1, t) for t in range(tiles)]
    centre = [at(planes[0], t) for t in range(total)]
    for p in planes:
        after = [at(p + 1, t) for t in range(total)]
        for t in range(tiles):
            wrapped = jnp.where(lane == LANES - 1, centre[t - 1], centre[t])
            near = turn(wrapped, 1)
            wrapped = jnp.where(lane == 0, centre[(t + 1) % total], centre[t])
            near = near + turn(wrapped, -1)
            near = near + (at(p, t, -1) + at(p, t, 1))
            near = near + (before[t] + after[t])
            use(p, t, centre[t], near)
        before, centre = centre, after


def sweep(src, dst, right, mask, nx, low, high, tiles):
    total, ye, _ = mask.shape
    first, last = ends("gx")
    up = jnp.where(last, 0.0, 1.0)
    down = jnp.where(first, 0.0, 1.0)

    def rows(r, _):
        base = tiles[1](r)
        m = [mask[t, pl.ds(base, 8), :] for t in range(total)]

        def use(p, t, centre, near):
            here = pl.ds((p + O) * ye + base, 8)
            factor = m[t] * down if p < 0 else m[t] * up if p >= nx else m[t]
            dst[t, here, :] = factor * (near + (centre + right[t, here, :]))

        stencil(src, ye, base, range(-low, nx + high), total, use)
        return 0

    lax.fori_loop(0, tiles[0], rows, 0, unroll=tiles[0] if tiles[0] <= 4 else 1)


def residual_x(s2, re, rx, nx, ny, tiles):
    ye = ny + 2 * O

    def rows(r, _):
        base = tiles[1](r)
        at = base - O
        quarter, half = {}, {}

        def use(p, t, centre, near):
            value = (near + re[t, pl.ds((p + O) * ye + base, 8), :]) - 6.0 * centre
            if p % 2:
                half[t] = 0.5 * value
                if p == nx - 1:
                    rx[t, pl.ds((nx // 2) * ny + at, 8), :] = quarter[t] + half[t]
                return
            value = 0.25 * value
            part = value if p == 0 else (quarter[t] + half[t]) + value
            rx[t, pl.ds((p // 2) * ny + at, 8), :] = part
            quarter[t] = value

        stencil(s2, ye, base, range(nx), rx.shape[0], use)
        return 0

    lax.fori_loop(0, tiles[0], rows, 0, unroll=tiles[0] if tiles[0] <= 4 else 1)


def every(ye):
    return ye // 8, lambda r: pl.multiple_of(r * 8, 8)


def split_dot(value, weight):
    high = value.astype(jnp.bfloat16)
    rest = value - high.astype(jnp.float32)
    mid = rest.astype(jnp.bfloat16)
    small = (rest - mid.astype(jnp.float32)).astype(jnp.bfloat16)
    dot = functools.partial(jnp.dot, preferred_element_type=jnp.float32)
    return dot(high, weight) + dot(mid, weight) + dot(small, weight)


def lane_dot(src, src_at, dst, dst_at, rows, weight):
    step = max(s for s in range(8, 273, 8) if rows % s == 0)
    for at in range(0, rows, step):
        value = jnp.concatenate([src[t, pl.ds(src_at + at, step), :] for t in range(weight.shape[0] // LANES)], axis=1)
        got = split_dot(value, weight)
        for t in range(weight.shape[1] // LANES):
            dst[t, pl.ds(dst_at + at, step), :] = got[:, t * LANES:(t + 1) * LANES]


def transfer_weights(fine, coarse, halo, fine_dim, inner, outer):
    shape = (fine, coarse + halo) if fine_dim == 0 else (coarse + halo, fine)
    z = iota(shape, fine_dim)
    k = iota(shape, 1 - fine_dim)
    k = jnp.where(k >= coarse, k - (coarse + halo), k)
    off = z - 2 * k
    weight = jnp.where(off == 1, inner, jnp.where((off == 0) | (off == 2), outer, 0.0))
    return jnp.where(k < -1, 0.0, weight).astype(jnp.bfloat16)


def inner_body(nx, ny, nz, se, re, s1, s2, rx, mask):
    fill_mask(mask, ny)
    many = ny // 8 - 1
    sweep(se, s1, re, mask, nx, 2, 2, (many, lambda r: pl.multiple_of(r * 8 + 8, 8)))
    sweep(s1, s2, re, mask, nx, 1, 1, (many, lambda r: jnp.minimum(r * 8 + 9, ny - 9)))
    residual_x(s2, re, rx, nx, ny, (many, lambda r: O + jnp.minimum(r * 8 + 6, ny - 14)))


def outer_body(nx, ny, nz, nin, *refs):
    halo = refs[:nin]
    se, re, s1, s2, rx, coarse = refs[nin + 5:nin + 11]
    outs = refs[nin + 11:-2]
    ry, mask = refs[-2:]
    nt = nz // LANES
    place_y(halo, se, re, nx, ny)
    fill_mask(mask, ny)
    sweep(se, s1, re, mask, nx, 2, 2, (2, lambda r: pl.multiple_of(r * ny, 8)))
    sweep(s1, s2, re, mask, nx, 1, 1, (2, lambda r: r * (ny - 2) + 1))
    residual_x(s2, re, rx, nx, ny, (2, lambda r: O + r * (ny - 8)))

    cx, cy, cz = nx // 2, ny // 2, nz // 2
    ct = cz // LANES
    cye = cy + 2 * O
    restrict_yz(rx, ry, coarse, ny, cx, cz, [(0, CL), (cx + 1 - CL, CL)])
    faces(
        outs, RING,
        lambda t, j: coarse[t, pl.ds((O - 1 + j) * cye, cye), :],
        lambda t, j: coarse[t, pl.ds((cx + j) * cye, cye), :],
        ct,
    )


def restrict_yz(rx, ry, coarse, ny, cx, cz, spans):
    nt = rx.shape[0]
    nz = nt * LANES
    cy = ny // 2
    cye = cy + 2 * O
    row = iota((8, LANES), 0)
    zero = jnp.zeros((8, LANES), jnp.float32)
    weight = transfer_weights(nz, cz, LANES, 0, 2.0, 1.0)

    def restrict_y(i, _):
        for t in range(nt):
            for k in range(cy // 8):
                at = i * ny + 16 * k
                even = 0.25 * rx[t, pl.ds(at, 8, stride=2), :]
                odd = 0.5 * rx[t, pl.ds(at + 1, 8, stride=2), :]
                after = 0.25 * rx[t, pl.ds(at + 2, 8, stride=2), :]
                if k == cy // 8 - 1:
                    after = jnp.where(row == 7, 0.0, after)
                if k == 0:
                    ry[t, pl.ds(i * cye, 8), :] = jnp.where(row == O - 1, even[0:1], 0.0)
                    ry[t, pl.ds(i * cye + cy, 8), :] = zero
                ry[t, pl.ds(i * cye + O + 8 * k, 8), :] = (even + odd) + after
        return 0

    for t in range(nt):
        rx[t, pl.ds((cx + 1) * ny, 8), :] = zero
    for first, many in spans:
        unroll = max(u for u in (5, 4, 3, 2, 1) if many % u == 0)
        lax.fori_loop(first, first + many, restrict_y, 0, unroll=unroll)
        lane_dot(ry, first * cye, coarse, (O - 1 + first) * cye, many * cye, weight)


def rest_body(nx, ny, nz, rx, _, rx_out, coarse, ry):
    cx = nx // 2
    restrict_yz(rx_out, ry, coarse, ny, cx, nz // 2, [(CL, cx + 1 - 2 * CL)])
    ct = coarse.shape[0] - 1
    cye = ny // 2 + 2 * O
    for t in range(ct + 1):
        coarse[t, pl.ds((cx + 2 * O - 1) * cye, cye), :] = jnp.zeros((cye, LANES), jnp.float32)


def pack_coarse(outs, coarse, cx, cy):
    ct = coarse.shape[0] - 1
    ye = cy + 2 * O
    lane = iota((8, LANES), 1)

    def rows(r, _):
        base = pl.multiple_of(r * 8, 8)
        for group in range(-(-(cx + CL + CH) // CPER)):
            low = high = None
            for j in range(min(CPER, cx + CL + CH - group * CPER)):
                at = j * CL
                rows8 = pl.ds((group * CPER + j) * ye + base, 8)
                head = jnp.where(lane < CL - 1, coarse[0, rows8, :], coarse[ct, rows8, :])
                head = turn(head, at + 1)
                tail = turn(coarse[ct - 1, rows8, :], at + CL)
                low = head if low is None else jnp.where(lane >= at, head, low)
                high = tail if high is None else jnp.where(lane >= at, tail, high)
            emit(outs, (group, pl.ds(base, 8)), "gz", lambda: low, lambda: high)
        return 0

    lax.fori_loop(0, ye // 8, rows, 0)


def faces(outs, axis, low, high, ct):
    extra_low = extra_high = None
    for j in range(CL):
        for t in range(ct):
            emit(outs, (j * ct + t,), axis, lambda: low(t, j), lambda: high(t, j))
        a = turn(low(ct, j), 8 * j + CL)
        b = turn(high(ct, j), 8 * j + CL)
        lane = iota(a.shape, 1)
        extra_low = a if j == 0 else jnp.where(lane >= 8 * j, a, extra_low)
        extra_high = b if j == 0 else jnp.where(lane >= 8 * j, b, extra_high)
    emit(outs, (CL * ct,), axis, lambda: extra_low, lambda: extra_high)


def place_faces(refs, axis, ct, size, read, write):
    for t in range(ct + 1):
        for j in range(CL):
            if t < ct:
                high, low = arrived(refs, (j * ct + t,), axis)
            else:
                high, low = arrived(refs, (CL * ct,), axis)
                lane = iota(high.shape, 1)
                used = (lane < CH) | (lane >= LANES - CL)
                high = jnp.where(used, turn(high, -8 * j - CL), 0.0)
                low = jnp.where(used, turn(low, -8 * j - CL), 0.0)
            q = size - 1 + j
            write(t, q, read(t, q) + high if j == 0 else high)
            q = j - CL
            write(t, q, read(t, q) + low if j == CL - 1 else low)


def coarse_z_body(cx, cy, cz, nin, *refs):
    halo = refs[:nin]
    coarse, outs = refs[nin + 1], refs[nin + 2:]
    ct = cz // LANES
    xe, ye = cx + 2 * O, cy + 2 * O
    lane = iota((8, LANES), 1)

    def unpack(r, _):
        base = pl.multiple_of(r * 8, 8)
        for group in range(-(-(cx + CL + CH) // CPER)):
            high, low = arrived(halo, (group, pl.ds(base, 8)), "gz")
            for j in range(min(CPER, cx + CL + CH - group * CPER)):
                here = pl.ds((group * CPER + j) * ye + base, 8)
                fromhigh = turn(high, -j * CL - 1)
                fromlow = turn(low, -j * CL - CL)
                edge = lane == LANES - 1
                tail = coarse[ct - 1, here, :]
                own = coarse[ct, here, :]
                coarse[ct - 1, here, :] = tail + jnp.where(edge, fromhigh, 0.0)
                wing = jnp.where(lane < CH, fromhigh, jnp.where(lane >= LANES - CL, fromlow, 0.0))
                coarse[ct, here, :] = wing + jnp.where(edge, own, 0.0)
        return 0

    lax.fori_loop(0, ye // 8, unpack, 0)
    faces(
        outs, "gy",
        lambda t, j: coarse[t, pl.ds(O - 1 + j, xe, stride=ye), :],
        lambda t, j: coarse[t, pl.ds(cy + j, xe, stride=ye), :],
        ct,
    )


def coarse_x_body(cx, cy, cz, nin, *refs):
    halo = refs[:nin]
    coarse, outs = refs[nin + 1], refs[nin + 2:]
    ct = cz // LANES
    xe, ye = cx + 2 * O, cy + 2 * O

    def read(t, q):
        return coarse[t, pl.ds((q + O) * ye, ye), :]

    def write(t, q, value):
        coarse[t, pl.ds((q + O) * ye, ye), :] = value

    place_faces(halo, RING, ct, cx, read, write)
    pack_coarse(outs, coarse, cx, cy)


def coarse_sweeps(coarse, c, mask, cx, cy, first, tiles):
    total, ye, _ = mask.shape
    begin, last = ends("gx")
    up = jnp.where(last, 0.0, 1.0)
    down = jnp.where(begin, 0.0, 1.0)

    def rows(r, _):
        base = first[1](r)
        m = [mask[t, pl.ds(base, 8), :] for t in range(total)]
        for q in range(cx + 2 * O - 1):
            here = pl.ds(q * ye + base, 8)
            for t in range(total):
                factor = m[t] * down if q < O else m[t] * up if q >= O + cx else m[t]
                c[0][t, here, :] = factor * coarse[t, here, :]
        return 0

    lax.fori_loop(0, first[0], rows, 0)
    for n, (low, high) in enumerate(((3, 2), (2, 1), (1, 0))):
        sweep(c[n], c[n + 1], coarse, mask, cx, low, high, tiles[n])


def prolong_add(c, fine, smooth, stage, cx, cy, cz, pieces, tiles):
    ye = cy + 2 * O
    nx, ny, nz = 2 * cx, 2 * cy, 2 * cz
    nt = nz // LANES
    fye = ny + 2 * O
    weight = transfer_weights(nz, cz, LANES, 1, 1.0, 0.5)
    starts = [q * ye + piece for q in range(cx + 1) for piece in pieces]
    for at in range(0, len(starts), 33):
        some = starts[at:at + 33]
        wide = range(weight.shape[0] // LANES)
        value = jnp.concatenate(
            [
                jnp.concatenate([c[t, pl.ds((O - 1) * ye + s, 8), :] for s in some], axis=0)
                for t in wide
            ],
            axis=1,
        )
        got = split_dot(value, weight)
        for n, s in enumerate(some):
            for t in range(nt):
                fine[t, pl.ds(s, 8), :] = got[8 * n:8 * n + 8, t * LANES:(t + 1) * LANES]
    flat = stage.reshape(nt, nx * ny, LANES)

    def add(i, _):
        for t in range(nt):
            for row in tiles:
                at = (i + 1) * ye + O + row
                here = fine[t, pl.ds(at, 8), :]
                mid = 0.5 * (here + fine[t, pl.ds(at - 1, 8), :])
                before = fine[t, pl.ds(at - ye, 8), :]
                before_mid = 0.5 * (before + fine[t, pl.ds(at - ye - 1, 8), :])
                parts = (0.5 * (before_mid + mid), 0.5 * (before + here), mid, here)
                for n, part in enumerate(parts):
                    src = (2 * i + n // 2 + O) * fye + O + 2 * row + n % 2
                    dst = (2 * i + n // 2) * ny + 2 * row + n % 2
                    flat[t, pl.ds(dst, 8, stride=2), :] = smooth[t, pl.ds(src, 8, stride=2), :] + part
        return 0

    return add


def write_out(add, stage, out, sems, cx, spans):
    chunks = sems.shape[0]
    per = cx // chunks
    nt = stage.shape[0]

    def copies(c):
        at = c * 2 * per
        return [
            pltpu.make_async_copy(
                stage.at[t, pl.ds(at, 2 * per), pl.ds(row, many)],
                out.at[pl.ds(at, 2 * per), pl.ds(row, many), pl.ds(t * LANES, LANES)],
                sems.at[c, t * len(spans) + n],
            )
            for t in range(nt)
            for n, (row, many) in enumerate(spans)
        ]

    for c in range(chunks):
        lax.fori_loop(c * per, (c + 1) * per, add, 0)
        for copy in copies(c):
            copy.start()
    for c in range(chunks):
        for copy in copies(c):
            copy.wait()


def finish_inner_body(cx, cy, cz, smooth, coarse, c0, c1, c2, c3, out, mask, fine, stage, sems):
    c = [c0, c1, c2, c3]
    fill_mask(mask, cy)
    tiles = []
    for n in (1, 2, 3):
        many = -(-(cy - 1 - 2 * n) // 8)
        tiles.append((many, lambda r, n=n: jnp.minimum(O + n + 8 * r, O + cy - 1 - n - 8)))
    coarse_sweeps(coarse, c, mask, cx, cy, every(cy + 2 * O), tiles)
    add = prolong_add(c3, fine, smooth, stage, cx, cy, cz, range(0, cy, 8), range(4, cy - 4, 8))
    write_out(add, stage, out, sems, cx, [(8, 2 * cy - 16)])


def finish_outer_body(cx, cy, cz, nin, *refs):
    halo = refs[:nin]
    smooth, coarse = refs[nin], refs[nin + 7]
    c = refs[nin + 8:nin + 12]
    out = refs[nin + 12]
    mask, fine, stage, sems = refs[nin + 13:]
    ct = cz // LANES
    xe, ye = cx + 2 * O, cy + 2 * O

    def read(t, q):
        return coarse[t, pl.ds(q + O, xe, stride=ye), :]

    def write(t, q, value):
        coarse[t, pl.ds(q + O, xe, stride=ye), :] = value

    place_faces(halo, "gy", ct, cy, read, write)
    fill_mask(mask, cy)
    both = (2, lambda r: pl.multiple_of(r * cy, 8))
    coarse_sweeps(coarse, c, mask, cx, cy, both, [both] * 3)
    add = prolong_add(c[3], fine, smooth, stage, cx, cy, cz, (0, cy - 1), (0, cy - 8))
    write_out(add, stage, out, sems, cx, [(0, 8), (2 * cy - 8, 8)])


def on_device(start, right):
    nx, ny, nz = start.shape
    nt = nz // LANES
    xe, ye = nx + 2 * O, ny + 2 * O
    cx, cy, cz = nx // 2, ny // 2, nz // 2
    ct = cz // LANES
    cxe, cye = cx + 2 * O, cy + 2 * O
    big = f32(nt + 1, xe * ye, LANES)
    mb = 1 << 20

    msgs = call(
        xpack_body, "xpack", [start[:F], right[:G], start[nx - F:], right[nx - G:]],
        [f32(SLOT, ny, nz)] * count("gx"), limit=4 * mb, cost=9e9,
    )
    halo = exchange(msgs, "gx")
    face = [f32(-(-xe // PER), ny, LANES)] * count("gz")
    se, re, *msgs = call(build_body, "build", [start, right], [big, big] + face, limit=8 * mb)

    xhalo, n = halo, len(halo)
    msgs = call(
        functools.partial(xhalo_body, nx, ny, nz, n), "xhalo", [*xhalo, *msgs],
        face, alias={n + i: i for i in range(len(msgs))}, limit=8 * mb,
    )
    halo = exchange(msgs, "gz")
    yface = [f32(SLOT * nt + 1, xe, LANES)] * count("gy")
    se, re, *msgs = call(
        functools.partial(middle_body, nx, ny, nz, n), "middle", [*xhalo, se, re],
        [big, big] + yface, alias={n: 0, n + 1: 1}, limit=8 * mb, cost=2e9,
    )
    n = len(halo)
    se, re, *msgs = call(
        functools.partial(zhalo_body, nx, ny, nz, n), "zhalo", [*halo, se, re, *msgs],
        [big, big] + yface, alias={n + i: i for i in range(2 + len(msgs))}, limit=8 * mb,
    )
    halo = exchange(msgs, "gy")
    part = f32(nt, (cx + 1) * ny + 8, LANES)
    masks = pltpu.VMEM((nt + 1, ye, LANES), jnp.float32)
    s1, s2, rx = call(
        functools.partial(inner_body, nx, ny, nz), "inner", [se, re], [big, big, part], scratch=[masks],
        limit=8 * mb, cost=9e9,
    )
    n = len(halo)
    small = f32(ct + 1, cxe * cye, LANES)
    se, re, s1, s2, rx, coarse, *msgs = call(
        functools.partial(outer_body, nx, ny, nz, n), "outer", [*halo, se, re, s1, s2, rx],
        [big, big, big, big, part, small] + [f32(CL * ct + 1, cye, LANES)] * count(RING),
        scratch=[pltpu.VMEM((nt, (cx + 1) * cye, LANES), jnp.float32), masks],
        alias={n + i: i for i in range(5)}, limit=8 * mb,
    )
    halo = exchange(msgs, RING)
    rx, coarse = call(
        functools.partial(rest_body, nx, ny, nz), "rest", [rx, coarse], [part, small],
        scratch=[pltpu.VMEM((nt, (cx + 1) * cye, LANES), jnp.float32)], alias={0: 0, 1: 1}, limit=8 * mb, cost=2e9,
    )
    n = len(halo)
    coarse, *msgs = call(
        functools.partial(coarse_x_body, cx, cy, cz, n), "coarse_x", [*halo, coarse],
        [small] + [f32(-(-(cx + CL + CH) // CPER), cye, LANES)] * count("gz"), alias={n: 0}, limit=8 * mb,
    )
    halo = exchange(msgs, "gz")
    n = len(halo)
    coarse, *msgs = call(
        functools.partial(coarse_z_body, cx, cy, cz, n), "coarse_z", [*halo, coarse],
        [small] + [f32(CL * ct + 1, cxe, LANES)] * count("gy"), alias={n: 0}, limit=8 * mb,
    )
    halo = exchange(msgs, "gy")
    n = len(halo)
    stage = [
        pltpu.VMEM((ct + 1, cye, LANES), jnp.float32),
        pltpu.VMEM((nt, (cx + 1) * cye, LANES), jnp.float32),
        pltpu.VMEM((nt, nx, ny, LANES), jnp.float32),
    ]
    *c, out = call(
        functools.partial(finish_inner_body, cx, cy, cz), "finish_inner", [s2, coarse],
        [small] * 4 + [f32(nx, ny, nz)], scratch=stage + [pltpu.SemaphoreType.DMA((8, nt))],
        limit=10 * mb, out_specs=[VMEM] * 4 + [ANY], cost=5e9,
    )
    *_, out = call(
        functools.partial(finish_outer_body, cx, cy, cz, n), "finish_outer", [*halo, s2, coarse, *c, out],
        [small] * 5 + [f32(nx, ny, nz)], scratch=stage + [pltpu.SemaphoreType.DMA((2, 2 * nt))],
        alias={n + 1 + i: i for i in range(6)}, limit=10 * mb,
        in_specs=[VMEM] * (n + 6) + [ANY], out_specs=[VMEM] * 5 + [ANY],
    )
    return out


def solution(mesh):
    spec = P("gx", "gy", "gz")
    return jax.shard_map(on_device, mesh=mesh, in_specs=(spec, spec), out_specs=spec, check_vma=False)
```

```python
import functools

import jax
import jax.numpy as jnp
from jax import lax
from jax.experimental import pallas as pl
from jax.experimental.pallas import tpu as pltpu
from jax.sharding import PartitionSpec as P

LANES = 128
O = 4
F = 3
G = 2
SLOT = F + G
PER = LANES // SLOT
CL = 4
CH = 3
CPER = LANES // CL

VMEM = pl.BlockSpec(memory_space=pltpu.VMEM)
ANY = pl.BlockSpec(memory_space=pl.ANY)


def f32(*shape):
    return jax.ShapeDtypeStruct(shape, jnp.float32)


def call(body, name, ins, outs, scratch=(), alias=None, limit=None, out_specs=None, cost=1e8,
         in_specs=None):
    return pl.pallas_call(
        body,
        name=name,
        in_specs=[VMEM] * len(ins) if in_specs is None else in_specs,
        out_specs=[VMEM] * len(outs) if out_specs is None else out_specs,
        out_shape=outs,
        scratch_shapes=list(scratch),
        input_output_aliases=alias or {},
        cost_estimate=pl.CostEstimate(flops=int(cost), bytes_accessed=0, transcendentals=0),
        compiler_params=pltpu.CompilerParams(vmem_limit_bytes=limit),
    )(*ins)


def iota(shape, dim):
    return lax.broadcasted_iota(jnp.int32, shape, dim)


RING = "gx/ring"


def size_of(axis):
    return lax.axis_size(axis.split("/")[0])


def ends(axis):
    i = lax.axis_index(axis.split("/")[0])
    return i == 0, i == size_of(axis) - 1


def paired(axis):
    return axis != RING


def exchange(msgs, axis):
    n = size_of(axis)
    if not paired(axis):
        axis = axis.split("/")[0]
        down = lax.ppermute(msgs[0], axis, [(i, (i - 1) % n) for i in range(n)])
        up = lax.ppermute(msgs[1], axis, [(i, (i + 1) % n) for i in range(n)])
        return [down, up]
    found = [None] * len(msgs)
    for phase in reversed(range(len(msgs))):
        routes = []
        for i in range(phase, n - 1, 2):
            routes += [(i, i + 1), (i + 1, i)]
        found[phase] = lax.ppermute(msgs[phase], axis, routes)
    return found


def emit(outs, index, axis, low, high):
    if isinstance(outs, Kept):
        outs.lows.append(low())
        outs.highs.append(high())
    elif paired(axis):
        even = lax.axis_index(axis) % 2 == 0
        low, high = low(), high()
        outs[0][index] = jnp.where(even, high, low)
        if len(outs) > 1:
            outs[1][index] = jnp.where(even, low, high)
    else:
        outs[0][index] = low()
        outs[1][index] = high()


def arrived(refs, index, axis):
    a = refs[0][index]
    b = refs[1][index] if len(refs) > 1 else jnp.zeros_like(a)
    if paired(axis):
        even = lax.axis_index(axis) % 2 == 0
        return jnp.where(even, a, b), jnp.where(even, b, a)
    first, last = ends(axis)
    return jnp.where(last, 0.0, a), jnp.where(first, 0.0, b)


def written(outs, index, axis):
    a = outs[0][index]
    b = outs[1][index] if len(outs) > 1 else jnp.zeros_like(a)
    if paired(axis):
        even = lax.axis_index(axis) % 2 == 0
        return jnp.where(even, a, b), jnp.where(even, b, a)
    return b, a


def count(axis):
    return 1 if paired(axis) and size_of(axis) == 2 else 2


def loop(many, body, most=5):
    if many <= most:
        for r in range(many):
            body(r, 0)
    else:
        unroll = max(u for u in range(1, most + 1) if many % u == 0)
        lax.fori_loop(0, many, body, 0, unroll=unroll)


def turn(value, lanes):
    return pltpu.roll(value, lanes % LANES, 1)


def xpack_body(*refs):
    joined, *outs = refs
    for k in range(SLOT):
        emit(outs, (k,), "gx", lambda: joined[k], lambda: joined[SLOT + k])


def pack(outs, at_row, group, planes, load, partial):
    lane = iota((8, LANES), 1)
    low, high = partial
    done = None
    wrapped = None
    for q in planes:
        at = (q - group * PER) * SLOT
        s_low, s_high, r_low, r_high = load(q)
        one = turn(jnp.where(lane < 64, s_low, r_high), at + G)
        two = turn(jnp.where(lane < 64, r_low, s_high), at)
        start_at = lane >= at
        start_g = lane >= at + G
        if done is not None and done != q - 1:
            raise ValueError("planes")
        low = jnp.where(start_g, one, jnp.where(start_at, two, low))
        if at == 0:
            wrapped = two
            high = jnp.where(start_at, one, high)
        else:
            high = jnp.where(start_at, one, jnp.where(lane >= at - F, two, high))
        done = q
    if wrapped is not None:
        high = jnp.where(lane >= LANES - F, wrapped, high)
    if planes:
        emit(outs, (group, pl.ds(at_row, 8)), "gz", lambda: low, lambda: high)


def build_body(start, right, se, re, *outs):
    nx, ny, nz = start.shape
    xe, ye = nx + 2 * O, ny + 2 * O
    nt = nz // LANES

    def rows(r, _):
        at = pl.multiple_of(r * 8, 8)
        zero = jnp.zeros((8, LANES), jnp.float32)

        def load(q):
            found = {}
            for t in range(nt):
                for key, src, dst in (("s", start, se), ("r", right, re)):
                    value = src[q - O, pl.ds(at, 8), t * LANES:(t + 1) * LANES]
                    dst[t, pl.ds(q * ye + at + O, 8), :] = value
                    found[key, t] = value
            return found["s", 0], found["s", nt - 1], found["r", 0], found["r", nt - 1]

        for group in range(-(-xe // PER)):
            planes = range(max(O, group * PER), min(O + nx, (group + 1) * PER))
            pack(outs, at, group, planes, load, (zero, zero))
        return 0

    loop(ny // 8, rows)


def xhalo_body(nx, ny, nz, nin, *refs):
    halo = refs[:nin]
    outs = refs[nin + count("gz"):]
    xe = nx + 2 * O
    first, final = slice(0, LANES), slice(nz - LANES, nz)
    lane = iota((8, LANES), 1)

    def rows(r, _):
        at = pl.multiple_of(r * 8, 8)

        def load(q):
            after = q >= O
            s_layer = q - O - nx if after else q - O + F
            r_layer = F + (min(q - O - nx, G - 1) if after else max(q - O + G, 0))

            def get(layer, cut):
                high, low = arrived(halo, (layer, pl.ds(at, 8), cut), "gx")
                return high if after else low

            return get(s_layer, first), get(s_layer, final), get(r_layer, first), get(r_layer, final)

        for group in range(-(-xe // PER)):
            span = range(group * PER, min(xe, (group + 1) * PER))
            before = [q for q in span if O - F <= q < O]
            after = [q for q in span if O + nx <= q < O + nx + F]
            if not before and not after:
                continue
            core_high, core_low = written(outs, (group, pl.ds(at, 8)), "gz")
            lows, highs = [], []
            pack(Kept(lows, highs), at, group, before, load, (core_low, core_high))
            if before:
                top = (O - group * PER) * SLOT
                low = jnp.where(lane < top, lows[0], core_low)
                high = jnp.where((lane < top - F) | (lane >= LANES - F), highs[0], core_high)
                core_low, core_high = low, high
            if after:
                lows, highs = [], []
                pack(Kept(lows, highs), at, group, after, load, (core_low, core_high))
                core_low, core_high = lows[0], jnp.where(lane >= LANES - F, core_high, highs[0])
            emit(outs, (group, pl.ds(at, 8)), "gz", lambda: core_low, lambda: core_high)
        return 0

    loop(ny // 8, rows)


class Kept:
    def __init__(self, lows, highs):
        self.lows, self.highs = lows, highs


def middle_body(nx, ny, nz, nin, *refs):
    halo = refs[:nin]
    se, re, outs = refs[nin + 2], refs[nin + 3], refs[nin + 4:]
    xe, ye = nx + 2 * O, ny + 2 * O
    nt = nz // LANES
    for t in range(nt):
        cut = slice(t * LANES, (t + 1) * LANES)
        for k in range(SLOT):
            high, low = arrived(halo, (k, slice(None), cut), "gx")
            dst, size, j = (se, F, k) if k < F else (re, G, k - F)
            dst[t, pl.ds((O + nx + j) * ye + O, ny), :] = high
            dst[t, pl.ds((O - size + j) * ye + O, ny), :] = low
    for k in range(SLOT):
        src, size, j = (se, F, k) if k < F else (re, G, k - F)
        for t in range(nt):
            emit(
                outs, (k * nt + t,), "gy",
                lambda: src[t, pl.ds(O + j, xe, stride=ye), :],
                lambda: src[t, pl.ds(O + ny - size + j, xe, stride=ye), :],
            )


def zhalo_body(nx, ny, nz, nin, *refs):
    halo = refs[:nin]
    outs = refs[nin + 2 + count("gy"):]
    se, re, outs = outs[0], outs[1], outs[2:]
    xe, ye = nx + 2 * O, ny + 2 * O
    nt = nz // LANES
    lane = iota((8, LANES), 1)

    def unpack(r, _):
        at_row = pl.multiple_of(r * 8, 8)
        for group in range(-(-xe // PER)):
            high, low = arrived(halo, (group, pl.ds(at_row, 8)), "gz")
            pick = lane % SLOT < G
            one = jnp.where(pick, high, low)
            two = jnp.where(pick, low, high)
            one = jnp.where(lane >= LANES - F, low, one)
            for j in range(min(PER, xe - group * PER)):
                a = turn(one, -j * SLOT)
                b = turn(two, -j * SLOT - G)
                here = pl.ds((group * PER + j) * ye + at_row + O, 8)
                se[nt, here, :] = jnp.where(lane < 64, b, a)
                re[nt, here, :] = jnp.where(lane < 64, a, b)
        return 0

    loop(ny // 8, unpack)
    lane = iota((xe, LANES), 1)
    extra_low = extra_high = jnp.zeros((xe, LANES), jnp.float32)
    for k in range(SLOT):
        src, size, j = (se, F, k) if k < F else (re, G, k - F)
        low = src[nt, pl.ds(O + j, xe, stride=ye), :]
        high = src[nt, pl.ds(O + ny - size + j, xe, stride=ye), :]
        here = (lane >= 8 * k) & (lane < 8 * k + 2 * F)
        extra_low = jnp.where(here, turn(low, 8 * k + F), extra_low)
        extra_high = jnp.where(here, turn(high, 8 * k + F), extra_high)
    emit(outs, (SLOT * nt,), "gy", lambda: extra_low, lambda: extra_high)


def place_y(halo, se, re, nx, ny):
    xe, ye = nx + 2 * O, ny + 2 * O
    nt = se.shape[0] - 1
    for k in range(SLOT):
        dst, size, j = (se, F, k) if k < F else (re, G, k - F)
        for t in range(nt + 1):
            if t < nt:
                high, low = arrived(halo, (k * nt + t,), "gy")
            else:
                high, low = (turn(v, -8 * k - F) for v in arrived(halo, (SLOT * nt,), "gy"))
            dst[t, pl.ds(O + ny + j, xe, stride=ye), :] = high
            dst[t, pl.ds(O - size + j, xe, stride=ye), :] = low


def inside(shape, dim, offset, cells, axis):
    first, last = ends(axis)
    at = iota(shape, dim) - offset
    up = jnp.where(last, 0.0, 1.0)
    down = jnp.where(first, 0.0, 1.0)
    return jnp.where(at < 0, down, jnp.where(at < cells, 1.0, up))


def fill_mask(mask, ny):
    total, ye, _ = mask.shape
    valid = inside((ye, LANES), 0, O, ny, "gy") * (1.0 / 7.0)
    for t in range(total - 1):
        mask[t] = valid
    first, last = ends("gz")
    lane = iota((ye, LANES), 1)
    mask[total - 1] = valid * jnp.where(
        lane < CH, jnp.where(last, 0.0, 1.0), jnp.where(lane >= LANES - CL, jnp.where(first, 0.0, 1.0), 0.0)
    )


def stencil(ref, ye, base, planes, tiles, use):
    total = ref.shape[0]
    lane = iota((8, LANES), 1)

    def at(p, t, shift=0):
        return ref[t, pl.ds((p + O) * ye + base + shift, 8), :]

    before = [at(planes[0] - 1, t) for t in range(tiles)]
    centre = [at(planes[0], t) for t in range(total)]
    for p in planes:
        after = [at(p + 1, t) for t in range(total)]
        for t in range(tiles):
            wrapped = jnp.where(lane == LANES - 1, centre[t - 1], centre[t])
            near = turn(wrapped, 1)
            wrapped = jnp.where(lane == 0, centre[(t + 1) % total], centre[t])
            near = near + turn(wrapped, -1)
            near = near + (at(p, t, -1) + at(p, t, 1))
            near = near + (before[t] + after[t])
            use(p, t, centre[t], near)
        before, centre = centre, after


def sweep(src, dst, right, mask, nx, low, high, tiles):
    total, ye, _ = mask.shape
    first, last = ends("gx")
    up = jnp.where(last, 0.0, 1.0)
    down = jnp.where(first, 0.0, 1.0)

    def rows(r, _):
        base = tiles[1](r)
        m = [mask[t, pl.ds(base, 8), :] for t in range(total)]

        def use(p, t, centre, near):
            here = pl.ds((p + O) * ye + base, 8)
            factor = m[t] * down if p < 0 else m[t] * up if p >= nx else m[t]
            dst[t, here, :] = factor * (near + (centre + right[t, here, :]))

        stencil(src, ye, base, range(-low, nx + high), total, use)
        return 0

    loop(tiles[0], rows, 4)


def residual_x(s2, re, rx, nx, ny, tiles):
    ye = ny + 2 * O

    def rows(r, _):
        base = tiles[1](r)
        at = base - O
        quarter, half = {}, {}

        def use(p, t, centre, near):
            value = (near + re[t, pl.ds((p + O) * ye + base, 8), :]) - 6.0 * centre
            if p % 2:
                half[t] = 0.5 * value
                if p == nx - 1:
                    rx[t, pl.ds((nx // 2) * ny + at, 8), :] = quarter[t] + half[t]
                return
            value = 0.25 * value
            part = value if p == 0 else (quarter[t] + half[t]) + value
            rx[t, pl.ds((p // 2) * ny + at, 8), :] = part
            quarter[t] = value

        stencil(s2, ye, base, range(nx), rx.shape[0], use)
        return 0

    loop(tiles[0], rows, 4)


def every(ye):
    return ye // 8, lambda r: pl.multiple_of(r * 8, 8)


def split_dot(value, weight):
    high = value.astype(jnp.bfloat16)
    rest = value - high.astype(jnp.float32)
    mid = rest.astype(jnp.bfloat16)
    small = (rest - mid.astype(jnp.float32)).astype(jnp.bfloat16)
    dot = functools.partial(jnp.dot, preferred_element_type=jnp.float32)
    return dot(high, weight) + dot(mid, weight) + dot(small, weight)


def lane_dot(src, src_at, dst, dst_at, rows, weight):
    step = max(s for s in range(8, 273, 8) if rows % s == 0)
    for at in range(0, rows, step):
        value = jnp.concatenate([src[t, pl.ds(src_at + at, step), :] for t in range(weight.shape[0] // LANES)], axis=1)
        got = split_dot(value, weight)
        for t in range(weight.shape[1] // LANES):
            dst[t, pl.ds(dst_at + at, step), :] = got[:, t * LANES:(t + 1) * LANES]


def transfer_weights(fine, coarse, halo, fine_dim, inner, outer):
    shape = (fine, coarse + halo) if fine_dim == 0 else (coarse + halo, fine)
    z = iota(shape, fine_dim)
    k = iota(shape, 1 - fine_dim)
    k = jnp.where(k >= coarse, k - (coarse + halo), k)
    off = z - 2 * k
    weight = jnp.where(off == 1, inner, jnp.where((off == 0) | (off == 2), outer, 0.0))
    return jnp.where(k < -1, 0.0, weight).astype(jnp.bfloat16)


def inner_body(nx, ny, nz, se, re, s1, s2, rx, mask):
    fill_mask(mask, ny)
    many = ny // 8 - 1
    sweep(se, s1, re, mask, nx, 2, 2, (many, lambda r: pl.multiple_of(r * 8 + 8, 8)))
    sweep(s1, s2, re, mask, nx, 1, 1, (many, lambda r: jnp.minimum(r * 8 + 9, ny - 9)))
    residual_x(s2, re, rx, nx, ny, (many, lambda r: O + jnp.minimum(r * 8 + 6, ny - 14)))


def outer_body(nx, ny, nz, nin, *refs):
    halo = refs[:nin]
    se, re, s1, s2, rx, coarse = refs[nin + 5:nin + 11]
    outs = refs[nin + 11:-2]
    ry, mask = refs[-2:]
    nt = nz // LANES
    place_y(halo, se, re, nx, ny)
    fill_mask(mask, ny)
    sweep(se, s1, re, mask, nx, 2, 2, (2, lambda r: pl.multiple_of(r * ny, 8)))
    sweep(s1, s2, re, mask, nx, 1, 1, (2, lambda r: r * (ny - 2) + 1))
    residual_x(s2, re, rx, nx, ny, (2, lambda r: O + r * (ny - 8)))

    cx, cy, cz = nx // 2, ny // 2, nz // 2
    ct = cz // LANES
    cye = cy + 2 * O
    restrict_yz(rx, ry, coarse, ny, cx, cz, [(0, CL), (cx + 1 - CL, CL)])
    faces(
        outs, RING,
        lambda t, j: coarse[t, pl.ds((O - 1 + j) * cye, cye), :],
        lambda t, j: coarse[t, pl.ds((cx + j) * cye, cye), :],
        ct,
    )


def restrict_yz(rx, ry, coarse, ny, cx, cz, spans):
    nt = rx.shape[0]
    nz = nt * LANES
    cy = ny // 2
    cye = cy + 2 * O
    row = iota((8, LANES), 0)
    zero = jnp.zeros((8, LANES), jnp.float32)
    weight = transfer_weights(nz, cz, LANES, 0, 2.0, 1.0)

    def restrict_y(i, _):
        for t in range(nt):
            for k in range(cy // 8):
                at = i * ny + 16 * k
                even = 0.25 * rx[t, pl.ds(at, 8, stride=2), :]
                odd = 0.5 * rx[t, pl.ds(at + 1, 8, stride=2), :]
                after = 0.25 * rx[t, pl.ds(at + 2, 8, stride=2), :]
                if k == cy // 8 - 1:
                    after = jnp.where(row == 7, 0.0, after)
                if k == 0:
                    ry[t, pl.ds(i * cye, 8), :] = jnp.where(row == O - 1, even[0:1], 0.0)
                    ry[t, pl.ds(i * cye + cy, 8), :] = zero
                ry[t, pl.ds(i * cye + O + 8 * k, 8), :] = (even + odd) + after
        return 0

    for t in range(nt):
        rx[t, pl.ds((cx + 1) * ny, 8), :] = zero
    for first, many in spans:
        unroll = max(u for u in (5, 4, 3, 2, 1) if many % u == 0)
        lax.fori_loop(first, first + many, restrict_y, 0, unroll=unroll)
        lane_dot(ry, first * cye, coarse, (O - 1 + first) * cye, many * cye, weight)


def rest_body(nx, ny, nz, rx, _, rx_out, coarse, ry):
    cx = nx // 2
    restrict_yz(rx_out, ry, coarse, ny, cx, nz // 2, [(CL, cx + 1 - 2 * CL)])
    ct = coarse.shape[0] - 1
    cye = ny // 2 + 2 * O
    for t in range(ct + 1):
        coarse[t, pl.ds((cx + 2 * O - 1) * cye, cye), :] = jnp.zeros((cye, LANES), jnp.float32)


def pack_coarse(outs, coarse, cx, cy):
    ct = coarse.shape[0] - 1
    ye = cy + 2 * O
    lane = iota((8, LANES), 1)

    def rows(r, _):
        base = pl.multiple_of(r * 8, 8)
        for group in range(-(-(cx + CL + CH) // CPER)):
            low = high = None
            for j in range(min(CPER, cx + CL + CH - group * CPER)):
                at = j * CL
                rows8 = pl.ds((group * CPER + j) * ye + base, 8)
                head = jnp.where(lane < CL - 1, coarse[0, rows8, :], coarse[ct, rows8, :])
                head = turn(head, at + 1)
                tail = turn(coarse[ct - 1, rows8, :], at + CL)
                low = head if low is None else jnp.where(lane >= at, head, low)
                high = tail if high is None else jnp.where(lane >= at, tail, high)
            emit(outs, (group, pl.ds(base, 8)), "gz", lambda: low, lambda: high)
        return 0

    loop(ye // 8, rows)


def faces(outs, axis, low, high, ct):
    extra_low = extra_high = None
    for j in range(CL):
        for t in range(ct):
            emit(outs, (j * ct + t,), axis, lambda: low(t, j), lambda: high(t, j))
        a = turn(low(ct, j), 8 * j + CL)
        b = turn(high(ct, j), 8 * j + CL)
        lane = iota(a.shape, 1)
        extra_low = a if j == 0 else jnp.where(lane >= 8 * j, a, extra_low)
        extra_high = b if j == 0 else jnp.where(lane >= 8 * j, b, extra_high)
    emit(outs, (CL * ct,), axis, lambda: extra_low, lambda: extra_high)


def place_faces(refs, axis, ct, size, read, write):
    for t in range(ct + 1):
        for j in range(CL):
            if t < ct:
                high, low = arrived(refs, (j * ct + t,), axis)
            else:
                high, low = arrived(refs, (CL * ct,), axis)
                lane = iota(high.shape, 1)
                used = (lane < CH) | (lane >= LANES - CL)
                high = jnp.where(used, turn(high, -8 * j - CL), 0.0)
                low = jnp.where(used, turn(low, -8 * j - CL), 0.0)
            q = size - 1 + j
            write(t, q, read(t, q) + high if j == 0 else high)
            q = j - CL
            write(t, q, read(t, q) + low if j == CL - 1 else low)


def coarse_z_body(cx, cy, cz, nin, *refs):
    halo = refs[:nin]
    coarse, outs = refs[nin + 1], refs[nin + 2:]
    ct = cz // LANES
    xe, ye = cx + 2 * O, cy + 2 * O
    lane = iota((8, LANES), 1)

    def unpack(r, _):
        base = pl.multiple_of(r * 8, 8)
        for group in range(-(-(cx + CL + CH) // CPER)):
            high, low = arrived(halo, (group, pl.ds(base, 8)), "gz")
            for j in range(min(CPER, cx + CL + CH - group * CPER)):
                here = pl.ds((group * CPER + j) * ye + base, 8)
                fromhigh = turn(high, -j * CL - 1)
                fromlow = turn(low, -j * CL - CL)
                edge = lane == LANES - 1
                tail = coarse[ct - 1, here, :]
                own = coarse[ct, here, :]
                coarse[ct - 1, here, :] = tail + jnp.where(edge, fromhigh, 0.0)
                wing = jnp.where(lane < CH, fromhigh, jnp.where(lane >= LANES - CL, fromlow, 0.0))
                coarse[ct, here, :] = wing + jnp.where(edge, own, 0.0)
        return 0

    loop(ye // 8, unpack)
    faces(
        outs, "gy",
        lambda t, j: coarse[t, pl.ds(O - 1 + j, xe, stride=ye), :],
        lambda t, j: coarse[t, pl.ds(cy + j, xe, stride=ye), :],
        ct,
    )


def coarse_x_body(cx, cy, cz, nin, *refs):
    halo = refs[:nin]
    coarse, outs = refs[nin + 1], refs[nin + 2:]
    ct = cz // LANES
    xe, ye = cx + 2 * O, cy + 2 * O

    def read(t, q):
        return coarse[t, pl.ds((q + O) * ye, ye), :]

    def write(t, q, value):
        coarse[t, pl.ds((q + O) * ye, ye), :] = value

    place_faces(halo, RING, ct, cx, read, write)
    pack_coarse(outs, coarse, cx, cy)


def coarse_sweeps(coarse, c, mask, cx, cy, first, tiles):
    total, ye, _ = mask.shape
    begin, last = ends("gx")
    up = jnp.where(last, 0.0, 1.0)
    down = jnp.where(begin, 0.0, 1.0)

    def rows(r, _):
        base = first[1](r)
        m = [mask[t, pl.ds(base, 8), :] for t in range(total)]
        for q in range(cx + 2 * O - 1):
            here = pl.ds(q * ye + base, 8)
            for t in range(total):
                factor = m[t] * down if q < O else m[t] * up if q >= O + cx else m[t]
                c[0][t, here, :] = factor * coarse[t, here, :]
        return 0

    loop(first[0], rows)
    for n, (low, high) in enumerate(((3, 2), (2, 1), (1, 0))):
        sweep(c[n], c[n + 1], coarse, mask, cx, low, high, tiles[n])


def prolong_add(c, fine, smooth, stage, cx, cy, cz, pieces, tiles):
    ye = cy + 2 * O
    nx, ny, nz = 2 * cx, 2 * cy, 2 * cz
    nt = nz // LANES
    fye = ny + 2 * O
    weight = transfer_weights(nz, cz, LANES, 1, 1.0, 0.5)
    starts = [q * ye + piece for q in range(cx + 1) for piece in pieces]
    for at in range(0, len(starts), 33):
        some = starts[at:at + 33]
        wide = range(weight.shape[0] // LANES)
        value = jnp.concatenate(
            [
                jnp.concatenate([c[t, pl.ds((O - 1) * ye + s, 8), :] for s in some], axis=0)
                for t in wide
            ],
            axis=1,
        )
        got = split_dot(value, weight)
        for n, s in enumerate(some):
            for t in range(nt):
                fine[t, pl.ds(s, 8), :] = got[8 * n:8 * n + 8, t * LANES:(t + 1) * LANES]
    flat = stage.reshape(nt, nx * ny, LANES)

    def add(i, _):
        for t in range(nt):
            for row in tiles:
                at = (i + 1) * ye + O + row
                here = fine[t, pl.ds(at, 8), :]
                mid = 0.5 * (here + fine[t, pl.ds(at - 1, 8), :])
                before = fine[t, pl.ds(at - ye, 8), :]
                before_mid = 0.5 * (before + fine[t, pl.ds(at - ye - 1, 8), :])
                parts = (0.5 * (before_mid + mid), 0.5 * (before + here), mid, here)
                for n, part in enumerate(parts):
                    src = (2 * i + n // 2 + O) * fye + O + 2 * row + n % 2
                    dst = (2 * i + n // 2) * ny + 2 * row + n % 2
                    flat[t, pl.ds(dst, 8, stride=2), :] = smooth[t, pl.ds(src, 8, stride=2), :] + part
        return 0

    return add


def write_out(add, stage, out, sems, cx, spans):
    chunks = sems.shape[0]
    per = cx // chunks
    nt = stage.shape[0]

    def copies(c):
        at = c * 2 * per
        return [
            pltpu.make_async_copy(
                stage.at[t, pl.ds(at, 2 * per), pl.ds(row, many)],
                out.at[pl.ds(at, 2 * per), pl.ds(row, many), pl.ds(t * LANES, LANES)],
                sems.at[c, t * len(spans) + n],
            )
            for t in range(nt)
            for n, (row, many) in enumerate(spans)
        ]

    for c in range(chunks):
        unroll = max(u for u in (4, 2, 1) if per % u == 0)
        lax.fori_loop(c * per, (c + 1) * per, add, 0, unroll=unroll)
        for copy in copies(c):
            copy.start()
    for c in range(chunks):
        for copy in copies(c):
            copy.wait()


def finish_inner_body(cx, cy, cz, smooth, coarse, c0, c1, c2, c3, out, mask, fine, stage, sems):
    c = [c0, c1, c2, c3]
    fill_mask(mask, cy)
    tiles = []
    for n in (1, 2, 3):
        many = -(-(cy - 1 - 2 * n) // 8)
        tiles.append((many, lambda r, n=n: jnp.minimum(O + n + 8 * r, O + cy - 1 - n - 8)))
    coarse_sweeps(coarse, c, mask, cx, cy, every(cy + 2 * O), tiles)
    add = prolong_add(c3, fine, smooth, stage, cx, cy, cz, range(0, cy, 8), range(4, cy - 4, 8))
    write_out(add, stage, out, sems, cx, [(8, 2 * cy - 16)])


def finish_outer_body(cx, cy, cz, nin, *refs):
    halo = refs[:nin]
    smooth, coarse = refs[nin], refs[nin + 7]
    c = refs[nin + 8:nin + 12]
    out = refs[nin + 12]
    mask, fine, stage, sems = refs[nin + 13:]
    ct = cz // LANES
    xe, ye = cx + 2 * O, cy + 2 * O

    def read(t, q):
        return coarse[t, pl.ds(q + O, xe, stride=ye), :]

    def write(t, q, value):
        coarse[t, pl.ds(q + O, xe, stride=ye), :] = value

    place_faces(halo, "gy", ct, cy, read, write)
    fill_mask(mask, cy)
    both = (2, lambda r: pl.multiple_of(r * cy, 8))
    coarse_sweeps(coarse, c, mask, cx, cy, both, [both] * 3)
    add = prolong_add(c[3], fine, smooth, stage, cx, cy, cz, (0, cy - 1), (0, cy - 8))
    write_out(add, stage, out, sems, cx, [(0, 8), (2 * cy - 8, 8)])


def joined_faces(start, right):
    nx = start.shape[0]
    i = lax.broadcasted_iota(jnp.int32, (2 * SLOT, 1, 1), 0)
    z = jnp.float32(0)

    def put(v, first, many, at):
        return lax.pad(v, z, [(at - first, (2 * SLOT - at) - (nx - first), 0), (0, 0, 0), (0, 0, 0)])

    a = put(start, 0, F, 0)
    b = put(right, 0, G, F)
    c = put(start, nx - F, F, SLOT)
    d = put(right, nx - G, G, SLOT + F)
    return jnp.where(i < F, a, jnp.where(i < SLOT, b, jnp.where(i < SLOT + F, c, d)))


def on_device(start, right):
    nx, ny, nz = start.shape
    nt = nz // LANES
    xe, ye = nx + 2 * O, ny + 2 * O
    cx, cy, cz = nx // 2, ny // 2, nz // 2
    ct = cz // LANES
    cxe, cye = cx + 2 * O, cy + 2 * O
    big = f32(nt + 1, xe * ye, LANES)
    mb = 1 << 20

    msgs = call(
        xpack_body, "xpack", [joined_faces(start, right)],
        [f32(SLOT, ny, nz)] * count("gx"), limit=4 * mb, cost=9e9,
    )
    halo = exchange(msgs, "gx")
    face = [f32(-(-xe // PER), ny, LANES)] * count("gz")
    se, re, *msgs = call(build_body, "build", [start, right], [big, big] + face, limit=8 * mb)

    xhalo, n = halo, len(halo)
    msgs = call(
        functools.partial(xhalo_body, nx, ny, nz, n), "xhalo", [*xhalo, *msgs],
        face, alias={n + i: i for i in range(len(msgs))}, limit=8 * mb,
    )
    halo = exchange(msgs, "gz")
    yface = [f32(SLOT * nt + 1, xe, LANES)] * count("gy")
    se, re, *msgs = call(
        functools.partial(middle_body, nx, ny, nz, n), "middle", [*xhalo, se, re],
        [big, big] + yface, alias={n: 0, n + 1: 1}, limit=8 * mb, cost=2e9,
    )
    n = len(halo)
    se, re, *msgs = call(
        functools.partial(zhalo_body, nx, ny, nz, n), "zhalo", [*halo, se, re, *msgs],
        [big, big] + yface, alias={n + i: i for i in range(2 + len(msgs))}, limit=8 * mb,
    )
    halo = exchange(msgs, "gy")
    part = f32(nt, (cx + 1) * ny + 8, LANES)
    masks = pltpu.VMEM((nt + 1, ye, LANES), jnp.float32)
    s1, s2, rx = call(
        functools.partial(inner_body, nx, ny, nz), "inner", [se, re], [big, big, part], scratch=[masks],
        limit=8 * mb, cost=9e9,
    )
    n = len(halo)
    small = f32(ct + 1, cxe * cye, LANES)
    se, re, s1, s2, rx, coarse, *msgs = call(
        functools.partial(outer_body, nx, ny, nz, n), "outer", [*halo, se, re, s1, s2, rx],
        [big, big, big, big, part, small] + [f32(CL * ct + 1, cye, LANES)] * count(RING),
        scratch=[pltpu.VMEM((nt, (cx + 1) * cye, LANES), jnp.float32), masks],
        alias={n + i: i for i in range(5)}, limit=8 * mb,
    )
    halo = exchange(msgs, RING)
    rx, coarse = call(
        functools.partial(rest_body, nx, ny, nz), "rest", [rx, coarse], [part, small],
        scratch=[pltpu.VMEM((nt, (cx + 1) * cye, LANES), jnp.float32)], alias={0: 0, 1: 1}, limit=8 * mb, cost=2e9,
    )
    n = len(halo)
    coarse, *msgs = call(
        functools.partial(coarse_x_body, cx, cy, cz, n), "coarse_x", [*halo, coarse],
        [small] + [f32(-(-(cx + CL + CH) // CPER), cye, LANES)] * count("gz"), alias={n: 0}, limit=8 * mb,
    )
    halo = exchange(msgs, "gz")
    n = len(halo)
    coarse, *msgs = call(
        functools.partial(coarse_z_body, cx, cy, cz, n), "coarse_z", [*halo, coarse],
        [small] + [f32(CL * ct + 1, cxe, LANES)] * count("gy"), alias={n: 0}, limit=8 * mb,
    )
    halo = exchange(msgs, "gy")
    n = len(halo)
    stage = [
        pltpu.VMEM((ct + 1, cye, LANES), jnp.float32),
        pltpu.VMEM((nt, (cx + 1) * cye, LANES), jnp.float32),
        pltpu.VMEM((nt, nx, ny, LANES), jnp.float32),
    ]
    *c, out = call(
        functools.partial(finish_inner_body, cx, cy, cz), "finish_inner", [s2, coarse],
        [small] * 4 + [f32(nx, ny, nz)], scratch=stage + [pltpu.SemaphoreType.DMA((8, nt))],
        limit=10 * mb, out_specs=[VMEM] * 4 + [ANY], cost=5e9,
    )
    *_, out = call(
        functools.partial(finish_outer_body, cx, cy, cz, n), "finish_outer", [*halo, s2, coarse, *c, out],
        [small] * 5 + [f32(nx, ny, nz)], scratch=stage + [pltpu.SemaphoreType.DMA((2, 2 * nt))],
        alias={n + 1 + i: i for i in range(6)}, limit=10 * mb,
        in_specs=[VMEM] * (n + 6) + [ANY], out_specs=[VMEM] * 5 + [ANY],
    )
    return out


def solution(mesh):
    spec = P("gx", "gy", "gz")
    return jax.shard_map(on_device, mesh=mesh, in_specs=(spec, spec), out_specs=spec, check_vma=False)
```

```python
import functools

import jax
import jax.numpy as jnp
from jax import lax
from jax.experimental import pallas as pl
from jax.experimental.pallas import tpu as pltpu
from jax.sharding import PartitionSpec as P

LANES = 128
O = 4
F = 3
G = 2
SLOT = F + G
PER = LANES // SLOT
CL = 4
CH = 3
CPER = LANES // CL

VMEM = pl.BlockSpec(memory_space=pltpu.VMEM)
ANY = pl.BlockSpec(memory_space=pl.ANY)


def f32(*shape):
    return jax.ShapeDtypeStruct(shape, jnp.float32)


def call(body, name, ins, outs, scratch=(), alias=None, limit=None, out_specs=None, cost=1e8,
         in_specs=None):
    return pl.pallas_call(
        body,
        name=name,
        in_specs=[VMEM] * len(ins) if in_specs is None else in_specs,
        out_specs=[VMEM] * len(outs) if out_specs is None else out_specs,
        out_shape=outs,
        scratch_shapes=list(scratch),
        input_output_aliases=alias or {},
        cost_estimate=pl.CostEstimate(flops=int(cost), bytes_accessed=0, transcendentals=0),
        compiler_params=pltpu.CompilerParams(vmem_limit_bytes=limit),
    )(*ins)


def iota(shape, dim):
    return lax.broadcasted_iota(jnp.int32, shape, dim)


RING = "gx/ring"


def size_of(axis):
    return lax.axis_size(axis.split("/")[0])


def ends(axis):
    i = lax.axis_index(axis.split("/")[0])
    return i == 0, i == size_of(axis) - 1


def paired(axis):
    return axis != RING


def exchange(msgs, axis):
    n = size_of(axis)
    if not paired(axis):
        axis = axis.split("/")[0]
        down = lax.ppermute(msgs[0], axis, [(i, (i - 1) % n) for i in range(n)])
        up = lax.ppermute(msgs[1], axis, [(i, (i + 1) % n) for i in range(n)])
        return [down, up]
    found = [None] * len(msgs)
    for phase in reversed(range(len(msgs))):
        routes = []
        for i in range(phase, n - 1, 2):
            routes += [(i, i + 1), (i + 1, i)]
        found[phase] = lax.ppermute(msgs[phase], axis, routes)
    return found


def emit(outs, index, axis, low, high):
    if isinstance(outs, Kept):
        outs.lows.append(low())
        outs.highs.append(high())
    elif paired(axis):
        even = lax.axis_index(axis) % 2 == 0
        low, high = low(), high()
        outs[0][index] = jnp.where(even, high, low)
        if len(outs) > 1:
            outs[1][index] = jnp.where(even, low, high)
    else:
        outs[0][index] = low()
        outs[1][index] = high()


def arrived(refs, index, axis):
    a = refs[0][index]
    b = refs[1][index] if len(refs) > 1 else jnp.zeros_like(a)
    if paired(axis):
        even = lax.axis_index(axis) % 2 == 0
        return jnp.where(even, a, b), jnp.where(even, b, a)
    first, last = ends(axis)
    return jnp.where(last, 0.0, a), jnp.where(first, 0.0, b)


def written(outs, index, axis):
    a = outs[0][index]
    b = outs[1][index] if len(outs) > 1 else jnp.zeros_like(a)
    if paired(axis):
        even = lax.axis_index(axis) % 2 == 0
        return jnp.where(even, a, b), jnp.where(even, b, a)
    return b, a


def count(axis):
    return 1 if paired(axis) and size_of(axis) == 2 else 2


def loop(many, body, most=5):
    if many <= most:
        for r in range(many):
            body(r, 0)
    else:
        unroll = max(u for u in range(1, most + 1) if many % u == 0)
        lax.fori_loop(0, many, body, 0, unroll=unroll)


def turn(value, lanes):
    return pltpu.roll(value, lanes % LANES, 1)


def xpack_body(*refs):
    joined, *outs = refs
    for k in range(SLOT):
        emit(outs, (k,), "gx", lambda: joined[k], lambda: joined[SLOT + k])


def pack(outs, at_row, group, planes, load, partial):
    lane = iota((8, LANES), 1)
    low, high = partial
    done = None
    wrapped = None
    for q in planes:
        at = (q - group * PER) * SLOT
        s_low, s_high, r_low, r_high = load(q)
        one = turn(jnp.where(lane < 64, s_low, r_high), at + G)
        two = turn(jnp.where(lane < 64, r_low, s_high), at)
        start_at = lane >= at
        start_g = lane >= at + G
        if done is not None and done != q - 1:
            raise ValueError("planes")
        low = jnp.where(start_g, one, jnp.where(start_at, two, low))
        if at == 0:
            wrapped = two
            high = jnp.where(start_at, one, high)
        else:
            high = jnp.where(start_at, one, jnp.where(lane >= at - F, two, high))
        done = q
    if wrapped is not None:
        high = jnp.where(lane >= LANES - F, wrapped, high)
    if planes:
        emit(outs, (group, pl.ds(at_row, 8)), "gz", lambda: low, lambda: high)


def build_body(start, right, se, re, *outs):
    nx, ny, nz = start.shape
    xe, ye = nx + 2 * O, ny + 2 * O
    nt = nz // LANES

    def rows(r, _):
        at = pl.multiple_of(r * 8, 8)
        zero = jnp.zeros((8, LANES), jnp.float32)

        def load(q):
            found = {}
            for t in range(nt):
                for key, src, dst in (("s", start, se), ("r", right, re)):
                    value = src[q - O, pl.ds(at, 8), t * LANES:(t + 1) * LANES]
                    dst[t, pl.ds(q * ye + at + O, 8), :] = value
                    found[key, t] = value
            return found["s", 0], found["s", nt - 1], found["r", 0], found["r", nt - 1]

        for group in range(-(-xe // PER)):
            planes = range(max(O, group * PER), min(O + nx, (group + 1) * PER))
            pack(outs, at, group, planes, load, (zero, zero))
        return 0

    loop(ny // 8, rows, 8)


def xhalo_body(nx, ny, nz, nin, *refs):
    halo = refs[:nin]
    outs = refs[nin + count("gz"):]
    xe = nx + 2 * O
    first, final = slice(0, LANES), slice(nz - LANES, nz)
    lane = iota((8, LANES), 1)

    def rows(r, _):
        at = pl.multiple_of(r * 8, 8)

        def load(q):
            after = q >= O
            s_layer = q - O - nx if after else q - O + F
            r_layer = F + (min(q - O - nx, G - 1) if after else max(q - O + G, 0))

            def get(layer, cut):
                high, low = arrived(halo, (layer, pl.ds(at, 8), cut), "gx")
                return high if after else low

            return get(s_layer, first), get(s_layer, final), get(r_layer, first), get(r_layer, final)

        for group in range(-(-xe // PER)):
            span = range(group * PER, min(xe, (group + 1) * PER))
            before = [q for q in span if O - F <= q < O]
            after = [q for q in span if O + nx <= q < O + nx + F]
            if not before and not after:
                continue
            core_high, core_low = written(outs, (group, pl.ds(at, 8)), "gz")
            lows, highs = [], []
            pack(Kept(lows, highs), at, group, before, load, (core_low, core_high))
            if before:
                top = (O - group * PER) * SLOT
                low = jnp.where(lane < top, lows[0], core_low)
                high = jnp.where((lane < top - F) | (lane >= LANES - F), highs[0], core_high)
                core_low, core_high = low, high
            if after:
                lows, highs = [], []
                pack(Kept(lows, highs), at, group, after, load, (core_low, core_high))
                core_low, core_high = lows[0], jnp.where(lane >= LANES - F, core_high, highs[0])
            emit(outs, (group, pl.ds(at, 8)), "gz", lambda: core_low, lambda: core_high)
        return 0

    loop(ny // 8, rows, 8)


class Kept:
    def __init__(self, lows, highs):
        self.lows, self.highs = lows, highs


def middle_body(nx, ny, nz, nin, *refs):
    halo = refs[:nin]
    se, re, outs = refs[nin + 2], refs[nin + 3], refs[nin + 4:]
    xe, ye = nx + 2 * O, ny + 2 * O
    nt = nz // LANES
    for t in range(nt):
        cut = slice(t * LANES, (t + 1) * LANES)
        for k in range(SLOT):
            high, low = arrived(halo, (k, slice(None), cut), "gx")
            dst, size, j = (se, F, k) if k < F else (re, G, k - F)
            dst[t, pl.ds((O + nx + j) * ye + O, ny), :] = high
            dst[t, pl.ds((O - size + j) * ye + O, ny), :] = low
    for k in range(SLOT):
        src, size, j = (se, F, k) if k < F else (re, G, k - F)
        for t in range(nt):
            emit(
                outs, (k * nt + t,), "gy",
                lambda: src[t, pl.ds(O + j, xe, stride=ye), :],
                lambda: src[t, pl.ds(O + ny - size + j, xe, stride=ye), :],
            )


def zhalo_body(nx, ny, nz, nin, *refs):
    halo = refs[:nin]
    outs = refs[nin + 2 + count("gy"):]
    se, re, outs = outs[0], outs[1], outs[2:]
    xe, ye = nx + 2 * O, ny + 2 * O
    nt = nz // LANES
    lane = iota((8, LANES), 1)

    def unpack(r, _):
        at_row = pl.multiple_of(r * 8, 8)
        for group in range(-(-xe // PER)):
            high, low = arrived(halo, (group, pl.ds(at_row, 8)), "gz")
            pick = lane % SLOT < G
            one = jnp.where(pick, high, low)
            two = jnp.where(pick, low, high)
            one = jnp.where(lane >= LANES - F, low, one)
            for j in range(min(PER, xe - group * PER)):
                a = turn(one, -j * SLOT)
                b = turn(two, -j * SLOT - G)
                here = pl.ds((group * PER + j) * ye + at_row + O, 8)
                se[nt, here, :] = jnp.where(lane < 64, b, a)
                re[nt, here, :] = jnp.where(lane < 64, a, b)
        return 0

    loop(ny // 8, unpack, 8)
    lane = iota((xe, LANES), 1)
    extra_low = extra_high = jnp.zeros((xe, LANES), jnp.float32)
    for k in range(SLOT):
        src, size, j = (se, F, k) if k < F else (re, G, k - F)
        low = src[nt, pl.ds(O + j, xe, stride=ye), :]
        high = src[nt, pl.ds(O + ny - size + j, xe, stride=ye), :]
        here = (lane >= 8 * k) & (lane < 8 * k + 2 * F)
        extra_low = jnp.where(here, turn(low, 8 * k + F), extra_low)
        extra_high = jnp.where(here, turn(high, 8 * k + F), extra_high)
    emit(outs, (SLOT * nt,), "gy", lambda: extra_low, lambda: extra_high)


def place_y(halo, se, re, nx, ny):
    xe, ye = nx + 2 * O, ny + 2 * O
    nt = se.shape[0] - 1
    for k in range(SLOT):
        dst, size, j = (se, F, k) if k < F else (re, G, k - F)
        for t in range(nt + 1):
            if t < nt:
                high, low = arrived(halo, (k * nt + t,), "gy")
            else:
                high, low = (turn(v, -8 * k - F) for v in arrived(halo, (SLOT * nt,), "gy"))
            dst[t, pl.ds(O + ny + j, xe, stride=ye), :] = high
            dst[t, pl.ds(O - size + j, xe, stride=ye), :] = low


def inside(shape, dim, offset, cells, axis):
    first, last = ends(axis)
    at = iota(shape, dim) - offset
    up = jnp.where(last, 0.0, 1.0)
    down = jnp.where(first, 0.0, 1.0)
    return jnp.where(at < 0, down, jnp.where(at < cells, 1.0, up))


def fill_mask(mask, ny):
    total, ye, _ = mask.shape
    valid = inside((ye, LANES), 0, O, ny, "gy") * (1.0 / 7.0)
    for t in range(total - 1):
        mask[t] = valid
    first, last = ends("gz")
    lane = iota((ye, LANES), 1)
    mask[total - 1] = valid * jnp.where(
        lane < CH, jnp.where(last, 0.0, 1.0), jnp.where(lane >= LANES - CL, jnp.where(first, 0.0, 1.0), 0.0)
    )


def stencil(ref, ye, base, planes, tiles, use):
    total = ref.shape[0]
    lane = iota((8, LANES), 1)

    def at(p, t, shift=0):
        return ref[t, pl.ds((p + O) * ye + base + shift, 8), :]

    before = [at(planes[0] - 1, t) for t in range(tiles)]
    centre = [at(planes[0], t) for t in range(total)]
    for p in planes:
        after = [at(p + 1, t) for t in range(total)]
        for t in range(tiles):
            wrapped = jnp.where(lane == LANES - 1, centre[t - 1], centre[t])
            near = turn(wrapped, 1)
            wrapped = jnp.where(lane == 0, centre[(t + 1) % total], centre[t])
            near = near + turn(wrapped, -1)
            near = near + (at(p, t, -1) + at(p, t, 1))
            near = near + (before[t] + after[t])
            use(p, t, centre[t], near)
        before, centre = centre, after


def sweep(src, dst, right, mask, nx, low, high, tiles):
    total, ye, _ = mask.shape
    first, last = ends("gx")
    up = jnp.where(last, 0.0, 1.0)
    down = jnp.where(first, 0.0, 1.0)

    def rows(r, _):
        base = tiles[1](r)
        m = [mask[t, pl.ds(base, 8), :] for t in range(total)]

        def use(p, t, centre, near):
            here = pl.ds((p + O) * ye + base, 8)
            factor = m[t] * down if p < 0 else m[t] * up if p >= nx else m[t]
            dst[t, here, :] = factor * (near + (centre + right[t, here, :]))

        stencil(src, ye, base, range(-low, nx + high), total, use)
        return 0

    loop(tiles[0], rows, 4)


def residual_x(s2, re, rx, nx, ny, tiles):
    ye = ny + 2 * O

    def rows(r, _):
        base = tiles[1](r)
        at = base - O
        quarter, half = {}, {}

        def use(p, t, centre, near):
            value = (near + re[t, pl.ds((p + O) * ye + base, 8), :]) - 6.0 * centre
            if p % 2:
                half[t] = 0.5 * value
                if p == nx - 1:
                    rx[t, pl.ds((nx // 2) * ny + at, 8), :] = quarter[t] + half[t]
                return
            value = 0.25 * value
            part = value if p == 0 else (quarter[t] + half[t]) + value
            rx[t, pl.ds((p // 2) * ny + at, 8), :] = part
            quarter[t] = value

        stencil(s2, ye, base, range(nx), rx.shape[0], use)
        return 0

    loop(tiles[0], rows, 4)


def every(ye):
    return ye // 8, lambda r: pl.multiple_of(r * 8, 8)


def split_dot(value, weight):
    high = value.astype(jnp.bfloat16)
    rest = value - high.astype(jnp.float32)
    mid = rest.astype(jnp.bfloat16)
    small = (rest - mid.astype(jnp.float32)).astype(jnp.bfloat16)
    dot = functools.partial(jnp.dot, preferred_element_type=jnp.float32)
    return dot(high, weight) + dot(mid, weight) + dot(small, weight)


def lane_dot(src, src_at, dst, dst_at, rows, weight):
    step = max(s for s in range(8, 273, 8) if rows % s == 0)
    for at in range(0, rows, step):
        value = jnp.concatenate([src[t, pl.ds(src_at + at, step), :] for t in range(weight.shape[0] // LANES)], axis=1)
        got = split_dot(value, weight)
        for t in range(weight.shape[1] // LANES):
            dst[t, pl.ds(dst_at + at, step), :] = got[:, t * LANES:(t + 1) * LANES]


def transfer_weights(fine, coarse, halo, fine_dim, inner, outer):
    shape = (fine, coarse + halo) if fine_dim == 0 else (coarse + halo, fine)
    z = iota(shape, fine_dim)
    k = iota(shape, 1 - fine_dim)
    k = jnp.where(k >= coarse, k - (coarse + halo), k)
    off = z - 2 * k
    weight = jnp.where(off == 1, inner, jnp.where((off == 0) | (off == 2), outer, 0.0))
    return jnp.where(k < -1, 0.0, weight).astype(jnp.bfloat16)


def inner_body(nx, ny, nz, se, re, s1, s2, rx, mask):
    fill_mask(mask, ny)
    many = ny // 8 - 1
    sweep(se, s1, re, mask, nx, 2, 2, (many, lambda r: pl.multiple_of(r * 8 + 8, 8)))
    sweep(s1, s2, re, mask, nx, 1, 1, (many, lambda r: jnp.minimum(r * 8 + 9, ny - 9)))
    residual_x(s2, re, rx, nx, ny, (many, lambda r: O + jnp.minimum(r * 8 + 6, ny - 14)))


def outer_body(nx, ny, nz, nin, *refs):
    halo = refs[:nin]
    se, re, s1, s2, rx, coarse = refs[nin + 5:nin + 11]
    outs = refs[nin + 11:-2]
    ry, mask = refs[-2:]
    nt = nz // LANES
    place_y(halo, se, re, nx, ny)
    fill_mask(mask, ny)
    sweep(se, s1, re, mask, nx, 2, 2, (2, lambda r: pl.multiple_of(r * ny, 8)))
    sweep(s1, s2, re, mask, nx, 1, 1, (2, lambda r: r * (ny - 2) + 1))
    residual_x(s2, re, rx, nx, ny, (2, lambda r: O + r * (ny - 8)))

    cx, cy, cz = nx // 2, ny // 2, nz // 2
    ct = cz // LANES
    cye = cy + 2 * O
    restrict_yz(rx, ry, coarse, ny, cx, cz, [(0, CL), (cx + 1 - CL, CL)])
    faces(
        outs, RING,
        lambda t, j: coarse[t, pl.ds((O - 1 + j) * cye, cye), :],
        lambda t, j: coarse[t, pl.ds((cx + j) * cye, cye), :],
        ct,
    )


def restrict_yz(rx, ry, coarse, ny, cx, cz, spans):
    nt = rx.shape[0]
    nz = nt * LANES
    cy = ny // 2
    cye = cy + 2 * O
    row = iota((8, LANES), 0)
    zero = jnp.zeros((8, LANES), jnp.float32)
    weight = transfer_weights(nz, cz, LANES, 0, 2.0, 1.0)

    def restrict_y(i, _):
        for t in range(nt):
            for k in range(cy // 8):
                at = i * ny + 16 * k
                even = 0.25 * rx[t, pl.ds(at, 8, stride=2), :]
                odd = 0.5 * rx[t, pl.ds(at + 1, 8, stride=2), :]
                after = 0.25 * rx[t, pl.ds(at + 2, 8, stride=2), :]
                if k == cy // 8 - 1:
                    after = jnp.where(row == 7, 0.0, after)
                if k == 0:
                    ry[t, pl.ds(i * cye, 8), :] = jnp.where(row == O - 1, even[0:1], 0.0)
                    ry[t, pl.ds(i * cye + cy, 8), :] = zero
                ry[t, pl.ds(i * cye + O + 8 * k, 8), :] = (even + odd) + after
        return 0

    for t in range(nt):
        rx[t, pl.ds((cx + 1) * ny, 8), :] = zero
    for first, many in spans:
        unroll = max(u for u in (5, 4, 3, 2, 1) if many % u == 0)
        lax.fori_loop(first, first + many, restrict_y, 0, unroll=unroll)
        lane_dot(ry, first * cye, coarse, (O - 1 + first) * cye, many * cye, weight)


def rest_body(nx, ny, nz, rx, _, rx_out, coarse, ry):
    cx = nx // 2
    restrict_yz(rx_out, ry, coarse, ny, cx, nz // 2, [(CL, cx + 1 - 2 * CL)])
    ct = coarse.shape[0] - 1
    cye = ny // 2 + 2 * O
    for t in range(ct + 1):
        coarse[t, pl.ds((cx + 2 * O - 1) * cye, cye), :] = jnp.zeros((cye, LANES), jnp.float32)


def pack_coarse(outs, coarse, cx, cy):
    ct = coarse.shape[0] - 1
    ye = cy + 2 * O
    lane = iota((8, LANES), 1)

    def rows(r, _):
        base = pl.multiple_of(r * 8, 8)
        for group in range(-(-(cx + CL + CH) // CPER)):
            low = high = None
            for j in range(min(CPER, cx + CL + CH - group * CPER)):
                at = j * CL
                rows8 = pl.ds((group * CPER + j) * ye + base, 8)
                head = jnp.where(lane < CL - 1, coarse[0, rows8, :], coarse[ct, rows8, :])
                head = turn(head, at + 1)
                tail = turn(coarse[ct - 1, rows8, :], at + CL)
                low = head if low is None else jnp.where(lane >= at, head, low)
                high = tail if high is None else jnp.where(lane >= at, tail, high)
            emit(outs, (group, pl.ds(base, 8)), "gz", lambda: low, lambda: high)
        return 0

    loop(ye // 8, rows)


def faces(outs, axis, low, high, ct):
    extra_low = extra_high = None
    for j in range(CL):
        for t in range(ct):
            emit(outs, (j * ct + t,), axis, lambda: low(t, j), lambda: high(t, j))
        a = turn(low(ct, j), 8 * j + CL)
        b = turn(high(ct, j), 8 * j + CL)
        lane = iota(a.shape, 1)
        extra_low = a if j == 0 else jnp.where(lane >= 8 * j, a, extra_low)
        extra_high = b if j == 0 else jnp.where(lane >= 8 * j, b, extra_high)
    emit(outs, (CL * ct,), axis, lambda: extra_low, lambda: extra_high)


def place_faces(refs, axis, ct, size, read, write):
    for t in range(ct + 1):
        for j in range(CL):
            if t < ct:
                high, low = arrived(refs, (j * ct + t,), axis)
            else:
                high, low = arrived(refs, (CL * ct,), axis)
                lane = iota(high.shape, 1)
                used = (lane < CH) | (lane >= LANES - CL)
                high = jnp.where(used, turn(high, -8 * j - CL), 0.0)
                low = jnp.where(used, turn(low, -8 * j - CL), 0.0)
            q = size - 1 + j
            write(t, q, read(t, q) + high if j == 0 else high)
            q = j - CL
            write(t, q, read(t, q) + low if j == CL - 1 else low)


def coarse_z_body(cx, cy, cz, nin, *refs):
    halo = refs[:nin]
    coarse, outs = refs[nin + 1], refs[nin + 2:]
    ct = cz // LANES
    xe, ye = cx + 2 * O, cy + 2 * O
    lane = iota((8, LANES), 1)

    def unpack(r, _):
        base = pl.multiple_of(r * 8, 8)
        for group in range(-(-(cx + CL + CH) // CPER)):
            high, low = arrived(halo, (group, pl.ds(base, 8)), "gz")
            for j in range(min(CPER, cx + CL + CH - group * CPER)):
                here = pl.ds((group * CPER + j) * ye + base, 8)
                fromhigh = turn(high, -j * CL - 1)
                fromlow = turn(low, -j * CL - CL)
                edge = lane == LANES - 1
                tail = coarse[ct - 1, here, :]
                own = coarse[ct, here, :]
                coarse[ct - 1, here, :] = tail + jnp.where(edge, fromhigh, 0.0)
                wing = jnp.where(lane < CH, fromhigh, jnp.where(lane >= LANES - CL, fromlow, 0.0))
                coarse[ct, here, :] = wing + jnp.where(edge, own, 0.0)
        return 0

    loop(ye // 8, unpack)
    faces(
        outs, "gy",
        lambda t, j: coarse[t, pl.ds(O - 1 + j, xe, stride=ye), :],
        lambda t, j: coarse[t, pl.ds(cy + j, xe, stride=ye), :],
        ct,
    )


def coarse_x_body(cx, cy, cz, nin, *refs):
    halo = refs[:nin]
    coarse, outs = refs[nin + 1], refs[nin + 2:]
    ct = cz // LANES
    xe, ye = cx + 2 * O, cy + 2 * O

    def read(t, q):
        return coarse[t, pl.ds((q + O) * ye, ye), :]

    def write(t, q, value):
        coarse[t, pl.ds((q + O) * ye, ye), :] = value

    place_faces(halo, RING, ct, cx, read, write)
    pack_coarse(outs, coarse, cx, cy)


def coarse_sweeps(coarse, c, mask, cx, cy, first, tiles):
    total, ye, _ = mask.shape
    begin, last = ends("gx")
    up = jnp.where(last, 0.0, 1.0)
    down = jnp.where(begin, 0.0, 1.0)

    def rows(r, _):
        base = first[1](r)
        m = [mask[t, pl.ds(base, 8), :] for t in range(total)]
        for q in range(cx + 2 * O - 1):
            here = pl.ds(q * ye + base, 8)
            for t in range(total):
                factor = m[t] * down if q < O else m[t] * up if q >= O + cx else m[t]
                c[0][t, here, :] = factor * coarse[t, here, :]
        return 0

    loop(first[0], rows)
    for n, (low, high) in enumerate(((3, 2), (2, 1), (1, 0))):
        sweep(c[n], c[n + 1], coarse, mask, cx, low, high, tiles[n])


def prolong_add(c, fine, smooth, stage, cx, cy, cz, pieces, tiles):
    ye = cy + 2 * O
    nx, ny, nz = 2 * cx, 2 * cy, 2 * cz
    nt = nz // LANES
    fye = ny + 2 * O
    weight = transfer_weights(nz, cz, LANES, 1, 1.0, 0.5)
    starts = [q * ye + piece for q in range(cx + 1) for piece in pieces]
    for at in range(0, len(starts), 33):
        some = starts[at:at + 33]
        wide = range(weight.shape[0] // LANES)
        value = jnp.concatenate(
            [
                jnp.concatenate([c[t, pl.ds((O - 1) * ye + s, 8), :] for s in some], axis=0)
                for t in wide
            ],
            axis=1,
        )
        got = split_dot(value, weight)
        for n, s in enumerate(some):
            for t in range(nt):
                fine[t, pl.ds(s, 8), :] = got[8 * n:8 * n + 8, t * LANES:(t + 1) * LANES]
    flat = stage.reshape(nt, nx * ny, LANES)

    def add(i, _):
        for t in range(nt):
            for row in tiles:
                at = (i + 1) * ye + O + row
                here = fine[t, pl.ds(at, 8), :]
                mid = 0.5 * (here + fine[t, pl.ds(at - 1, 8), :])
                before = fine[t, pl.ds(at - ye, 8), :]
                before_mid = 0.5 * (before + fine[t, pl.ds(at - ye - 1, 8), :])
                parts = (0.5 * (before_mid + mid), 0.5 * (before + here), mid, here)
                for n, part in enumerate(parts):
                    src = (2 * i + n // 2 + O) * fye + O + 2 * row + n % 2
                    dst = (2 * i + n // 2) * ny + 2 * row + n % 2
                    flat[t, pl.ds(dst, 8, stride=2), :] = smooth[t, pl.ds(src, 8, stride=2), :] + part
        return 0

    return add


def write_out(add, stage, out, sems, cx, spans):
    chunks = sems.shape[0]
    per = cx // chunks
    nt = stage.shape[0]

    def copies(c):
        at = c * 2 * per
        return [
            pltpu.make_async_copy(
                stage.at[t, pl.ds(at, 2 * per), pl.ds(row, many)],
                out.at[pl.ds(at, 2 * per), pl.ds(row, many), pl.ds(t * LANES, LANES)],
                sems.at[c, t * len(spans) + n],
            )
            for t in range(nt)
            for n, (row, many) in enumerate(spans)
        ]

    for c in range(chunks):
        unroll = max(u for u in (4, 2, 1) if per % u == 0)
        lax.fori_loop(c * per, (c + 1) * per, add, 0, unroll=unroll)
        for copy in copies(c):
            copy.start()
    for c in range(chunks):
        for copy in copies(c):
            copy.wait()


def finish_inner_body(cx, cy, cz, smooth, coarse, c0, c1, c2, c3, out, mask, fine, stage, sems):
    c = [c0, c1, c2, c3]
    fill_mask(mask, cy)
    tiles = []
    for n in (1, 2, 3):
        many = -(-(cy - 1 - 2 * n) // 8)
        tiles.append((many, lambda r, n=n: jnp.minimum(O + n + 8 * r, O + cy - 1 - n - 8)))
    coarse_sweeps(coarse, c, mask, cx, cy, every(cy + 2 * O), tiles)
    add = prolong_add(c3, fine, smooth, stage, cx, cy, cz, range(0, cy, 8), range(4, cy - 4, 8))
    write_out(add, stage, out, sems, cx, [(8, 2 * cy - 16)])


def finish_outer_body(cx, cy, cz, nin, *refs):
    halo = refs[:nin]
    smooth, coarse = refs[nin], refs[nin + 7]
    c = refs[nin + 8:nin + 12]
    out = refs[nin + 12]
    mask, fine, stage, sems = refs[nin + 13:]
    ct = cz // LANES
    xe, ye = cx + 2 * O, cy + 2 * O

    def read(t, q):
        return coarse[t, pl.ds(q + O, xe, stride=ye), :]

    def write(t, q, value):
        coarse[t, pl.ds(q + O, xe, stride=ye), :] = value

    place_faces(halo, "gy", ct, cy, read, write)
    fill_mask(mask, cy)
    both = (2, lambda r: pl.multiple_of(r * cy, 8))
    coarse_sweeps(coarse, c, mask, cx, cy, both, [both] * 3)
    add = prolong_add(c[3], fine, smooth, stage, cx, cy, cz, (0, cy - 1), (0, cy - 8))
    write_out(add, stage, out, sems, cx, [(0, 8), (2 * cy - 8, 8)])


def joined_faces(start, right):
    nx = start.shape[0]
    i = lax.broadcasted_iota(jnp.int32, (2 * SLOT, 1, 1), 0)
    z = jnp.float32(0)

    def put(v, first, many, at):
        return lax.pad(v, z, [(at - first, (2 * SLOT - at) - (nx - first), 0), (0, 0, 0), (0, 0, 0)])

    a = put(start, 0, F, 0)
    b = put(right, 0, G, F)
    c = put(start, nx - F, F, SLOT)
    d = put(right, nx - G, G, SLOT + F)
    return jnp.where(i < F, a, jnp.where(i < SLOT, b, jnp.where(i < SLOT + F, c, d)))


def on_device(start, right):
    nx, ny, nz = start.shape
    nt = nz // LANES
    xe, ye = nx + 2 * O, ny + 2 * O
    cx, cy, cz = nx // 2, ny // 2, nz // 2
    ct = cz // LANES
    cxe, cye = cx + 2 * O, cy + 2 * O
    big = f32(nt + 1, xe * ye, LANES)
    mb = 1 << 20

    msgs = call(
        xpack_body, "xpack", [joined_faces(start, right)],
        [f32(SLOT, ny, nz)] * count("gx"), limit=4 * mb, cost=9e9,
    )
    halo = exchange(msgs, "gx")
    face = [f32(-(-xe // PER), ny, LANES)] * count("gz")
    se, re, *msgs = call(build_body, "build", [start, right], [big, big] + face, limit=8 * mb)

    xhalo, n = halo, len(halo)
    msgs = call(
        functools.partial(xhalo_body, nx, ny, nz, n), "xhalo", [*xhalo, *msgs],
        face, alias={n + i: i for i in range(len(msgs))}, limit=8 * mb,
    )
    halo = exchange(msgs, "gz")
    yface = [f32(SLOT * nt + 1, xe, LANES)] * count("gy")
    se, re, *msgs = call(
        functools.partial(middle_body, nx, ny, nz, n), "middle", [*xhalo, se, re],
        [big, big] + yface, alias={n: 0, n + 1: 1}, limit=8 * mb, cost=2e9,
    )
    n = len(halo)
    se, re, *msgs = call(
        functools.partial(zhalo_body, nx, ny, nz, n), "zhalo", [*halo, se, re, *msgs],
        [big, big] + yface, alias={n + i: i for i in range(2 + len(msgs))}, limit=8 * mb,
    )
    halo = exchange(msgs, "gy")
    part = f32(nt, (cx + 1) * ny + 8, LANES)
    masks = pltpu.VMEM((nt + 1, ye, LANES), jnp.float32)
    s1, s2, rx = call(
        functools.partial(inner_body, nx, ny, nz), "inner", [se, re], [big, big, part], scratch=[masks],
        limit=8 * mb, cost=9e9,
    )
    n = len(halo)
    small = f32(ct + 1, cxe * cye, LANES)
    se, re, s1, s2, rx, coarse, *msgs = call(
        functools.partial(outer_body, nx, ny, nz, n), "outer", [*halo, se, re, s1, s2, rx],
        [big, big, big, big, part, small] + [f32(CL * ct + 1, cye, LANES)] * count(RING),
        scratch=[pltpu.VMEM((nt, (cx + 1) * cye, LANES), jnp.float32), masks],
        alias={n + i: i for i in range(5)}, limit=8 * mb,
    )
    halo = exchange(msgs, RING)
    rx, coarse = call(
        functools.partial(rest_body, nx, ny, nz), "rest", [rx, coarse], [part, small],
        scratch=[pltpu.VMEM((nt, (cx + 1) * cye, LANES), jnp.float32)], alias={0: 0, 1: 1}, limit=8 * mb, cost=2e9,
    )
    n = len(halo)
    coarse, *msgs = call(
        functools.partial(coarse_x_body, cx, cy, cz, n), "coarse_x", [*halo, coarse],
        [small] + [f32(-(-(cx + CL + CH) // CPER), cye, LANES)] * count("gz"), alias={n: 0}, limit=8 * mb,
    )
    halo = exchange(msgs, "gz")
    n = len(halo)
    coarse, *msgs = call(
        functools.partial(coarse_z_body, cx, cy, cz, n), "coarse_z", [*halo, coarse],
        [small] + [f32(CL * ct + 1, cxe, LANES)] * count("gy"), alias={n: 0}, limit=8 * mb,
    )
    halo = exchange(msgs, "gy")
    n = len(halo)
    stage = [
        pltpu.VMEM((ct + 1, cye, LANES), jnp.float32),
        pltpu.VMEM((nt, (cx + 1) * cye, LANES), jnp.float32),
        pltpu.VMEM((nt, nx, ny, LANES), jnp.float32),
    ]
    *c, out = call(
        functools.partial(finish_inner_body, cx, cy, cz), "finish_inner", [s2, coarse],
        [small] * 4 + [f32(nx, ny, nz)], scratch=stage + [pltpu.SemaphoreType.DMA((8, nt))],
        limit=10 * mb, out_specs=[VMEM] * 4 + [ANY], cost=5e9,
    )
    *_, out = call(
        functools.partial(finish_outer_body, cx, cy, cz, n), "finish_outer", [*halo, s2, coarse, *c, out],
        [small] * 5 + [f32(nx, ny, nz)], scratch=stage + [pltpu.SemaphoreType.DMA((2, 2 * nt))],
        alias={n + 1 + i: i for i in range(6)}, limit=10 * mb,
        in_specs=[VMEM] * (n + 6) + [ANY], out_specs=[VMEM] * 5 + [ANY],
    )
    return out


def solution(mesh):
    spec = P("gx", "gy", "gz")
    return jax.shard_map(on_device, mesh=mesh, in_specs=(spec, spec), out_specs=spec, check_vma=False)
```
